16 devices in a mesh: dp: 16 (over z, y, x, core).
Axes of the slice: x: 2, y: 2, z: 2, core: 2. Of those that a mesh axis runs over, the one named last changes fastest.
Arguments:
- tokens: bfloat16 [4096, 128], P('dp')
- w_one: bfloat16 [128, 512], replicated
- w_two: bfloat16 [512, 128], replicated
- wi_one: bfloat16 [128, 512], replicated
- wi_two: bfloat16 [512, 128], replicated
- item_table: bfloat16 [524288, 128], P('dp')
- cand_ids: int32 [16384], replicated
- log_q: float32 [16384], replicated
- targets: int32 [4096], P('dp')
Outputs:
- output 1: float32 [], replicated
- output 2: float32 [524288, 128], P('dp')
- output 3: float32 [128, 512], replicated
- output 4: float32 [512, 128], replicated
- output 5: float32 [128, 512], replicated
- output 6: float32 [512, 128], replicated
All inputs are finite; a program needn't handle non-finite values.
Results may differ from the reference program's by a relative error of at most 0.011364.
Values are sent between devices in bfloat16 or wider.
A program may use at most 1 GiB of HBM per device.

```python
import math
import jax
import jax.numpy as jnp
from jax import lax

DIN = 128
FF = 512
D = 128
FF2 = 512
TOK_DEV = 256
CANDS = 16384
ROWS_DEV = 32768
DEVS = 16

TOKENS = TOK_DEV * DEVS
ROWS = ROWS_DEV * DEVS
HEAD_ROWS = 4 * CANDS
SCORE_GAIN = 3.0
HIT_VALUE = -1e9


def setup_inputs(seed: int = 0) -> dict:
    root_key = jax.random.key(seed)
    val_keys = jax.random.split(root_key, 7)
    tokens = jax.random.normal(val_keys[0], (TOKENS, DIN), jnp.float32).astype(jnp.bfloat16)
    w_one = (jax.random.normal(val_keys[1], (DIN, FF), jnp.float32) * DIN ** -0.5).astype(jnp.bfloat16)
    w_two = (jax.random.normal(val_keys[2], (FF, D), jnp.float32) * FF ** -0.5).astype(jnp.bfloat16)
    wi_one = (jax.random.normal(val_keys[3], (D, FF2), jnp.float32) * D ** -0.5).astype(jnp.bfloat16)
    wi_two = (jax.random.normal(val_keys[4], (FF2, D), jnp.float32) * FF2 ** -0.5).astype(jnp.bfloat16)
    item_table = jax.random.normal(val_keys[5], (ROWS, D), jnp.float32).astype(jnp.bfloat16)
    log_q = math.log(CANDS) + jax.random.uniform(val_keys[6], (CANDS,), jnp.float32, -3.0, 3.0)
    int_keys = jax.random.split(jax.random.fold_in(root_key, 1), 7)
    head_ids = jax.random.permutation(int_keys[0], HEAD_ROWS)[: CANDS // 2]
    tail_ids = HEAD_ROWS + jax.random.permutation(int_keys[1], ROWS - HEAD_ROWS)[: CANDS - CANDS // 2]
    cand_ids = jnp.concatenate([head_ids, tail_ids])[jax.random.permutation(int_keys[2], CANDS)].astype(jnp.int32)
    pick_mode = jax.random.randint(int_keys[3], (TOKENS,), 0, 4)
    from_cands = cand_ids[jax.random.randint(int_keys[4], (TOKENS,), 0, CANDS)]
    from_head = jax.random.randint(int_keys[5], (TOKENS,), 0, HEAD_ROWS)
    from_all = jax.random.randint(int_keys[6], (TOKENS,), 0, ROWS)
    targets = jnp.where(pick_mode == 0, from_cands, jnp.where(pick_mode == 1, from_head, from_all)).astype(jnp.int32)
    return {"tokens": tokens, "w_one": w_one, "w_two": w_two, "wi_one": wi_one, "wi_two": wi_two, "item_table": item_table, "cand_ids": cand_ids, "log_q": log_q, "targets": targets}


def tower_fwd(row_block, w_in, w_out):
    pre_act = jnp.dot(row_block, w_in, preferred_element_type=jnp.float32)
    hidden = jax.nn.gelu(pre_act).astype(jnp.bfloat16)
    tower_out = jnp.dot(hidden, w_out, preferred_element_type=jnp.float32).astype(jnp.bfloat16)
    return pre_act, hidden, tower_out


def tower_back(row_block, w_out, pre_act, hidden, grad_out):
    dw_out = jnp.dot(hidden.T, grad_out, preferred_element_type=jnp.float32)
    grad_hidden = jnp.dot(grad_out, w_out.T, preferred_element_type=jnp.float32)
    gelu_back = jax.vjp(jax.nn.gelu, pre_act)[1]
    grad_pre = gelu_back(grad_hidden)[0].astype(jnp.bfloat16)
    dw_in = jnp.dot(row_block.T, grad_pre, preferred_element_type=jnp.float32)
    return grad_pre, dw_in, dw_out


def reference(tokens, w_one, w_two, wi_one, wi_two, item_table, cand_ids, log_q, targets):
    logit_scale = SCORE_GAIN / math.sqrt(D)
    cand_raw = item_table[cand_ids]
    c_pre, c_hidden, cand_vec = tower_fwd(cand_raw, wi_one, wi_two)

    def block_step(carry, blk):
        loss_acc, dcand_acc, dw_one_acc, dw_two_acc, dwi_one_acc, dwi_two_acc = carry
        tok_blk, targ_blk = blk
        q_pre, q_hidden, query = tower_fwd(tok_blk, w_one, w_two)
        targ_raw = item_table[targ_blk]
        t_pre, t_hidden, targ_vec = tower_fwd(targ_raw, wi_one, wi_two)
        z_targ = jnp.sum(query.astype(jnp.float32) * targ_vec.astype(jnp.float32), axis=1) * logit_scale
        z_cand = jnp.dot(query, cand_vec.T, preferred_element_type=jnp.float32) * logit_scale - log_q[None, :]
        z_cand = jnp.where(targ_blk[:, None] == cand_ids[None, :], HIT_VALUE, z_cand)
        row_max = jnp.maximum(z_targ, jnp.max(z_cand, axis=1))
        e_targ = jnp.exp(z_targ - row_max)
        e_cand = jnp.exp(z_cand - row_max[:, None])
        denom_sum = e_targ + jnp.sum(e_cand, axis=1)
        loss_blk = jnp.sum(jnp.log(denom_sum) + row_max - z_targ)
        dz_targ = ((e_targ / denom_sum - 1.0) / TOKENS).astype(jnp.bfloat16).astype(jnp.float32)
        dz_cand = (e_cand / denom_sum[:, None] / TOKENS).astype(jnp.bfloat16)
        d_query = ((dz_targ[:, None] * targ_vec.astype(jnp.float32) + jnp.dot(dz_cand, cand_vec, preferred_element_type=jnp.float32)) * logit_scale).astype(jnp.bfloat16)
        d_targ_vec = (logit_scale * dz_targ[:, None] * query.astype(jnp.float32)).astype(jnp.bfloat16)
        dcand_new = dcand_acc + jnp.dot(dz_cand.T, query, preferred_element_type=jnp.float32)
        dw_one_blk, dw_two_blk = tower_back(tok_blk, w_two, q_pre, q_hidden, d_query)[1:]
        t_grad_pre, dwi_one_blk, dwi_two_blk = tower_back(targ_raw, wi_two, t_pre, t_hidden, d_targ_vec)
        d_targ_raw = jnp.dot(t_grad_pre, wi_one.T, preferred_element_type=jnp.float32).astype(jnp.bfloat16)
        new_carry = (loss_acc + loss_blk, dcand_new, dw_one_acc + dw_one_blk, dw_two_acc + dw_two_blk, dwi_one_acc + dwi_one_blk, dwi_two_acc + dwi_two_blk)
        return new_carry, d_targ_raw

    init_carry = (jnp.zeros((), jnp.float32), jnp.zeros((CANDS, D), jnp.float32), jnp.zeros((DIN, FF), jnp.float32), jnp.zeros((FF, D), jnp.float32), jnp.zeros((D, FF2), jnp.float32), jnp.zeros((FF2, D), jnp.float32))
    tok_blocks = tokens.reshape(DEVS, TOK_DEV, DIN)
    targ_blocks = targets.reshape(DEVS, TOK_DEV)
    final_carry, d_targ_rows = lax.scan(block_step, init_carry, (tok_blocks, targ_blocks))
    loss_acc, dcand_acc, dw_one, dw_two, dwi_one_t, dwi_two_t = final_carry
    d_cand_vec = (logit_scale * dcand_acc).astype(jnp.bfloat16)
    c_grad_pre, dwi_one_c, dwi_two_c = tower_back(cand_raw, wi_two, c_pre, c_hidden, d_cand_vec)
    d_cand_raw = jnp.dot(c_grad_pre, wi_one.T, preferred_element_type=jnp.float32).astype(jnp.bfloat16)
    row_grads = jnp.concatenate([d_cand_raw, d_targ_rows.reshape(TOKENS, D)]).astype(jnp.float32)
    row_ids = jnp.concatenate([cand_ids, targets])
    d_table = jax.ops.segment_sum(row_grads, row_ids, num_segments=ROWS)
    return loss_acc / TOKENS, d_table, dw_one, dw_two, dwi_one_t + dwi_one_c, dwi_two_t + dwi_two_c
```

```python
import functools
import math
import jax
import jax.numpy as jnp
from jax import lax
from jax.experimental import pallas as pl
from jax.experimental.pallas import tpu as pltpu
from jax.sharding import PartitionSpec as P

SCORE_GAIN = 3.0
HIT_VALUE = -1e9
LANES = 128
VMEM_CAP = 60 * 1024 * 1024
BF = jnp.bfloat16
F32 = jnp.float32
I32 = jnp.int32
VM = pl.BlockSpec(memory_space=pltpu.VMEM)
SM = pl.BlockSpec(memory_space=pltpu.SMEM)
HB = pl.BlockSpec(memory_space=pl.ANY)
BLK = 256


def compact(loc, num_rows):
    nr = loc.shape[0]
    own = jnp.where((loc >= 0) & (loc < num_rows), 1.0, 0.0)
    own16 = own.astype(BF)
    tri = jnp.where(lax.broadcasted_iota(I32, (LANES, LANES), 0) < lax.broadcasted_iota(I32, (LANES, LANES), 1), 1.0, 0.0).astype(BF)
    within = jnp.dot(own16, tri, preferred_element_type=F32)
    low = jnp.where(lax.broadcasted_iota(I32, (nr, nr), 1) < lax.broadcasted_iota(I32, (nr, nr), 0), 1.0, 0.0).astype(BF)
    before = jnp.sum(jnp.dot(low, own16, preferred_element_type=F32), axis=1, keepdims=True)
    lane = lax.broadcasted_iota(I32, (nr, LANES), 1)
    flat = lax.broadcasted_iota(I32, (nr, LANES), 0) * LANES + lane
    disp = flat - (within + before).astype(I32)
    val = jnp.where(own > 0, flat * 32768 + loc, -1)
    total = jnp.sum(own).astype(I32)

    def back(x, s):
        if s >= LANES:
            return pltpu.roll(x, nr - s // LANES, axis=0)
        here = pltpu.roll(x, LANES - s, axis=1)
        return jnp.where(lane < LANES - s, here, pltpu.roll(here, nr - 1, axis=0))

    bit = 0
    while (1 << bit) < nr * LANES:
        val_b, disp_b = back(val, 1 << bit), back(disp, 1 << bit)
        take = (val_b >= 0) & (((disp_b >> bit) & 1) == 1)
        stay = ((disp >> bit) & 1) == 0
        val = jnp.where(take, val_b, jnp.where(stay, val, -1))
        disp = jnp.where(take, disp_b, disp)
        bit += 1
    return jnp.where(flat < total, val, nr * LANES * 32768), own, total


def gather_kernel(chunks, head, base_ref, ids_ref, table_ref, out_ref, list_ref, cnt_ref, stage, tab, dense, plist, sem, psem):
    rows = tab.shape[0]
    npos = out_ref.shape[0]
    cr = rows // chunks

    def load(c):
        return pltpu.make_async_copy(table_ref.at[pl.ds(c * cr, cr), :], stage.at[pl.ds(c * cr, cr), :], sem.at[c])

    for c in range(chunks):
        load(c).start()
    packed, own, total = compact(ids_ref[...] - base_ref[0], rows)
    list_ref[...] = packed
    cnt_ref[0] = jnp.sum(own[:head // LANES]).astype(I32)
    cnt_ref[1] = total
    to_smem = pltpu.make_async_copy(list_ref, plist, psem)
    to_smem.start()

    def zero(i, _):
        dense[pl.ds(pl.multiple_of(i * BLK, BLK), BLK), :] = jnp.zeros((BLK, LANES), F32)
        return 0

    lax.fori_loop(0, npos // BLK, zero, 0)
    for c in range(chunks):
        load(c).wait()

        def conv(i, _, c=c):
            s = pl.ds(pl.multiple_of(c * cr + i * BLK, BLK), BLK)
            tab[s, :] = stage[s, :].astype(F32)
            return 0

        lax.fori_loop(0, cr // BLK, conv, 0)
    to_smem.wait()

    def pick(i, _):
        vals = []
        for u in range(LANES):
            w = plist[i, u]
            vals.append((w >> 15, tab[pl.ds(w & 32767, 1), :]))
        for p, v in vals:
            dense[pl.ds(p, 1), :] = v
        return 0

    lax.fori_loop(0, (total + LANES - 1) // LANES, pick, 0)

    def pack(i, _):
        s = pl.ds(pl.multiple_of(i * BLK, BLK), BLK)
        out_ref[s, :] = dense[s, :].astype(BF)
        return 0

    lax.fori_loop(0, npos // BLK, pack, 0)


def gather(table, ids, base, head):
    rows = table.shape[0]
    nr = ids.shape[0]
    npos = nr * LANES
    chunks = 8
    return pl.pallas_call(
        functools.partial(gather_kernel, chunks, head),
        out_shape=(jax.ShapeDtypeStruct((npos, LANES), BF), jax.ShapeDtypeStruct((nr, LANES), I32), jax.ShapeDtypeStruct((2,), I32)),
        in_specs=[SM, VM, HB],
        out_specs=(VM, VM, SM),
        scratch_shapes=[pltpu.VMEM((rows, LANES), BF), pltpu.VMEM((rows, LANES), F32), pltpu.VMEM((npos + 8, LANES), F32), pltpu.SMEM((nr, LANES), I32), pltpu.SemaphoreType.DMA((chunks,)), pltpu.SemaphoreType.DMA],
        compiler_params=pltpu.CompilerParams(vmem_limit_bytes=VMEM_CAP),
        name="gather_rows",
    )(base, ids, table)


ADDS = 4


def scatter_kernel(chunks, cnt_ref, list_ref, grad_ref, out_ref, acc, grad, plist, sem, psem):
    rows = out_ref.shape[0]
    npos = grad_ref.shape[0]
    to_smem = pltpu.make_async_copy(list_ref, plist, psem)
    to_smem.start()

    def zero(i, _):
        acc[pl.ds(pl.multiple_of(i * BLK, BLK), BLK), :] = jnp.zeros((BLK, LANES), F32)
        return 0

    lax.fori_loop(0, rows // BLK, zero, 0)

    def conv(i, _):
        s = pl.ds(pl.multiple_of(i * BLK, BLK), BLK)
        grad[s, :] = grad_ref[s, :].astype(F32)
        return 0

    lax.fori_loop(0, npos // BLK, conv, 0)
    grad[npos:, :] = jnp.zeros((8, LANES), F32)
    to_smem.wait()
    nhead = cnt_ref[0]
    total = cnt_ref[1]

    def put(i, _):
        vals = []
        for u in range(LANES):
            w = plist[i, u]
            vals.append((w & 32767, grad[pl.ds(w >> 15, 1), :]))
        for r, v in vals:
            acc[pl.ds(r, 1), :] = v
        return 0

    lax.fori_loop(0, nhead // LANES, put, 0)

    def add_one(i, _):
        w = plist[i >> 7, i & 127]
        r = pl.ds(w & 32767, 1)
        acc[r, :] = acc[r, :] + grad[pl.ds(w >> 15, 1), :]
        return 0

    def add_row(i, _):
        for j in range(0, LANES, ADDS):
            words = [plist[i, j + u] for u in range(ADDS)]
            rs = [w & 32767 for w in words]
            gs = [grad[pl.ds(w >> 15, 1), :] for w in words]
            outs = []
            for u in range(ADDS):
                v = acc[pl.ds(rs[u], 1), :] + gs[u]
                for t in range(u):
                    v = v + jnp.where(rs[t] == rs[u], gs[t], 0.0)
                outs.append(v)
            for u in range(ADDS):
                acc[pl.ds(rs[u], 1), :] = outs[u]
        return 0

    begin = nhead // LANES * LANES
    split = jnp.minimum((nhead + LANES - 1) // LANES * LANES, total)
    lax.fori_loop(begin, split, add_one, 0)
    lax.fori_loop((split + LANES - 1) // LANES, (total + LANES - 1) // LANES, add_row, 0)
    cr = rows // chunks

    def store(c):
        return pltpu.make_async_copy(acc.at[pl.ds(c * cr, cr), :], out_ref.at[pl.ds(c * cr, cr), :], sem.at[c])

    for c in range(chunks):
        store(c).start()
    for c in range(chunks):
        store(c).wait()


def scatter(grads, plist, counts, rows):
    nr = plist.shape[0]
    npos = nr * LANES
    chunks = 8
    return pl.pallas_call(
        functools.partial(scatter_kernel, chunks),
        out_shape=jax.ShapeDtypeStruct((rows, LANES), F32),
        in_specs=[SM, HB, VM],
        out_specs=HB,
        scratch_shapes=[pltpu.VMEM((rows, LANES), F32), pltpu.VMEM((npos + 8, LANES), F32), pltpu.SMEM((nr, LANES), I32), pltpu.SemaphoreType.DMA((chunks,)), pltpu.SemaphoreType.DMA],
        compiler_params=pltpu.CompilerParams(vmem_limit_bytes=VMEM_CAP),
        name="scatter_rows",
    )(counts, plist, grads)


MESHID = pl.DeviceIdType.MESH
CHIP_DIMS = (1, 2, 4)
SLOTS = tuple(range(8))


def place():
    me = lax.axis_index("dp")
    core = lax.rem(me, 2)
    chip = me // 2
    sign = {d: 1 - 2 * lax.rem(chip // d, 2) for d in CHIP_DIMS}
    return me, core, chip, sign


def chip_at(chip, sign, s):
    for d in CHIP_DIMS:
        if s & d:
            chip = chip + d * sign[d]
    return chip


def enter():
    me, core, chip, sign = place()
    barrier = pltpu.get_barrier_semaphore()
    peers = [me + 1 - 2 * core] + [2 * chip_at(chip, sign, d) + core for d in CHIP_DIMS]
    for peer in peers:
        pl.semaphore_signal(barrier, inc=1, device_id=(peer,), device_id_type=MESHID)
    pl.semaphore_wait(barrier, len(peers))


def order_of(k):
    return tuple(CHIP_DIMS[(k + i) % 3] for i in range(3))


def pieces_of(rows, unit):
    base = rows // unit
    cuts = [(base * i // 3) * unit for i in range(4)]
    return [(cuts[i], cuts[i + 1] - cuts[i]) for i in range(3)]


def remote(src, dst, send, recv, peer):
    return pltpu.make_async_remote_copy(src_ref=src, dst_ref=dst, send_sem=send, recv_sem=recv, device_id=(peer,), device_id_type=MESHID)


CORE_ORDER = (7, 3, 5, 6, 1, 2, 4, 0)


def stage_slots(k, t):
    dims = order_of(k)
    live = [s for s in SLOTS if all(not s & d for d in dims[:t])]
    return [(s, s ^ dims[t]) for s in live if s & dims[t]]


RS_BASE = (0, 4, 6)


def rs_scratch(rows, dtype):
    return [
        pltpu.VMEM((8, rows, LANES), dtype),
        pltpu.VMEM((8, rows, LANES), dtype),
        pltpu.VMEM((7, rows, LANES), dtype),
        pltpu.SemaphoreType.DMA((8,)),
        pltpu.SemaphoreType.DMA((8,)),
        pltpu.SemaphoreType.DMA((3, 7)),
        pltpu.SemaphoreType.DMA((3, 7)),
    ]


def reduce_scatter_steps(get, pieces, scratch):
    crecv, acc, recv, csend_s, crecv_s, send_s, recv_s = scratch
    me, core, chip, sign = place()
    other = me + 1 - 2 * core
    num = len(pieces)
    started = []

    def core_copy(s):
        return remote(get(2 * chip_at(chip, sign, s) + 1 - core), crecv.at[s], csend_s.at[s], crecv_s.at[s], other)

    def ici_copy(k, t, i, s):
        off, ln = pieces[k]
        slot = RS_BASE[t] + i
        peer = 2 * chip_at(chip, sign, order_of(k)[t]) + core
        return remote(acc.at[s, pl.ds(off, ln), :], recv.at[slot, pl.ds(off, ln), :], send_s.at[k, slot], recv_s.at[k, slot], peer)

    for s in CORE_ORDER:
        c = core_copy(s)
        c.start()
        started.append(c)
    yield
    for s in CORE_ORDER:
        core_copy(s).wait_recv()
        mine = get(2 * chip_at(chip, sign, s) + core)
        acc[s] = mine[...] + crecv[s]
        for k in range(num):
            for i, (src, dst) in enumerate(stage_slots(k, 0)):
                if src == s:
                    c = ici_copy(k, 0, i, s)
                    c.start()
                    started.append(c)
    yield
    for t in range(3):
        for i in reversed(range(len(stage_slots(0, t)))):
            for k in range(num):
                off, ln = pieces[k]
                src, dst = stage_slots(k, t)[i]
                ici_copy(k, t, i, src).wait_recv()
                p = pl.ds(off, ln)
                acc[dst, p, :] = acc[dst, p, :] + recv[RS_BASE[t] + i, p, :]
                if t < 2:
                    for i2, (src2, dst2) in enumerate(stage_slots(k, t + 1)):
                        if src2 == dst:
                            c = ici_copy(k, t + 1, i2, dst)
                            c.start()
                            started.append(c)
        yield
    for c in started:
        c.wait_send()


def ag_scratch():
    return [pltpu.SemaphoreType.DMA((3, 8)), pltpu.SemaphoreType.DMA((3, 8)), pltpu.SemaphoreType.DMA((3, 8)), pltpu.SemaphoreType.DMA((3, 8))]


def all_gather_steps(own, out, pieces, scratch):
    csend_s, crecv_s, send_s, recv_s = scratch
    me, core, chip, sign = place()
    other = me + 1 - 2 * core
    num = len(pieces)
    started = []

    def ref(k, s):
        off, ln = pieces[k]
        return out(2 * chip_at(chip, sign, s) + core).at[pl.ds(off, ln), :]

    def source(k, s):
        off, ln = pieces[k]
        return own.at[pl.ds(off, ln), :] if s == 0 else ref(k, s)

    def core_copy(k, s):
        return remote(source(k, s), ref(k, s), csend_s.at[k, s], crecv_s.at[k, s], other)

    def core_wait(k, s):
        off, ln = pieces[k]
        there = out(2 * chip_at(chip, sign, s) + 1 - core).at[pl.ds(off, ln), :]
        remote(there, there, csend_s.at[k, s], crecv_s.at[k, s], other).wait_recv()

    def ici_copy(k, t, s):
        d = order_of(k)[t]
        peer = 2 * chip_at(chip, sign, d) + core
        return remote(source(k, s), ref(k, s), send_s.at[k, s ^ d], recv_s.at[k, s ^ d], peer)

    def ici_wait(k, s):
        remote(ref(k, s), ref(k, s), send_s.at[k, s], recv_s.at[k, s], other).wait_recv()

    def go(c):
        c.start()
        started.append(c)

    def live(k, t):
        dims = order_of(k)[:t]
        rest = order_of(k)[t:]
        return [s for s in SLOTS if all(not s & d for d in rest)]

    for t in range(3):
        for k in range(num):
            go(ici_copy(k, t, 0))
    for k in range(num):
        go(core_copy(k, 0))
    yield
    for t in range(3):
        for i in range(len(live(0, t))):
            for k in range(num):
                d = order_of(k)[t]
                s = live(k, t)[i] ^ d
                ici_wait(k, s)
                for t2 in range(t + 1, 3):
                    go(ici_copy(k, t2, s))
                go(core_copy(k, s))
        yield
    for k in range(num):
        for s in SLOTS:
            core_wait(k, s)
    for c in started:
        c.wait_send()


def rs_kernel(pieces, x_ref, out_ref, *scratch):
    enter()
    for _ in reduce_scatter_steps(lambda dev: x_ref.at[dev], pieces, scratch):
        pass
    out_ref[...] = scratch[1][0]


def ag_kernel(pieces, x_ref, out_ref, *scratch):
    enter()
    out_ref[lax.axis_index("dp")] = x_ref[...]
    for _ in all_gather_steps(x_ref, lambda dev: out_ref.at[dev], pieces, scratch):
        pass


def ar_kernel(pieces, x_ref, out_ref, *scratch):
    enter()
    n = len(rs_scratch(8, F32))
    for _ in reduce_scatter_steps(lambda dev: x_ref.at[dev], pieces, scratch[:n]):
        pass
    acc = scratch[1]
    out_ref[lax.axis_index("dp")] = acc[0]
    for _ in all_gather_steps(acc.at[0], lambda dev: out_ref.at[dev], pieces, scratch[n:]):
        pass


def stats_kernel(x_ref, out_ref, held, recv, send_s, recv_s):
    enter()
    me, core, chip, sign = place()
    peers = [me + 1 - 2 * core] + [2 * chip_at(chip, sign, d) + core for d in CHIP_DIMS]
    src = x_ref
    for t, peer in enumerate(peers):
        c = remote(src, recv.at[t], send_s.at[t], recv_s.at[t], peer)
        c.start()
        c.wait()
        top = jnp.maximum(src[0], recv[t, 0])
        den = src[1] * jnp.exp(src[0] - top) + recv[t, 1] * jnp.exp(recv[t, 0] - top)
        dst = held.at[t] if t < 3 else out_ref
        dst[0] = top
        dst[1] = den
        src = dst


def comm_call(body, name, cid, out_shape, scratch, *args):
    return pl.pallas_call(
        body,
        out_shape=out_shape,
        in_specs=[VM] * len(args),
        out_specs=jax.tree.map(lambda _: VM, out_shape),
        scratch_shapes=scratch,
        compiler_params=pltpu.CompilerParams(collective_id=cid, has_side_effects=True, vmem_limit_bytes=VMEM_CAP),
        name=name,
    )(*args)


def cut(x):
    rows = x.shape[-2]
    return pieces_of(rows, 16 if x.dtype == BF else 8) if rows >= 48 else [(0, rows)]


def rs(x, cid):
    n, rows, _ = x.shape
    return comm_call(functools.partial(rs_kernel, cut(x)), "sum_scatter", cid, jax.ShapeDtypeStruct((rows, LANES), x.dtype), rs_scratch(rows, x.dtype), x)


def ag(x, cid, n=16):
    rows = x.shape[0]
    return comm_call(functools.partial(ag_kernel, cut(x)), "all_rows", cid, jax.ShapeDtypeStruct((n, rows, LANES), x.dtype), ag_scratch(), x)


def ar(x, cid):
    n, rows, _ = x.shape
    return comm_call(functools.partial(ar_kernel, cut(x)), "sum_all", cid, jax.ShapeDtypeStruct((n, rows, LANES), F32), rs_scratch(rows, F32) + ag_scratch(), x)


def stats(x, cid):
    sems = pltpu.SemaphoreType.DMA((4,))
    return comm_call(stats_kernel, "soft_stats", cid, jax.ShapeDtypeStruct(x.shape, F32), [pltpu.VMEM((3,) + x.shape, F32), pltpu.VMEM((4,) + x.shape, F32), sems, sems], x)


def tower_fwd(row_block, w_in, w_out):
    pre_act = jnp.dot(row_block, w_in, preferred_element_type=F32)
    hidden = jax.nn.gelu(pre_act).astype(BF)
    return pre_act, hidden, jnp.dot(hidden, w_out, preferred_element_type=F32).astype(BF)


def tower_back(row_block, w_out, pre_act, hidden, grad_out):
    dw_out = jnp.einsum("nf,nd->fd", hidden, grad_out, preferred_element_type=F32)
    grad_hidden = jnp.einsum("nd,fd->nf", grad_out, w_out, preferred_element_type=F32)
    grad_pre = jax.vjp(jax.nn.gelu, pre_act)[1](grad_hidden)[0].astype(BF)
    dw_in = jnp.einsum("ne,nf->ef", row_block, grad_pre, preferred_element_type=F32)
    return grad_pre, dw_in, dw_out


def solution(mesh):
    num_dev = mesh.shape["dp"]

    def local_step(tokens, w_one, w_two, wi_one, wi_two, table_loc, cand_ids, log_q, targ_loc):
        my_index = lax.axis_index("dp")
        rows_loc = table_loc.shape[0]
        num_tok = tokens.shape[0]
        tok_total = num_tok * num_dev
        num_cand = cand_ids.shape[0]
        cand_loc = num_cand // num_dev
        dim = table_loc.shape[1]
        scale = SCORE_GAIN / math.sqrt(dim)
        targ_all = ag(targ_loc.reshape(-1, LANES), 1).reshape(-1)
        ids = jnp.concatenate([cand_ids, targ_all]).reshape(-1, LANES)
        base = (my_index * rows_loc).reshape(1).astype(I32)
        owned, plist, counts = gather(table_loc, ids, base, num_cand)
        raw_c = rs(owned[:num_cand].reshape(num_dev, cand_loc, dim), 2)
        raw_t = rs(owned[num_cand:].reshape(num_dev, num_tok, dim), 3)
        q_pre, q_hidden, query = tower_fwd(tokens, w_one, w_two)
        query_all = ag(query, 4).reshape(tok_total, dim)
        raw = jnp.concatenate([raw_c, raw_t])
        i_pre, i_hidden, vec = tower_fwd(raw, wi_one, wi_two)
        cand_vec, targ_vec = vec[:cand_loc], vec[cand_loc:]
        my_ids = lax.dynamic_slice_in_dim(cand_ids, my_index * cand_loc, cand_loc)
        my_logq = lax.dynamic_slice_in_dim(log_q, my_index * cand_loc, cand_loc)
        z = jnp.einsum("td,sd->ts", query_all, cand_vec, preferred_element_type=F32) * scale - my_logq[None, :]
        z = jnp.where(targ_all[:, None] == my_ids[None, :], HIT_VALUE, z)
        top = jnp.max(z, axis=1)
        e = jnp.exp(z - top[:, None])
        den = jnp.sum(e, axis=1)
        z_targ = jnp.einsum("td,td->t", query, targ_vec, preferred_element_type=F32) * scale
        mine = my_index * num_tok
        z_all = lax.dynamic_update_slice_in_dim(jnp.full((tok_total,), -jnp.inf, F32), z_targ, mine, 0)
        top_t = jnp.maximum(top, z_all)
        den_t = den * jnp.exp(top - top_t) + jnp.exp(z_all - top_t)
        st = stats(jnp.stack([top_t, den_t]).reshape(2, -1, LANES), 5).reshape(2, tok_total)
        factor = jnp.exp(top - st[0]) / st[1] / tok_total
        dz = (e * factor[:, None]).astype(BF)
        dh_part = jnp.einsum("ts,sd->td", dz, cand_vec, preferred_element_type=F32)
        d_cand = (jnp.einsum("ts,td->sd", dz, query_all, preferred_element_type=F32) * scale).astype(BF)
        my_top = lax.dynamic_slice_in_dim(st[0], mine, num_tok)
        my_den = lax.dynamic_slice_in_dim(st[1], mine, num_tok)
        loss_sum = jnp.sum(jnp.log(my_den) + my_top - z_targ)
        dz_targ = ((jnp.exp(z_targ - my_top) / my_den - 1.0) / tok_total).astype(BF).astype(F32)
        dh_cand = rs(dh_part.reshape(num_dev, num_tok, dim), 6)
        d_query = ((dz_targ[:, None] * targ_vec.astype(F32) + dh_cand) * scale).astype(BF)
        d_targ = (scale * dz_targ[:, None] * query.astype(F32)).astype(BF)
        dw_one, dw_two = tower_back(tokens, w_two, q_pre, q_hidden, d_query)[1:]
        i_grad_pre, dwi_one, dwi_two = tower_back(raw, wi_two, i_pre, i_hidden, jnp.concatenate([d_cand, d_targ]))
        d_raw = jnp.einsum("nf,df->nd", i_grad_pre, wi_one, preferred_element_type=F32).astype(BF)
        back_c = ag(d_raw[:cand_loc], 7).reshape(num_cand, dim)
        back_t = ag(d_raw[cand_loc:], 8).reshape(tok_total, dim)
        d_table = scatter(jnp.concatenate([back_c, back_t]), plist, counts, rows_loc)
        extra = jnp.zeros((num_dev * 8, LANES), F32).at[0, 0].set(loss_sum)
        parts = jnp.concatenate([w.reshape(-1, LANES) for w in (dw_one, dw_two, dwi_one, dwi_two)] + [extra])
        sums = ar(parts.reshape(num_dev, -1, LANES), 9).reshape(-1, LANES)
        n = dw_one.size // LANES
        outs = [sums[i * n:(i + 1) * n].reshape(w.shape) for i, w in enumerate((dw_one, dw_two, dwi_one, dwi_two))]
        return (sums[4 * n, 0] / tok_total, d_table) + tuple(outs)

    return jax.shard_map(local_step, mesh=mesh, in_specs=(P("dp", None), P(), P(), P(), P(), P("dp", None), P(), P(), P("dp")), out_specs=(P(), P("dp", None), P(), P(), P(), P()), check_vma=False)
```

```python
import functools
import math
import jax
import jax.numpy as jnp
from jax import lax
from jax.experimental import pallas as pl
from jax.experimental.pallas import tpu as pltpu
from jax.sharding import PartitionSpec as P

SCORE_GAIN = 3.0
HIT_VALUE = -1e9
LANES = 128
VMEM_CAP = 60 * 1024 * 1024
BF = jnp.bfloat16
F32 = jnp.float32
I32 = jnp.int32
VM = pl.BlockSpec(memory_space=pltpu.VMEM)
SM = pl.BlockSpec(memory_space=pltpu.SMEM)
HB = pl.BlockSpec(memory_space=pl.ANY)
BLK = 256


def compact(loc, num_rows, parts, head):
    nr = loc.shape[0]
    own = jnp.where((loc >= 0) & (loc < num_rows), 1.0, 0.0)
    own16 = own.astype(BF)
    tri = jnp.where(lax.broadcasted_iota(I32, (LANES, LANES), 0) < lax.broadcasted_iota(I32, (LANES, LANES), 1), 1.0, 0.0).astype(BF)
    within = jnp.dot(own16, tri, preferred_element_type=F32)
    low = jnp.where(lax.broadcasted_iota(I32, (nr, nr), 1) < lax.broadcasted_iota(I32, (nr, nr), 0), 1.0, 0.0).astype(BF)
    before = jnp.sum(jnp.dot(low, own16, preferred_element_type=F32), axis=1, keepdims=True)
    lane = lax.broadcasted_iota(I32, (nr, LANES), 1)
    flat = lax.broadcasted_iota(I32, (nr, LANES), 0) * LANES + lane
    disp = flat - (within + before).astype(I32)
    n_head, n_tail = head // parts, (nr * LANES - head) // parts
    late = flat - head
    pos = jnp.where(flat < head, flat + flat // n_head * n_tail, late + (late // n_tail + 1) * n_head)
    val = jnp.where(own > 0, pos * 32768 + loc, -1)
    total = jnp.sum(own).astype(I32)

    def back(x, s):
        if s >= LANES:
            return pltpu.roll(x, nr - s // LANES, axis=0)
        here = pltpu.roll(x, LANES - s, axis=1)
        return jnp.where(lane < LANES - s, here, pltpu.roll(here, nr - 1, axis=0))

    bit = 0
    while (1 << bit) < nr * LANES:
        val_b, disp_b = back(val, 1 << bit), back(disp, 1 << bit)
        take = (val_b >= 0) & (((disp_b >> bit) & 1) == 1)
        stay = ((disp >> bit) & 1) == 0
        val = jnp.where(take, val_b, jnp.where(stay, val, -1))
        disp = jnp.where(take, disp_b, disp)
        bit += 1
    return jnp.where(flat < total, val, nr * LANES * 32768), own, total


def gather_kernel(chunks, head, parts, base_ref, ids_ref, table_ref, out_ref, list_ref, cnt_ref, stage, tab, dense, plist, sem, psem):
    rows = tab.shape[0]
    npos = out_ref.shape[0]
    cr = rows // chunks

    def load(c):
        return pltpu.make_async_copy(table_ref.at[pl.ds(c * cr, cr), :], stage.at[pl.ds(c * cr, cr), :], sem.at[c])

    for c in range(chunks):
        load(c).start()
    packed, own, total = compact(ids_ref[...] - base_ref[0], rows, parts, head)
    list_ref[...] = packed
    cnt_ref[0] = jnp.sum(own[:head // LANES]).astype(I32)
    cnt_ref[1] = total
    to_smem = pltpu.make_async_copy(list_ref, plist, psem)
    to_smem.start()

    def zero(i, _):
        dense[pl.ds(pl.multiple_of(i * BLK, BLK), BLK), :] = jnp.zeros((BLK, LANES), F32)
        return 0

    lax.fori_loop(0, npos // BLK, zero, 0)
    for c in range(chunks):
        load(c).wait()

        def conv(i, _, c=c):
            s = pl.ds(pl.multiple_of(c * cr + i * BLK, BLK), BLK)
            tab[s, :] = stage[s, :].astype(F32)
            return 0

        lax.fori_loop(0, cr // BLK, conv, 0)
    to_smem.wait()

    def pick(i, _):
        vals = []
        for u in range(LANES):
            w = plist[i, u]
            vals.append((w >> 15, tab[pl.ds(w & 32767, 1), :]))
        for p, v in vals:
            dense[pl.ds(p, 1), :] = v
        return 0

    lax.fori_loop(0, (total + LANES - 1) // LANES, pick, 0)

    def pack(i, _):
        s = pl.ds(pl.multiple_of(i * BLK, BLK), BLK)
        out_ref[s, :] = dense[s, :].astype(BF)
        return 0

    lax.fori_loop(0, npos // BLK, pack, 0)


def gather(table, ids, base, head, parts):
    rows = table.shape[0]
    nr = ids.shape[0]
    npos = nr * LANES
    chunks = 8
    return pl.pallas_call(
        functools.partial(gather_kernel, chunks, head, parts),
        out_shape=(jax.ShapeDtypeStruct((npos, LANES), BF), jax.ShapeDtypeStruct((nr, LANES), I32), jax.ShapeDtypeStruct((2,), I32)),
        in_specs=[SM, VM, HB],
        out_specs=(VM, VM, SM),
        scratch_shapes=[pltpu.VMEM((rows, LANES), BF), pltpu.VMEM((rows, LANES), F32), pltpu.VMEM((npos + 8, LANES), F32), pltpu.SMEM((nr, LANES), I32), pltpu.SemaphoreType.DMA((chunks,)), pltpu.SemaphoreType.DMA],
        compiler_params=pltpu.CompilerParams(vmem_limit_bytes=VMEM_CAP),
        name="gather_rows",
    )(base, ids, table)


ADDS = 4


def scatter_kernel(chunks, cnt_ref, list_ref, grad_ref, out_ref, acc, grad, plist, sem, psem):
    rows = out_ref.shape[0]
    npos = grad_ref.shape[0]
    to_smem = pltpu.make_async_copy(list_ref, plist, psem)
    to_smem.start()

    def zero(i, _):
        acc[pl.ds(pl.multiple_of(i * BLK, BLK), BLK), :] = jnp.zeros((BLK, LANES), F32)
        return 0

    lax.fori_loop(0, rows // BLK, zero, 0)

    def conv(i, _):
        s = pl.ds(pl.multiple_of(i * BLK, BLK), BLK)
        grad[s, :] = grad_ref[s, :].astype(F32)
        return 0

    lax.fori_loop(0, npos // BLK, conv, 0)
    grad[npos:, :] = jnp.zeros((8, LANES), F32)
    to_smem.wait()
    nhead = cnt_ref[0]
    total = cnt_ref[1]

    def put(i, _):
        vals = []
        for u in range(LANES):
            w = plist[i, u]
            vals.append((w & 32767, grad[pl.ds(w >> 15, 1), :]))
        for r, v in vals:
            acc[pl.ds(r, 1), :] = v
        return 0

    lax.fori_loop(0, nhead // LANES, put, 0)

    def add_one(i, _):
        w = plist[i >> 7, i & 127]
        r = pl.ds(w & 32767, 1)
        acc[r, :] = acc[r, :] + grad[pl.ds(w >> 15, 1), :]
        return 0

    def add_row(i, _):
        for j in range(0, LANES, ADDS):
            words = [plist[i, j + u] for u in range(ADDS)]
            rs = [w & 32767 for w in words]
            gs = [grad[pl.ds(w >> 15, 1), :] for w in words]
            outs = []
            for u in range(ADDS):
                v = acc[pl.ds(rs[u], 1), :] + gs[u]
                for t in range(u):
                    v = v + jnp.where(rs[t] == rs[u], gs[t], 0.0)
                outs.append(v)
            for u in range(ADDS):
                acc[pl.ds(rs[u], 1), :] = outs[u]
        return 0

    begin = nhead // LANES * LANES
    split = jnp.minimum((nhead + LANES - 1) // LANES * LANES, total)
    lax.fori_loop(begin, split, add_one, 0)
    lax.fori_loop((split + LANES - 1) // LANES, (total + LANES - 1) // LANES, add_row, 0)
    cr = rows // chunks

    def store(c):
        return pltpu.make_async_copy(acc.at[pl.ds(c * cr, cr), :], out_ref.at[pl.ds(c * cr, cr), :], sem.at[c])

    for c in range(chunks):
        store(c).start()
    for c in range(chunks):
        store(c).wait()


def scatter(grads, plist, counts, rows):
    nr = plist.shape[0]
    npos = nr * LANES
    chunks = 8
    return pl.pallas_call(
        functools.partial(scatter_kernel, chunks),
        out_shape=jax.ShapeDtypeStruct((rows, LANES), F32),
        in_specs=[SM, HB, VM],
        out_specs=HB,
        scratch_shapes=[pltpu.VMEM((rows, LANES), F32), pltpu.VMEM((npos + 8, LANES), F32), pltpu.SMEM((nr, LANES), I32), pltpu.SemaphoreType.DMA((chunks,)), pltpu.SemaphoreType.DMA],
        compiler_params=pltpu.CompilerParams(vmem_limit_bytes=VMEM_CAP),
        name="scatter_rows",
    )(counts, plist, grads)


MESHID = pl.DeviceIdType.MESH
CHIP_DIMS = (1, 2, 4)
SLOTS = tuple(range(8))


def place():
    me = lax.axis_index("dp")
    core = lax.rem(me, 2)
    chip = me // 2
    sign = {d: 1 - 2 * lax.rem(chip // d, 2) for d in CHIP_DIMS}
    return me, core, chip, sign


def chip_at(chip, sign, s):
    for d in CHIP_DIMS:
        if s & d:
            chip = chip + d * sign[d]
    return chip


def enter():
    me, core, chip, sign = place()
    barrier = pltpu.get_barrier_semaphore()
    peers = [me + 1 - 2 * core] + [2 * chip_at(chip, sign, d) + core for d in CHIP_DIMS]
    for peer in peers:
        pl.semaphore_signal(barrier, inc=1, device_id=(peer,), device_id_type=MESHID)
    pl.semaphore_wait(barrier, len(peers))


def order_of(k):
    return tuple(CHIP_DIMS[(k + i) % 3] for i in range(3))


def pieces_of(rows, unit):
    base = rows // unit
    cuts = [(base * i // 3) * unit for i in range(4)]
    return [(cuts[i], cuts[i + 1] - cuts[i]) for i in range(3)]


def remote(src, dst, send, recv, peer):
    return pltpu.make_async_remote_copy(src_ref=src, dst_ref=dst, send_sem=send, recv_sem=recv, device_id=(peer,), device_id_type=MESHID)


CORE_ORDER = (7, 3, 5, 6, 1, 2, 4, 0)


def stage_slots(k, t):
    dims = order_of(k)
    live = [s for s in SLOTS if all(not s & d for d in dims[:t])]
    return [(s, s ^ dims[t]) for s in live if s & dims[t]]


RS_BASE = (0, 4, 6)


def rs_scratch(rows, dtype, width=LANES):
    return [
        pltpu.VMEM((8, rows, width), dtype),
        pltpu.VMEM((8, rows, width), dtype),
        pltpu.VMEM((7, rows, width), dtype),
        pltpu.SemaphoreType.DMA((8,)),
        pltpu.SemaphoreType.DMA((8,)),
        pltpu.SemaphoreType.DMA((3, 7)),
        pltpu.SemaphoreType.DMA((3, 7)),
    ]


def reduce_scatter_steps(get, pieces, scratch):
    crecv, acc, recv, csend_s, crecv_s, send_s, recv_s = scratch
    me, core, chip, sign = place()
    other = me + 1 - 2 * core
    num = len(pieces)
    started = []

    def core_copy(s):
        return remote(get(2 * chip_at(chip, sign, s) + 1 - core), crecv.at[s], csend_s.at[s], crecv_s.at[s], other)

    def ici_copy(k, t, i, s):
        off, ln = pieces[k]
        slot = RS_BASE[t] + i
        peer = 2 * chip_at(chip, sign, order_of(k)[t]) + core
        return remote(acc.at[s, pl.ds(off, ln), :], recv.at[slot, pl.ds(off, ln), :], send_s.at[k, slot], recv_s.at[k, slot], peer)

    for s in CORE_ORDER:
        c = core_copy(s)
        c.start()
        started.append(c)
    yield
    for s in CORE_ORDER:
        core_copy(s).wait_recv()
        mine = get(2 * chip_at(chip, sign, s) + core)
        acc[s] = mine[...] + crecv[s]
        for k in range(num):
            for i, (src, dst) in enumerate(stage_slots(k, 0)):
                if src == s:
                    c = ici_copy(k, 0, i, s)
                    c.start()
                    started.append(c)
    yield
    for t in range(3):
        for i in reversed(range(len(stage_slots(0, t)))):
            for k in range(num):
                off, ln = pieces[k]
                src, dst = stage_slots(k, t)[i]
                ici_copy(k, t, i, src).wait_recv()
                p = pl.ds(off, ln)
                acc[dst, p, :] = acc[dst, p, :] + recv[RS_BASE[t] + i, p, :]
                if t < 2:
                    for i2, (src2, dst2) in enumerate(stage_slots(k, t + 1)):
                        if src2 == dst:
                            c = ici_copy(k, t + 1, i2, dst)
                            c.start()
                            started.append(c)
        yield
    for c in started:
        c.wait_send()


def ag_scratch():
    return [pltpu.SemaphoreType.DMA((3, 8)), pltpu.SemaphoreType.DMA((3, 8)), pltpu.SemaphoreType.DMA((3, 8)), pltpu.SemaphoreType.DMA((3, 8))]


def all_gather_steps(own, out, pieces, scratch):
    csend_s, crecv_s, send_s, recv_s = scratch
    me, core, chip, sign = place()
    other = me + 1 - 2 * core
    num = len(pieces)
    started = []

    def ref(k, s):
        off, ln = pieces[k]
        return out(2 * chip_at(chip, sign, s) + core).at[pl.ds(off, ln), :]

    def source(k, s):
        off, ln = pieces[k]
        return own.at[pl.ds(off, ln), :] if s == 0 else ref(k, s)

    def core_copy(k, s):
        return remote(source(k, s), ref(k, s), csend_s.at[k, s], crecv_s.at[k, s], other)

    def core_wait(k, s):
        off, ln = pieces[k]
        there = out(2 * chip_at(chip, sign, s) + 1 - core).at[pl.ds(off, ln), :]
        remote(there, there, csend_s.at[k, s], crecv_s.at[k, s], other).wait_recv()

    def ici_copy(k, t, s):
        d = order_of(k)[t]
        peer = 2 * chip_at(chip, sign, d) + core
        return remote(source(k, s), ref(k, s), send_s.at[k, s ^ d], recv_s.at[k, s ^ d], peer)

    def ici_wait(k, s):
        remote(ref(k, s), ref(k, s), send_s.at[k, s], recv_s.at[k, s], other).wait_recv()

    def go(c):
        c.start()
        started.append(c)

    def live(k, t):
        dims = order_of(k)[:t]
        rest = order_of(k)[t:]
        return [s for s in SLOTS if all(not s & d for d in rest)]

    for t in range(3):
        for k in range(num):
            go(ici_copy(k, t, 0))
    for k in range(num):
        go(core_copy(k, 0))
    yield
    for t in range(3):
        for i in range(len(live(0, t))):
            for k in range(num):
                d = order_of(k)[t]
                s = live(k, t)[i] ^ d
                ici_wait(k, s)
                for t2 in range(t + 1, 3):
                    go(ici_copy(k, t2, s))
                go(core_copy(k, s))
        yield
    for k in range(num):
        for s in SLOTS:
            core_wait(k, s)
    for c in started:
        c.wait_send()


def ag_kernel(pieces, x_ref, out_ref, *scratch):
    enter()
    out_ref[lax.axis_index("dp")] = x_ref[...]
    for _ in all_gather_steps(x_ref, lambda dev: out_ref.at[dev], pieces, scratch):
        pass


def comm_call(body, name, cid, out_shape, scratch, *args):
    return pl.pallas_call(
        body,
        out_shape=out_shape,
        in_specs=[VM] * len(args),
        out_specs=jax.tree.map(lambda _: VM, out_shape),
        scratch_shapes=scratch,
        compiler_params=pltpu.CompilerParams(collective_id=cid, has_side_effects=True, vmem_limit_bytes=VMEM_CAP),
        name=name,
    )(*args)


def cut(x):
    rows = x.shape[-2]
    return pieces_of(rows, 16 if x.dtype == BF else 8) if rows >= 48 else [(0, rows)]


def ag(x, cid, n=16):
    rows = x.shape[0]
    return comm_call(functools.partial(ag_kernel, cut(x)), "all_rows", cid, jax.ShapeDtypeStruct((n, rows, LANES), x.dtype), ag_scratch(), x)


LOG2E = 1.4426950408889634
GELU_C = math.sqrt(2.0 / math.pi)
GELU_A = 0.044715
ROW_BLK = 256


def gelu_both(x):
    x2 = x * x
    t = jnp.tanh(GELU_C * (x + GELU_A * (x2 * x)))
    half = 0.5 * (1.0 + t)
    return x * half, half + (0.5 * GELU_C) * x * (1.0 - t * t) * (1.0 + (3.0 * GELU_A) * x2)


def dot_nn(a, b):
    return jnp.dot(a, b, preferred_element_type=F32)


def dot_nt(a, b):
    return lax.dot_general(a, b, (((1,), (1,)), ((), ())), preferred_element_type=F32)


def turn(x):
    return x.astype(F32).T.astype(BF)


def tower_into(rows, load, w_in, w_out, slope_ref, hid_ref, out_ref):
    def blk(i, _):
        s = pl.ds(pl.multiple_of(i * ROW_BLK, ROW_BLK), ROW_BLK)
        act, slope = gelu_both(dot_nn(load(s), w_in[...]))
        slope_ref[s, :] = slope
        hid_ref[s, :] = act.astype(BF)
        out_ref[s, :] = dot_nn(hid_ref[s, :], w_out[...]).astype(BF)
        return 0

    lax.fori_loop(0, rows // ROW_BLK, blk, 0)


def tower_pre_grad(rows, grad_ref, w_out, slope_ref, pre_ref):
    def blk(i, _):
        s = pl.ds(pl.multiple_of(i * ROW_BLK, ROW_BLK), ROW_BLK)
        pre_ref[s, :] = (slope_ref[s, :] * dot_nt(grad_ref[s, :], w_out[...])).astype(BF)
        return 0

    lax.fori_loop(0, rows // ROW_BLK, blk, 0)


def weight_grads(row_t, grad_t, pre_ref, hid_ref, sums_ref, parts, off):
    d_in = dot_nn(row_t, pre_ref[...])
    d_out = dot_nn(grad_t, hid_ref[...])
    for which, w in enumerate((d_in, d_out)):
        for c in range(4):
            for h in range(2):
                sums_ref[which * 8 + c * 2 + h, :64, :] = w[h * 64:(h + 1) * 64, c * LANES:(c + 1) * LANES]


def step_kernel(shapes, names, x_ref, tok_ref, w1, w2, wi1, wi2, lq_ref, id_ref, targ_ref, rows_out, isum_out, qsum_out, *scratch):
    n_cand, n_tok, parts = shapes
    n_item = n_cand + n_tok
    total = float(n_tok * parts)
    scale = SCORE_GAIN / math.sqrt(LANES)
    v = dict(zip(names, scratch))

    def group(name):
        return [v[k] for k in names if k.startswith(name + ".")]

    enter()
    me, core, chip, sign = place()
    rs_rows = reduce_scatter_steps(lambda dev: x_ref.at[dev], pieces_of(n_item, 16), group("rs"))
    next(rs_rows)
    tower_into(n_tok, lambda s: tok_ref[s, :], w1, w2, v["q_slope"], v["q_hid"], v["q_vec"])
    q_all = v["q_all"]
    q_all[me] = v["q_vec"][...]
    ag_q = all_gather_steps(v["q_vec"], lambda dev: q_all.at[dev], pieces_of(n_tok, 16), group("agq"))
    next(ag_q)
    next(rs_rows)
    for _ in range(3):
        next(rs_rows)
        next(ag_q)
    for g in (rs_rows, ag_q):
        for _ in g:
            pass
    raw = v["rs.1"].at[0]
    tower_into(n_item, lambda s: raw[s, :], wi1, wi2, v["i_slope"], v["i_hid"], v["i_vec"])
    vec = v["i_vec"]
    z_ref, top_ref, den_ref = v["z"], v["top"], v["den"]
    jb = 128

    def pass_one(t, _):
        q_t = q_all[t]
        targ = targ_ref[pl.ds(t, 1), :]
        top8 = jnp.full((8, n_tok), -jnp.inf, F32)
        for j in range(n_cand // jb):
            s = pl.ds(j * jb, jb)
            lq = jnp.concatenate([lq_ref[s, :]] * 2, axis=1)
            ids = jnp.concatenate([id_ref[s, :]] * 2, axis=1)
            z = dot_nt(vec[s, :], q_t) * (scale * LOG2E) - lq
            z = jnp.where(ids == targ, HIT_VALUE * LOG2E, z)
            z_ref[t, s, :] = z
            top8 = jnp.maximum(top8, jnp.max(z.reshape(jb // 8, 8, n_tok), axis=0))
        top = jnp.max(top8, axis=0, keepdims=True)
        den8 = jnp.zeros((8, n_tok), F32)
        for j in range(n_cand // jb):
            e = jnp.exp2(z_ref[t, pl.ds(j * jb, jb), :] - top)
            den8 = den8 + jnp.sum(e.reshape(jb // 8, 8, n_tok), axis=0)
        top_ref[pl.ds(t, 1), :] = top
        den_ref[pl.ds(t, 1), :] = jnp.sum(den8, axis=0, keepdims=True)
        return 0

    lax.fori_loop(0, parts, pass_one, 0)
    own = pl.ds(me, 1)
    targ_vec = vec[pl.ds(n_cand, n_tok), :]
    q_own = v["q_vec"][...]
    eye = lax.broadcasted_iota(I32, (n_tok, n_tok), 0) == lax.broadcasted_iota(I32, (n_tok, n_tok), 1)
    z_own = jnp.sum(jnp.where(eye, dot_nt(targ_vec, q_own), 0.0), axis=0, keepdims=True) * (scale * LOG2E)
    new_top = jnp.maximum(top_ref[own, :], z_own)
    den_ref[own, :] = den_ref[own, :] * jnp.exp2(top_ref[own, :] - new_top) + jnp.exp2(z_own - new_top)
    top_ref[own, :] = new_top

    held, got, st_send, st_recv = group("st")
    held[0, 0] = top_ref[...]
    held[0, 1] = den_ref[...]
    peers = [me + 1 - 2 * core] + [2 * chip_at(chip, sign, d) + core for d in CHIP_DIMS]
    for i, peer in enumerate(peers):
        c = remote(held.at[i], got.at[i], st_send.at[i], st_recv.at[i], peer)
        c.start()
        c.wait()
        top = jnp.maximum(held[i, 0], got[i, 0])
        den = held[i, 1] * jnp.exp2(held[i, 0] - top) + got[i, 1] * jnp.exp2(got[i, 0] - top)
        held[i + 1, 0] = top
        held[i + 1, 1] = den
    last = len(peers)
    norm = v["norm"]
    norm[...] = held[last, 0] + jnp.log2(held[last, 1] * total)
    top_ref[...] = held[last, 0]
    den_ref[...] = held[last, 1]

    lse = top_ref[own, :] + jnp.log2(den_ref[own, :])
    loss = jnp.sum(lse - z_own, axis=1, keepdims=True) * (1.0 / LOG2E)
    dz_row = ((jnp.exp2(z_own - top_ref[own, :]) / den_ref[own, :] - 1.0) * (1.0 / total)).astype(BF).astype(F32)
    dz_col = jnp.sum(jnp.where(eye, dz_row, 0.0), axis=1, keepdims=True)
    grad = v["i_grad"]
    grad[pl.ds(n_cand, n_tok), :] = (scale * dz_col * q_own.astype(F32)).astype(BF)
    vec_t = v["vec_t"]
    vec_t[...] = turn(vec[:n_cand, :])
    d_acc, dz_s, dh = v["d_acc"], v["dz"], v["dh"]
    d_acc[...] = jnp.zeros_like(d_acc)

    def pass_two(t, _):
        shift = norm[pl.ds(t, 1), :]
        for j in range(n_cand // jb):
            s = pl.ds(j * jb, jb)
            dz_s[s, :] = jnp.exp2(z_ref[t, s, :] - shift).astype(BF)
        d_acc[...] += dot_nn(dz_s[...], q_all[t])
        dh[t] = dot_nn(vec_t[...], dz_s[...])
        return 0

    lax.fori_loop(0, parts, pass_two, 0)
    rs_dh = reduce_scatter_steps(lambda dev: dh.at[dev], pieces_of(LANES, 8), group("rsd"))
    next(rs_dh)
    grad[pl.ds(0, n_cand), :] = (d_acc[...] * scale).astype(BF)
    tower_pre_grad(n_item, grad, wi2, v["i_slope"], v["i_pre"])
    mine = rows_out.at[me]

    def input_grad(i, _):
        s = pl.ds(pl.multiple_of(i * ROW_BLK, ROW_BLK), ROW_BLK)
        mine[s, :] = dot_nt(v["i_pre"][s, :], wi1[...]).astype(BF)
        return 0

    lax.fori_loop(0, n_item // ROW_BLK, input_grad, 0)
    next(rs_dh)
    ag_rows = all_gather_steps(mine, lambda dev: rows_out.at[dev], pieces_of(n_item, 16), group("agr"))
    next(ag_rows)
    isum, qsum = v["isum"], v["qsum"]
    weight_grads(turn(raw[...]), turn(grad[...]), v["i_pre"], v["i_hid"], isum, parts, 0)
    ars = []
    for sums, out, name in ((isum, isum_out, "ai"), (qsum, qsum_out, "aq")):
        refs = group(name)
        n = len(refs) - 4
        pieces = pieces_of(sums.shape[1], 8)
        first = reduce_scatter_steps(lambda dev, sums=sums: sums.at[dev], pieces, refs[:n])
        second = all_gather_steps(refs[1].at[0], lambda dev, out=out: out.at[dev], pieces, refs[n:])
        ars.append((first, second, refs[1], out))
    ar_i, ag_i, acc_i, _ = ars[0]
    ar_q, ag_q2, acc_q, _ = ars[1]
    next(rs_dh)
    next(ar_i)
    next(ag_rows)
    next(rs_dh)
    next(ar_i)
    next(rs_dh)
    next(ag_rows)
    next(ar_i)
    d_query = ((dz_col * targ_vec.astype(F32) + v["rsd.1"][0].T) * scale).astype(BF)
    q_pre = v["q_pre"]
    q_pre[...] = (v["q_slope"][...] * dot_nt(d_query, w2[...])).astype(BF)
    weight_grads(turn(tok_ref[...]), turn(d_query), q_pre, v["q_hid"], qsum, parts, 0)
    zero = jnp.zeros((8, LANES), F32)
    for dev in range(parts):
        qsum[dev, 64:, :] = zero + loss if dev == 0 else zero
    next(ar_q)
    next(ar_i)
    next(ag_rows)
    next(ar_q)
    next(ar_i)
    isum_out[me] = acc_i[0]
    next(ag_i)
    next(ar_q)
    next(ag_i)
    next(ar_q)
    next(ag_i)
    next(ar_q)
    qsum_out[me] = acc_q[0]
    next(ag_q2)
    next(ag_i)
    for g in (ag_rows, rs_dh, ar_i, ag_i, ar_q, ag_q2):
        for _ in g:
            pass


def step(x, tokens, weights, lq, ids, targ, cid):
    parts, n_item, _ = x.shape
    n_tok = tokens.shape[0]
    n_cand = n_item - n_tok
    ff = weights[0].shape[1]
    spec = []

    def add(name, shape, dtype):
        spec.append((name, pltpu.VMEM(shape, dtype)))

    def add_group(name, items):
        spec.extend((f"{name}.{i}", s) for i, s in enumerate(items))

    add_group("rs", rs_scratch(n_item, BF))
    add_group("agq", ag_scratch())
    add_group("st", [pltpu.VMEM((5, 2, parts, n_tok), F32), pltpu.VMEM((4, 2, parts, n_tok), F32), pltpu.SemaphoreType.DMA((4,)), pltpu.SemaphoreType.DMA((4,))])
    add_group("rsd", rs_scratch(LANES, F32, n_tok))
    add_group("agr", ag_scratch())
    add_group("ai", rs_scratch(64, F32) + ag_scratch())
    add_group("aq", rs_scratch(72, F32) + ag_scratch())
    for n, pre in ((n_tok, "q"), (n_item, "i")):
        add(pre + "_slope", (n, ff), F32)
        add(pre + "_hid", (n, ff), BF)
        add(pre + "_pre", (n, ff), BF)
        add(pre + "_vec", (n, LANES), BF)
        add(pre + "_grad", (n, LANES), BF)
    add("q_all", (parts, n_tok, LANES), BF)
    add("z", (parts, n_cand, n_tok), F32)
    for name in ("top", "den", "norm"):
        add(name, (parts, n_tok), F32)
    add("vec_t", (LANES, n_cand), BF)
    add("d_acc", (n_cand, LANES), F32)
    add("dz", (n_cand, n_tok), BF)
    add("dh", (parts, LANES, n_tok), F32)
    add("isum", (parts, 64, LANES), F32)
    add("qsum", (parts, 72, LANES), F32)
    names = tuple(n for n, _ in spec)
    outs = (jax.ShapeDtypeStruct((parts, n_item, LANES), BF), jax.ShapeDtypeStruct((parts, 64, LANES), F32), jax.ShapeDtypeStruct((parts, 72, LANES), F32))
    return comm_call(functools.partial(step_kernel, (n_cand, n_tok, parts), names), "softmax_step", cid, outs, [s for _, s in spec], x, tokens, *weights, lq, ids, targ)


def solution(mesh):
    num_dev = mesh.shape["dp"]

    def local_step(tokens, w_one, w_two, wi_one, wi_two, table_loc, cand_ids, log_q, targ_loc):
        my_index = lax.axis_index("dp")
        rows_loc, dim = table_loc.shape
        num_tok = tokens.shape[0]
        num_cand = cand_ids.shape[0]
        cand_loc = num_cand // num_dev
        targ_all = ag(targ_loc.reshape(-1, LANES), 1)
        ids = jnp.concatenate([cand_ids.reshape(-1, LANES), targ_all.reshape(-1, LANES)])
        base = (my_index * rows_loc).reshape(1).astype(I32)
        owned, plist, counts = gather(table_loc, ids, base, num_cand, num_dev)
        my_ids = lax.dynamic_slice_in_dim(cand_ids, my_index * cand_loc, cand_loc)
        my_logq = lax.dynamic_slice_in_dim(log_q, my_index * cand_loc, cand_loc)
        wide = (cand_loc, LANES)
        back, isum, qsum = step(owned.reshape(num_dev, cand_loc + num_tok, dim), tokens, (w_one, w_two, wi_one, wi_two), jnp.broadcast_to((my_logq * LOG2E)[:, None], wide), jnp.broadcast_to(my_ids[:, None], wide), targ_all.reshape(num_dev, num_tok), 2)
        d_table = scatter(back.reshape(-1, dim), plist, counts, rows_loc)

        def grads(sums):
            w = sums[:, :64].reshape(2, 4, 2, 64, LANES).transpose(0, 2, 3, 1, 4).reshape(2, LANES, 4 * LANES)
            return w[0], w[1].T

        loss = qsum[0, 64, 0] / (num_tok * num_dev)
        return (loss, d_table) + grads(qsum) + grads(isum)

    return jax.shard_map(local_step, mesh=mesh, in_specs=(P("dp", None), P(), P(), P(), P(), P("dp", None), P(), P(), P("dp")), out_specs=(P(), P("dp", None), P(), P(), P(), P()), check_vma=False)
```

```python
import functools
import math
import jax
import jax.numpy as jnp
from jax import lax
from jax.experimental import pallas as pl
from jax.experimental.pallas import tpu as pltpu
from jax.sharding import PartitionSpec as P

SCORE_GAIN = 3.0
HIT_VALUE = -1e9
LANES = 128
VMEM_CAP = 60 * 1024 * 1024
BF = jnp.bfloat16
F32 = jnp.float32
I32 = jnp.int32
VM = pl.BlockSpec(memory_space=pltpu.VMEM)
SM = pl.BlockSpec(memory_space=pltpu.SMEM)
HB = pl.BlockSpec(memory_space=pl.ANY)
BLK = 256


def compact(loc, num_rows, parts, head):
    nr = loc.shape[0]
    own = jnp.where((loc >= 0) & (loc < num_rows), 1.0, 0.0)
    own16 = own.astype(BF)
    tri = jnp.where(lax.broadcasted_iota(I32, (LANES, LANES), 0) < lax.broadcasted_iota(I32, (LANES, LANES), 1), 1.0, 0.0).astype(BF)
    within = jnp.dot(own16, tri, preferred_element_type=F32)
    low = jnp.where(lax.broadcasted_iota(I32, (nr, nr), 1) < lax.broadcasted_iota(I32, (nr, nr), 0), 1.0, 0.0).astype(BF)
    before = jnp.sum(jnp.dot(low, own16, preferred_element_type=F32), axis=1, keepdims=True)
    lane = lax.broadcasted_iota(I32, (nr, LANES), 1)
    flat = lax.broadcasted_iota(I32, (nr, LANES), 0) * LANES + lane
    disp = flat - (within + before).astype(I32)
    n_head, n_tail = head // parts, (nr * LANES - head) // parts
    late = flat - head
    pos = jnp.where(flat < head, flat + flat // n_head * n_tail, late + (late // n_tail + 1) * n_head)
    val = jnp.where(own > 0, pos * 32768 + loc, -1)
    total = jnp.sum(own).astype(I32)

    def back(x, s):
        if s >= LANES:
            return pltpu.roll(x, nr - s // LANES, axis=0)
        here = pltpu.roll(x, LANES - s, axis=1)
        return jnp.where(lane < LANES - s, here, pltpu.roll(here, nr - 1, axis=0))

    bit = 0
    while (1 << bit) < nr * LANES:
        val_b, disp_b = back(val, 1 << bit), back(disp, 1 << bit)
        take = (val_b >= 0) & (((disp_b >> bit) & 1) == 1)
        stay = ((disp >> bit) & 1) == 0
        val = jnp.where(take, val_b, jnp.where(stay, val, -1))
        disp = jnp.where(take, disp_b, disp)
        bit += 1
    return jnp.where(flat < total, val, nr * LANES * 32768), own, total


def gather_kernel(chunks, cand_ref, targ_ref, table_ref, out_ref, list_ref, cnt_ref, ids_ref, stage, tab, dense, plist, sem, psem):
    rows = tab.shape[0]
    npos = out_ref.shape[0]
    cr = rows // chunks

    def load(c):
        return pltpu.make_async_copy(table_ref.at[pl.ds(c * cr, cr), :], stage.at[pl.ds(c * cr, cr), :], sem.at[c])

    for c in range(chunks):
        load(c).start()
    parts, sub, _ = targ_ref.shape
    n_head = cand_ref.shape[0]
    head = n_head * LANES
    ids_ref[:n_head, :] = cand_ref[...]
    for d in range(parts):
        ids_ref[n_head + d * sub:n_head + (d + 1) * sub, :] = targ_ref[d]
    packed, own, total = compact(ids_ref[...] - lax.axis_index("dp") * rows, rows, parts, head)
    list_ref[...] = packed
    cnt_ref[0] = jnp.sum(own[:head // LANES]).astype(I32)
    cnt_ref[1] = total
    to_smem = pltpu.make_async_copy(list_ref, plist, psem)
    to_smem.start()

    def zero(i, _):
        dense[pl.ds(pl.multiple_of(i * BLK, BLK), BLK), :] = jnp.zeros((BLK, LANES), F32)
        return 0

    lax.fori_loop(0, npos // BLK, zero, 0)
    for c in range(chunks):
        load(c).wait()

        def conv(i, _, c=c):
            s = pl.ds(pl.multiple_of(c * cr + i * BLK, BLK), BLK)
            tab[s, :] = stage[s, :].astype(F32)
            return 0

        lax.fori_loop(0, cr // BLK, conv, 0)
    to_smem.wait()

    def pick(i, _):
        vals = []
        for u in range(LANES):
            w = plist[i, u]
            vals.append((w >> 15, tab[pl.ds(w & 32767, 1), :]))
        for p, v in vals:
            dense[pl.ds(p, 1), :] = v
        return 0

    lax.fori_loop(0, (total + LANES - 1) // LANES, pick, 0)

    def pack(i, _):
        s = pl.ds(pl.multiple_of(i * BLK, BLK), BLK)
        out_ref[s, :] = dense[s, :].astype(BF)
        return 0

    lax.fori_loop(0, npos // BLK, pack, 0)


def gather(table, cand, targ):
    rows = table.shape[0]
    nr = cand.shape[0] + targ.shape[0] * targ.shape[1]
    npos = nr * LANES
    chunks = 8
    return pl.pallas_call(
        functools.partial(gather_kernel, chunks),
        out_shape=(jax.ShapeDtypeStruct((npos, LANES), BF), jax.ShapeDtypeStruct((nr, LANES), I32), jax.ShapeDtypeStruct((2,), I32)),
        in_specs=[VM, VM, HB],
        out_specs=(VM, VM, SM),
        scratch_shapes=[pltpu.VMEM((nr, LANES), I32), pltpu.VMEM((rows, LANES), BF), pltpu.VMEM((rows, LANES), F32), pltpu.VMEM((npos + 8, LANES), F32), pltpu.SMEM((nr, LANES), I32), pltpu.SemaphoreType.DMA((chunks,)), pltpu.SemaphoreType.DMA],
        compiler_params=pltpu.CompilerParams(vmem_limit_bytes=VMEM_CAP),
        name="gather_rows",
    )(cand, targ, table)


ADDS = 4


def scatter_kernel(chunks, cnt_ref, list_ref, grad_ref, *refs):
    n = (len(refs) - 6) // 2
    passed, (out_ref, *kept, acc, grad, plist, sem, psem) = refs[:n], refs[n:]
    rows = out_ref.shape[0]
    npos = grad_ref.shape[0]
    to_smem = pltpu.make_async_copy(list_ref, plist, psem)
    to_smem.start()

    def zero(i, _):
        acc[pl.ds(pl.multiple_of(i * BLK, BLK), BLK), :] = jnp.zeros((BLK, LANES), F32)
        return 0

    lax.fori_loop(0, rows // BLK, zero, 0)

    def conv(i, _):
        s = pl.ds(pl.multiple_of(i * BLK, BLK), BLK)
        grad[s, :] = grad_ref[s, :].astype(F32)
        return 0

    lax.fori_loop(0, npos // BLK, conv, 0)
    grad[npos:, :] = jnp.zeros((8, LANES), F32)
    to_smem.wait()
    nhead = cnt_ref[0]
    total = cnt_ref[1]

    def put(i, _):
        vals = []
        for u in range(LANES):
            w = plist[i, u]
            vals.append((w & 32767, grad[pl.ds(w >> 15, 1), :]))
        for r, v in vals:
            acc[pl.ds(r, 1), :] = v
        return 0

    lax.fori_loop(0, nhead // LANES, put, 0)

    def add_one(i, _):
        w = plist[i >> 7, i & 127]
        r = pl.ds(w & 32767, 1)
        acc[r, :] = acc[r, :] + grad[pl.ds(w >> 15, 1), :]
        return 0

    def add_row(i, _):
        for j in range(0, LANES, ADDS):
            words = [plist[i, j + u] for u in range(ADDS)]
            rs = [w & 32767 for w in words]
            gs = [grad[pl.ds(w >> 15, 1), :] for w in words]
            outs = []
            for u in range(ADDS):
                v = acc[pl.ds(rs[u], 1), :] + gs[u]
                for t in range(u):
                    v = v + jnp.where(rs[t] == rs[u], gs[t], 0.0)
                outs.append(v)
            for u in range(ADDS):
                acc[pl.ds(rs[u], 1), :] = outs[u]
        return 0

    begin = nhead // LANES * LANES
    split = jnp.minimum((nhead + LANES - 1) // LANES * LANES, total)
    lax.fori_loop(begin, split, add_one, 0)
    lax.fori_loop((split + LANES - 1) // LANES, (total + LANES - 1) // LANES, add_row, 0)
    cr = rows // chunks

    def store(c):
        return pltpu.make_async_copy(acc.at[pl.ds(c * cr, cr), :], out_ref.at[pl.ds(c * cr, cr), :], sem.at[c])

    for c in range(chunks):
        store(c).start()
    for src, dst in zip(passed, kept):
        dst[...] = src[...]
    for c in range(chunks):
        store(c).wait()


def scatter(grads, plist, counts, rows, passed):
    nr = plist.shape[0]
    npos = nr * LANES
    chunks = 8
    return pl.pallas_call(
        functools.partial(scatter_kernel, chunks),
        out_shape=(jax.ShapeDtypeStruct((rows, LANES), F32),) + tuple(jax.ShapeDtypeStruct(p.shape, p.dtype) for p in passed),
        in_specs=[SM, HB, VM] + [VM] * len(passed),
        out_specs=(HB,) + (VM,) * len(passed),
        scratch_shapes=[pltpu.VMEM((rows, LANES), F32), pltpu.VMEM((npos + 8, LANES), F32), pltpu.SMEM((nr, LANES), I32), pltpu.SemaphoreType.DMA((chunks,)), pltpu.SemaphoreType.DMA],
        compiler_params=pltpu.CompilerParams(vmem_limit_bytes=VMEM_CAP),
        name="scatter_rows",
    )(counts, plist, grads, *passed)


MESHID = pl.DeviceIdType.MESH
CHIP_DIMS = (1, 2, 4)
SLOTS = tuple(range(8))
CORE_ORDER = (7, 3, 5, 6, 1, 2, 4, 0)
RS_BASE = (0, 4, 6)


def place():
    me = lax.axis_index("dp")
    core = lax.rem(me, 2)
    chip = me // 2
    sign = {d: 1 - 2 * lax.rem(chip // d, 2) for d in CHIP_DIMS}
    return me, core, chip, sign


def chip_at(chip, sign, s):
    for d in CHIP_DIMS:
        if s & d:
            chip = chip + d * sign[d]
    return chip


def enter(extra=()):
    me, core, chip, sign = place()
    barrier = pltpu.get_barrier_semaphore()
    peers = [me + 1 - 2 * core] + [2 * chip_at(chip, sign, d) + core for d in CHIP_DIMS] + list(extra)
    for peer in peers:
        pl.semaphore_signal(barrier, inc=1, device_id=(peer,), device_id_type=MESHID)
    pl.semaphore_wait(barrier, len(peers))


def order_of(k):
    return tuple(CHIP_DIMS[(k + i) % 3] for i in range(3))


def thirds(rows, unit, a=0):
    base = rows // unit
    cuts = [(base * i // 3) * unit for i in range(4)]
    return [(a, cuts[i], cuts[i + 1] - cuts[i], i) for i in range(3)]


def remote(src, dst, send, recv, peer):
    return pltpu.make_async_remote_copy(src_ref=src, dst_ref=dst, send_sem=send, recv_sem=recv, device_id=(peer,), device_id_type=MESHID)


def stage_slots(order, t):
    dims = order_of(order)
    live = [s for s in SLOTS if all(not s & d for d in dims[:t])]
    return [(s, s ^ dims[t]) for s in live if s & dims[t]]


def rs_scratch(arrays, num):
    out = []
    for rows, width, dtype in arrays:
        out += [pltpu.VMEM((8, rows, width), dtype), pltpu.VMEM((8, rows, width), dtype), pltpu.VMEM((7, rows, width), dtype)]
    n = len(arrays)
    dma = pltpu.SemaphoreType.DMA
    return out + [dma((n, 8)), dma((n, 8)), dma((num, 7)), dma((num, 7))]


def reduce_scatter_steps(get, pieces, scratch):
    csend_s, crecv_s, send_s, recv_s = scratch[-4:]
    me, core, chip, sign = place()
    other = me + 1 - 2 * core
    num = len(pieces)
    arrays = range((len(scratch) - 4) // 3)
    crecv, acc, recv = ([scratch[3 * a + i] for a in arrays] for i in range(3))
    started = []

    def core_copy(s, a):
        return remote(get(2 * chip_at(chip, sign, s) + 1 - core, a), crecv[a].at[s], csend_s.at[a, s], crecv_s.at[a, s], other)

    def ici_copy(k, t, i, s):
        a, off, ln, order = pieces[k]
        slot = RS_BASE[t] + i
        peer = 2 * chip_at(chip, sign, order_of(order)[t]) + core
        return remote(acc[a].at[s, pl.ds(off, ln), :], recv[a].at[slot, pl.ds(off, ln), :], send_s.at[k, slot], recv_s.at[k, slot], peer)

    def go(c):
        c.start()
        started.append(c)

    for s in CORE_ORDER:
        for a in arrays:
            go(core_copy(s, a))
    yield
    for s in CORE_ORDER:
        for a in arrays:
            core_copy(s, a).wait_recv()
            acc[a][s] = get(2 * chip_at(chip, sign, s) + core, a)[...] + crecv[a][s]
        for k in range(num):
            for i, (src, dst) in enumerate(stage_slots(pieces[k][3], 0)):
                if src == s:
                    go(ici_copy(k, 0, i, s))
    yield
    for t in range(3):
        for i in reversed(range(4 >> t)):
            for k in range(num):
                a, off, ln, order = pieces[k]
                src, dst = stage_slots(order, t)[i]
                ici_copy(k, t, i, src).wait_recv()
                p = pl.ds(off, ln)
                acc[a][dst, p, :] = acc[a][dst, p, :] + recv[a][RS_BASE[t] + i, p, :]
                if t < 2:
                    for i2, (src2, dst2) in enumerate(stage_slots(order, t + 1)):
                        if src2 == dst:
                            go(ici_copy(k, t + 1, i2, dst))
        yield
    for c in started:
        c.wait_send()


def ag_scratch(num):
    return [pltpu.SemaphoreType.DMA((num, 8))] * 4


def all_gather_steps(own, out, pieces, scratch):
    csend_s, crecv_s, send_s, recv_s = scratch
    me, core, chip, sign = place()
    other = me + 1 - 2 * core
    num = len(pieces)
    started = []

    def ref(k, s, c):
        a, off, ln, _ = pieces[k]
        return out(2 * chip_at(chip, sign, s) + c, a).at[pl.ds(off, ln), :]

    def source(k, s):
        a, off, ln, _ = pieces[k]
        return own(a).at[pl.ds(off, ln), :] if s == 0 else ref(k, s, core)

    def go(c):
        c.start()
        started.append(c)

    def core_send(k, s):
        go(remote(source(k, s), ref(k, s, core), csend_s.at[k, s], crecv_s.at[k, s], other))

    def send(k, t, s):
        d = order_of(pieces[k][3])[t]
        peer = 2 * chip_at(chip, sign, d) + core
        go(remote(source(k, s), ref(k, s, core), send_s.at[k, s ^ d], recv_s.at[k, s ^ d], peer))

    def arrive(k, s):
        there = ref(k, s, core)
        remote(there, there, send_s.at[k, s], recv_s.at[k, s], other).wait_recv()
        core_send(k, s)

    plan = (((), (0, 0)), ((), (1, 0)), ((1,), (1, 1)), ((), (2, 0)), ((), (2, 1)), ((2,), (2, 2)), ((3,), (2, 3)), ((4, 5, 6, 7), None))
    for i, (waits, sends) in enumerate(plan):
        for j in waits or (None,):
            for k in range(num):
                d = order_of(pieces[k][3])

                def slot(bits):
                    return sum(d[b] for b in range(3) if bits >> b & 1)

                if j is not None:
                    arrive(k, slot(j))
                if sends is not None:
                    send(k, sends[0], slot(sends[1]))
                if i == 0:
                    core_send(k, 0)
        yield
    for k in range(num):
        for s in SLOTS:
            there = ref(k, s, 1 - core)
            remote(there, there, csend_s.at[k, s], crecv_s.at[k, s], other).wait_recv()
    for c in started:
        c.wait_send()


def drain(*steps):
    live = list(steps)
    while live:
        live = [g for g in live if next(g, StopIteration) is not StopIteration]


def kernel_call(body, name, cid, out_shape, scratch, *args):
    names = tuple(n for n, _ in scratch)

    def kernel(*refs):
        n = len(args) + len(jax.tree.leaves(out_shape))
        body(*refs[:n], dict(zip(names, refs[n:])))

    return pl.pallas_call(
        kernel,
        out_shape=out_shape,
        in_specs=[VM] * len(args),
        out_specs=jax.tree.map(lambda _: VM, out_shape),
        scratch_shapes=[s for _, s in scratch],
        compiler_params=pltpu.CompilerParams(collective_id=cid, has_side_effects=True, vmem_limit_bytes=VMEM_CAP),
        name=name,
    )(*args)


def grouped(name, items):
    return [(f"{name}.{i}", s) for i, s in enumerate(items)]


def group(scratch, name):
    return [v for k, v in scratch.items() if k.startswith(name + ".")]
LOG2E = 1.4426950408889634
GELU_C = math.sqrt(2.0 / math.pi)
GELU_A = 0.044715
ROW_BLK = 256
COL_BLK = 128


def gelu_both(x):
    x2 = x * x
    t = jnp.tanh(GELU_C * (x + GELU_A * (x2 * x)))
    half = 0.5 * (1.0 + t)
    return x * half, half + (0.5 * GELU_C) * x * (1.0 - t * t) * (1.0 + (3.0 * GELU_A) * x2)


def dot_nn(a, b):
    return jnp.dot(a, b, preferred_element_type=F32)


def dot_nt(a, b):
    return lax.dot_general(a, b, (((1,), (1,)), ((), ())), preferred_element_type=F32)


def turn(x):
    return x.astype(F32).T.astype(BF)


def row_blocks(rows, body):
    def blk(i, _):
        body(pl.ds(pl.multiple_of(i * ROW_BLK, ROW_BLK), ROW_BLK))
        return 0

    lax.fori_loop(0, rows // ROW_BLK, blk, 0)


def tower_into(rows, load, w_in, w_out, slope_ref, hid_ref, out_ref):
    def blk(s):
        act, slope = gelu_both(dot_nn(load(s), w_in[...]))
        slope_ref[s, :] = slope
        hid_ref[s, :] = act.astype(BF)
        out_ref[s, :] = dot_nn(hid_ref[s, :], w_out[...]).astype(BF)

    row_blocks(rows, blk)


def start_kernel(tok_ref, w1, w2, targ_ref, targ_out, q_out, v):
    enter()
    me = lax.axis_index("dp")
    targ_out[me] = targ_ref[...]
    sub = targ_ref.shape[0]
    n_tok = tok_ref.shape[0]
    ag_t = all_gather_steps(lambda a: targ_ref, lambda dev, a: targ_out.at[dev], [(0, 0, sub, 0)], group(v, "agt"))
    next(ag_t)
    next(ag_t)
    tower_into(n_tok, lambda s: tok_ref[s, :], w1, w2, v["slope"], v["hid"], v["vec"])
    q_out[me] = v["vec"][...]
    ag_q = all_gather_steps(lambda a: v["vec"], lambda dev, a: q_out.at[dev], thirds(n_tok, 16), group(v, "agq"))
    drain(ag_t, ag_q)


def start(tokens, w_one, w_two, targ, parts, cid):
    n_tok = tokens.shape[0]
    ff = w_one.shape[1]
    scratch = grouped("agt", ag_scratch(1)) + grouped("agq", ag_scratch(3))
    scratch += [("slope", pltpu.VMEM((n_tok, ff), F32)), ("hid", pltpu.VMEM((n_tok, ff), BF)), ("vec", pltpu.VMEM((n_tok, LANES), BF))]
    outs = (jax.ShapeDtypeStruct((parts,) + targ.shape, I32), jax.ShapeDtypeStruct((parts, n_tok, LANES), BF))
    return kernel_call(start_kernel, "start_step", cid, outs, scratch, tokens, w_one, w_two, targ)


def weight_grads(row_t, grad_t, pre_ref, hid_ref, in_ref, out_ref):
    parts, n_in, _ = in_ref.shape
    n_out = out_ref.shape[1]
    d_in = dot_nn(row_t, pre_ref[...])
    d_out = dot_nn(grad_t, hid_ref[...]).T
    for dev in range(parts):
        in_ref[dev] = d_in[dev * n_in:(dev + 1) * n_in, :]
        out_ref[dev] = d_out[dev * n_out:(dev + 1) * n_out, :]


def step_kernel(x_ref, tok_ref, w1, w2, wi1, wi2, q_all, cand_ref, logq_ref, targ_ref, rows_out, di_in_out, di_out_out, dq_in_out, dq_out_out, loss_out, v):
    parts, n_item, _ = x_ref.shape
    n_tok = tok_ref.shape[0]
    n_cand = n_item - n_tok
    total = float(n_tok * parts)
    scale = SCORE_GAIN / math.sqrt(LANES)
    me, core, chip, sign = place()
    x_chip = 2 * chip_at(chip, sign, 1)
    diag = 2 * chip_at(chip, sign, 6) + core
    rounds = ((me + 1 - 2 * core, x_chip + core, x_chip + 1 - core), (2 * chip_at(chip, sign, 2) + core, 2 * chip_at(chip, sign, 4) + core, diag))
    enter((x_chip + 1 - core, diag))
    rs_rows = reduce_scatter_steps(lambda dev, a: x_ref.at[dev], thirds(n_item, 16), group(v, "rs"))
    next(rs_rows)
    tower_into(n_tok, lambda s: tok_ref[s, :], w1, w2, v["q_slope"], v["q_hid"], v["q_vec"])
    next(rs_rows)
    n_sub = n_cand // LANES
    for r in range(n_sub):
        s = pl.ds(r * LANES, LANES)
        row = pl.ds(me * n_sub + r, 1)
        v["lq"][s, :] = jnp.broadcast_to(logq_ref[row, :] * LOG2E, (LANES, LANES)).T
        v["ids"][s, :] = jnp.broadcast_to(cand_ref[row, :].astype(F32), (LANES, LANES)).T
    drain(rs_rows)
    raw = v["rs.1"].at[0]
    tower_into(n_item, lambda s: raw[s, :], wi1, wi2, v["i_slope"], v["i_hid"], v["i_vec"])
    vec = v["i_vec"]
    z_ref, top_ref, den_ref, own_ref = v["z"], v["top"], v["den"], v["own"]
    own = pl.ds(me, 1)
    targ_vec = vec[pl.ds(n_cand, n_tok), :]
    q_own = v["q_vec"][...]
    eye = lax.broadcasted_iota(I32, (n_tok, n_tok), 0) == lax.broadcasted_iota(I32, (n_tok, n_tok), 1)
    z_own = jnp.sum(jnp.where(eye, dot_nt(targ_vec, q_own), 0.0), axis=0, keepdims=True) * (scale * LOG2E)
    own_ref[...] = jnp.full(own_ref.shape, -jnp.inf, F32)
    own_ref[own, :] = z_own

    def pass_one(t, _):
        q_t = q_all[t]
        targ = jnp.concatenate([targ_ref[t, pl.ds(i, 1), :] for i in range(n_tok // LANES)], axis=1).astype(F32)
        z_t = own_ref[pl.ds(t, 1), :]
        top8 = jnp.broadcast_to(z_t, (8, n_tok))
        for j in range(n_cand // COL_BLK):
            s = pl.ds(j * COL_BLK, COL_BLK)
            lq = jnp.concatenate([v["lq"][s, :]] * (n_tok // LANES), axis=1)
            ids = jnp.concatenate([v["ids"][s, :]] * (n_tok // LANES), axis=1)
            z = dot_nt(vec[s, :], q_t) * (scale * LOG2E) - lq
            z = jnp.where(ids == targ, HIT_VALUE * LOG2E, z)
            z_ref[t, s, :] = z
            top8 = jnp.maximum(top8, jnp.max(z.reshape(COL_BLK // 8, 8, n_tok), axis=0))
        top = jnp.max(top8, axis=0, keepdims=True)
        den8 = jnp.zeros((8, n_tok), F32)
        for j in range(n_cand // COL_BLK):
            e = jnp.exp2(z_ref[t, pl.ds(j * COL_BLK, COL_BLK), :] - top)
            den8 = den8 + jnp.sum(e.reshape(COL_BLK // 8, 8, n_tok), axis=0)
        top_ref[pl.ds(t, 1), :] = top
        den_ref[pl.ds(t, 1), :] = jnp.sum(den8, axis=0, keepdims=True) + jnp.exp2(z_t - top)
        return 0

    lax.fori_loop(0, parts, pass_one, 0)
    held, got, st_send, st_recv = group(v, "st")
    held[0, 0] = top_ref[...]
    held[0, 1] = den_ref[...]
    for r, peers in enumerate(rounds):
        copies = [remote(held.at[r], got.at[r, i], st_send.at[r, i], st_recv.at[r, i], peer) for i, peer in enumerate(peers)]
        for c in copies:
            c.start()
        for c in copies:
            c.wait()
        tops = [held[r, 0]] + [got[r, i, 0] for i in range(3)]
        dens = [held[r, 1]] + [got[r, i, 1] for i in range(3)]
        top = jnp.maximum(jnp.maximum(tops[0], tops[1]), jnp.maximum(tops[2], tops[3]))
        held[r + 1, 0] = top
        held[r + 1, 1] = sum(d * jnp.exp2(m - top) for m, d in zip(tops, dens))
    norm = v["norm"]
    norm[...] = held[2, 0] + jnp.log2(held[2, 1] * total)
    top_ref[...] = held[2, 0]
    den_ref[...] = held[2, 1]
    lse = top_ref[own, :] + jnp.log2(den_ref[own, :])
    loss = jnp.sum(lse - z_own, axis=1, keepdims=True) * (1.0 / (LOG2E * total))
    dz_row = ((jnp.exp2(z_own - top_ref[own, :]) / den_ref[own, :] - 1.0) * (1.0 / total)).astype(BF).astype(F32)
    dz_col = jnp.sum(jnp.where(eye, dz_row, 0.0), axis=1, keepdims=True)
    grad = v["i_grad"]
    grad[pl.ds(n_cand, n_tok), :] = (scale * dz_col * q_own.astype(F32)).astype(BF)
    vec_t = v["vec_t"]
    vec_t[...] = turn(vec[:n_cand, :])
    d_acc, dz_s, dh = v["d_acc"], v["dz"], v["dh"]
    d_acc[...] = jnp.zeros_like(d_acc)

    def pass_two(t, _):
        shift = norm[pl.ds(t, 1), :]
        for j in range(n_cand // COL_BLK):
            s = pl.ds(j * COL_BLK, COL_BLK)
            dz_s[s, :] = jnp.exp2(z_ref[t, s, :] - shift).astype(BF)
        d_acc[...] += dot_nn(dz_s[...], q_all[t])
        dh[t] = dot_nn(vec_t[...], dz_s[...])
        return 0

    lax.fori_loop(0, parts, pass_two, 0)
    rs_dh = reduce_scatter_steps(lambda dev, a: dh.at[dev], thirds(LANES, 8), group(v, "rsd"))
    next(rs_dh)
    grad[pl.ds(0, n_cand), :] = (d_acc[...] * scale).astype(BF)
    i_pre, i_slope = v["i_pre"], v["i_slope"]

    def pre_grad(s):
        i_pre[s, :] = (i_slope[s, :] * dot_nt(grad[s, :], wi2[...])).astype(BF)

    row_blocks(n_item, pre_grad)
    next(rs_dh)
    mine = rows_out.at[me]

    def input_grad(s):
        mine[s, :] = dot_nt(i_pre[s, :], wi1[...]).astype(BF)

    row_blocks(n_item, input_grad)
    next(rs_dh)
    ag_rows = all_gather_steps(lambda a: mine, lambda dev, a: rows_out.at[dev], thirds(n_item, 16), group(v, "agr"))
    next(ag_rows)
    weight_grads(turn(raw[...]), turn(grad[...]), i_pre, v["i_hid"], v["di_in"], v["di_out"])
    next(rs_dh)
    next(ag_rows)

    def sum_all(name, parts_in, orders, outs):
        pieces = [(a, 0, r.shape[1], o) for a, (r, o) in enumerate(zip(parts_in, orders))]
        refs = group(v, name)
        sums = [refs[3 * a + 1].at[0] for a in range(len(parts_in))]
        first = reduce_scatter_steps(lambda dev, a: parts_in[a].at[dev], pieces, refs[:-4])
        yield from (x for _, x in zip(range(5), first))
        for a, out in enumerate(outs):
            out[me] = sums[a][...]
        yield from all_gather_steps(lambda a: sums[a], lambda dev, a: outs[a].at[dev], pieces, refs[-4:])
        for _ in first:
            pass

    ar_i = sum_all("ai", (v["di_in"], v["di_out"]), (0, 1), (di_in_out, di_out_out))
    next(ar_i)
    next(rs_dh)
    d_query = ((dz_col * targ_vec.astype(F32) + v["rsd.1"][0].T) * scale).astype(BF)
    q_pre = v["q_pre"]
    q_pre[...] = (v["q_slope"][...] * dot_nt(d_query, w2[...])).astype(BF)
    weight_grads(turn(tok_ref[...]), turn(d_query), q_pre, v["q_hid"], v["dq_in"], v["dq_out"])
    loss_part = v["loss"]
    loss_part[...] = jnp.zeros_like(loss_part)
    loss_part[0] = jnp.broadcast_to(loss, loss_part.shape[1:])
    ar_q = sum_all("aq", (v["dq_in"], v["dq_out"], loss_part), (1, 2, 0), (dq_in_out, dq_out_out, loss_out))
    drain(ar_q, ar_i, ag_rows, rs_dh)


def step(x, tokens, weights, q_all, cand, logq, targ, cid):
    parts, n_item, _ = x.shape
    n_tok = tokens.shape[0]
    n_cand = n_item - n_tok
    ff = weights[0].shape[1]
    dma = pltpu.SemaphoreType.DMA
    n_in, n_out = LANES // parts, ff // parts
    w_parts = [(n_in, ff, F32), (n_out, LANES, F32)]
    spec = grouped("rs", rs_scratch([(n_item, LANES, BF)], 3))
    spec += grouped("st", [pltpu.VMEM((3, 2, parts, n_tok), F32), pltpu.VMEM((2, 3, 2, parts, n_tok), F32), dma((2, 3)), dma((2, 3))])
    spec += grouped("rsd", rs_scratch([(LANES, n_tok, F32)], 3))
    spec += grouped("agr", ag_scratch(3))
    spec += grouped("ai", rs_scratch(w_parts, 2) + ag_scratch(2))
    spec += grouped("aq", rs_scratch(w_parts + [(8, LANES, F32)], 3) + ag_scratch(3))

    def add(name, shape, dtype=F32):
        spec.append((name, pltpu.VMEM(shape, dtype)))

    for n, pre in ((n_tok, "q"), (n_item, "i")):
        add(pre + "_slope", (n, ff))
        add(pre + "_hid", (n, ff), BF)
        add(pre + "_pre", (n, ff), BF)
        add(pre + "_vec", (n, LANES), BF)
        add("d" + pre + "_in", (parts, n_in, ff))
        add("d" + pre + "_out", (parts, n_out, LANES))
    add("i_grad", (n_item, LANES), BF)
    add("loss", (parts, 8, LANES))
    for name in ("lq", "ids", "d_acc"):
        add(name, (n_cand, LANES))
    add("z", (parts, n_cand, n_tok))
    for name in ("top", "den", "norm", "own"):
        add(name, (parts, n_tok))
    add("vec_t", (LANES, n_cand), BF)
    add("dz", (n_cand, n_tok), BF)
    add("dh", (parts, LANES, n_tok))
    sums = (jax.ShapeDtypeStruct((parts, n_in, ff), F32), jax.ShapeDtypeStruct((parts, n_out, LANES), F32))
    outs = (jax.ShapeDtypeStruct((parts, n_item, LANES), BF),) + sums + sums + (jax.ShapeDtypeStruct((parts, 8, LANES), F32),)
    return kernel_call(step_kernel, "softmax_step", cid, outs, spec, x, tokens, *weights, q_all, cand, logq, targ)


def solution(mesh):
    num_dev = mesh.shape["dp"]

    def local_step(tokens, w_one, w_two, wi_one, wi_two, table_loc, cand_ids, log_q, targ_loc):
        rows_loc, dim = table_loc.shape
        n_item = cand_ids.shape[0] // num_dev + tokens.shape[0]
        cand = cand_ids.reshape(-1, LANES)
        targ, q_all = start(tokens, w_one, w_two, targ_loc.reshape(-1, LANES), num_dev, 1)
        owned, plist, counts = gather(table_loc, cand, targ)
        back, *sums = step(owned.reshape(num_dev, n_item, dim), tokens, (w_one, w_two, wi_one, wi_two), q_all, cand, log_q.reshape(-1, LANES), targ, 2)
        d_table, di_in, di_out, dq_in, dq_out, loss = scatter(back.reshape(-1, dim), plist, counts, rows_loc, sums)
        shaped = [g.reshape(w.shape) for g, w in zip((dq_in, dq_out, di_in, di_out), (w_one, w_two, wi_one, wi_two))]
        return (loss[0, 0, 0], d_table) + tuple(shaped)

    return jax.shard_map(local_step, mesh=mesh, in_specs=(P("dp", None), P(), P(), P(), P(), P("dp", None), P(), P(), P("dp")), out_specs=(P(), P("dp", None), P(), P(), P(), P()), check_vma=False)
```

```python
import functools
import math
import jax
import jax.numpy as jnp
from jax import lax
from jax.experimental import pallas as pl
from jax.experimental.pallas import tpu as pltpu
from jax.sharding import PartitionSpec as P

SCORE_GAIN = 3.0
HIT_VALUE = -1e9
LANES = 128
VMEM_CAP = 60 * 1024 * 1024
BF = jnp.bfloat16
F32 = jnp.float32
I32 = jnp.int32
VM = pl.BlockSpec(memory_space=pltpu.VMEM)
SM = pl.BlockSpec(memory_space=pltpu.SMEM)
HB = pl.BlockSpec(memory_space=pl.ANY)
BLK = 256


def compact(loc, num_rows, parts, head):
    nr = loc.shape[0]
    own = jnp.where((loc >= 0) & (loc < num_rows), 1.0, 0.0)
    own16 = own.astype(BF)
    tri = jnp.where(lax.broadcasted_iota(I32, (LANES, LANES), 0) < lax.broadcasted_iota(I32, (LANES, LANES), 1), 1.0, 0.0).astype(BF)
    within = jnp.dot(own16, tri, preferred_element_type=F32)
    low = jnp.where(lax.broadcasted_iota(I32, (nr, nr), 1) < lax.broadcasted_iota(I32, (nr, nr), 0), 1.0, 0.0).astype(BF)
    before = jnp.sum(jnp.dot(low, own16, preferred_element_type=F32), axis=1, keepdims=True)
    lane = lax.broadcasted_iota(I32, (nr, LANES), 1)
    flat = lax.broadcasted_iota(I32, (nr, LANES), 0) * LANES + lane
    disp = flat - (within + before).astype(I32)
    n_head, n_tail = head // parts, (nr * LANES - head) // parts
    late = flat - head
    pos = jnp.where(flat < head, flat + flat // n_head * n_tail, late + (late // n_tail + 1) * n_head)
    val = jnp.where(own > 0, pos * 32768 + loc, -1)
    total = jnp.sum(own).astype(I32)

    def back(x, s):
        if s >= LANES:
            return pltpu.roll(x, nr - s // LANES, axis=0)
        here = pltpu.roll(x, LANES - s, axis=1)
        return jnp.where(lane < LANES - s, here, pltpu.roll(here, nr - 1, axis=0))

    bit = 0
    while (1 << bit) < nr * LANES:
        val_b, disp_b = back(val, 1 << bit), back(disp, 1 << bit)
        take = (val_b >= 0) & (((disp_b >> bit) & 1) == 1)
        stay = ((disp >> bit) & 1) == 0
        val = jnp.where(take, val_b, jnp.where(stay, val, -1))
        disp = jnp.where(take, disp_b, disp)
        bit += 1
    return jnp.where(flat < total, val, nr * LANES * 32768), own, total


def gather_kernel(chunks, cand_ref, targ_ref, table_ref, out_ref, list_ref, cnt_ref, ids_ref, stage, tab, dense, plist, packed_rows, sem, psem, osem):
    rows = tab.shape[0]
    npos = out_ref.shape[0]
    cr = rows // chunks

    def load(c):
        return pltpu.make_async_copy(table_ref.at[pl.ds(c * cr, cr), :], stage.at[pl.ds(c * cr, cr), :], sem.at[c])

    for c in range(chunks):
        load(c).start()
    parts, sub, _ = targ_ref.shape
    n_head = cand_ref.shape[0]
    head = n_head * LANES
    ids_ref[:n_head, :] = cand_ref[...]
    for d in range(parts):
        ids_ref[n_head + d * sub:n_head + (d + 1) * sub, :] = targ_ref[d]
    packed, own, total = compact(ids_ref[...] - lax.axis_index("dp") * rows, rows, parts, head)
    list_ref[...] = packed
    cnt_ref[0] = jnp.sum(own[:head // LANES]).astype(I32)
    cnt_ref[1] = total
    to_smem = pltpu.make_async_copy(list_ref, plist, psem)
    to_smem.start()

    def zero(i, _):
        dense[pl.ds(pl.multiple_of(i * BLK, BLK), BLK), :] = jnp.zeros((BLK, LANES), F32)
        return 0

    lax.fori_loop(0, npos // BLK, zero, 0)
    for c in range(chunks):
        load(c).wait()

        def conv(i, _, c=c):
            s = pl.ds(pl.multiple_of(c * cr + i * BLK, BLK), BLK)
            tab[s, :] = stage[s, :].astype(F32)
            return 0

        lax.fori_loop(0, cr // BLK, conv, 0)
    to_smem.wait()

    def pick(i, _):
        vals = []
        for u in range(LANES):
            w = plist[i, u]
            vals.append((w >> 15, tab[pl.ds(w & 32767, 1), :]))
        for p, v in vals:
            dense[pl.ds(p, 1), :] = v
        return 0

    lax.fori_loop(0, (total + LANES - 1) // LANES, pick, 0)

    part = npos // parts

    def leave(d):
        s = pl.ds(d * part, part)
        return pltpu.make_async_copy(packed_rows.at[s, :], out_ref.at[s, :], osem.at[d])

    for d in range(parts):
        packed_rows[pl.ds(d * part, part), :] = dense[pl.ds(d * part, part), :].astype(BF)
        leave(d).start()
    for d in range(parts):
        leave(d).wait()


def gather(table, cand, targ):
    rows = table.shape[0]
    nr = cand.shape[0] + targ.shape[0] * targ.shape[1]
    npos = nr * LANES
    chunks = 8
    return pl.pallas_call(
        functools.partial(gather_kernel, chunks),
        out_shape=(jax.ShapeDtypeStruct((npos, LANES), BF), jax.ShapeDtypeStruct((nr, LANES), I32), jax.ShapeDtypeStruct((2,), I32)),
        in_specs=[VM, VM, HB],
        out_specs=(HB, VM, SM),
        scratch_shapes=[pltpu.VMEM((nr, LANES), I32), pltpu.VMEM((rows, LANES), BF), pltpu.VMEM((rows, LANES), F32), pltpu.VMEM((npos + 8, LANES), F32), pltpu.SMEM((nr, LANES), I32), pltpu.VMEM((npos, LANES), BF), pltpu.SemaphoreType.DMA((chunks,)), pltpu.SemaphoreType.DMA, pltpu.SemaphoreType.DMA((targ.shape[0],))],
        compiler_params=pltpu.CompilerParams(vmem_limit_bytes=VMEM_CAP),
        name="gather_rows",
    )(cand, targ, table)


ADDS = 4


def scatter_kernel(chunks, cnt_ref, list_ref, grad_ref, *refs):
    n = (len(refs) - 10) // 3
    passed, (out_ref, *refs) = refs[:n], refs[n:]
    kept, held, (acc, raw, grad, plist, sem, psem, gsem, isem, osem) = refs[:n], refs[n:2 * n], refs[2 * n:]
    parts = gsem.shape[0]
    part = grad_ref.shape[0] // parts

    def arrive(d):
        s = pl.ds(d * part, part)
        return pltpu.make_async_copy(grad_ref.at[s, :], raw.at[s, :], gsem.at[d])

    for d in range(parts):
        arrive(d).start()
    ins = [pltpu.make_async_copy(src, dst, isem.at[i]) for i, (src, dst) in enumerate(zip(passed, held))]
    outs = [pltpu.make_async_copy(src, dst, osem.at[i]) for i, (src, dst) in enumerate(zip(held, kept))]
    for c in ins:
        c.start()
    rows = out_ref.shape[0]
    npos = grad_ref.shape[0]
    to_smem = pltpu.make_async_copy(list_ref, plist, psem)
    to_smem.start()

    def zero(i, _):
        acc[pl.ds(pl.multiple_of(i * BLK, BLK), BLK), :] = jnp.zeros((BLK, LANES), F32)
        return 0

    lax.fori_loop(0, rows // BLK, zero, 0)

    for d in range(parts):
        arrive(d).wait()
        s = pl.ds(d * part, part)
        grad[s, :] = raw[s, :].astype(F32)
    for i, o in zip(ins, outs):
        i.wait()
        o.start()
    grad[npos:, :] = jnp.zeros((8, LANES), F32)
    to_smem.wait()
    nhead = cnt_ref[0]
    total = cnt_ref[1]

    def put(i, _):
        vals = []
        for u in range(LANES):
            w = plist[i, u]
            vals.append((w & 32767, grad[pl.ds(w >> 15, 1), :]))
        for r, v in vals:
            acc[pl.ds(r, 1), :] = v
        return 0

    lax.fori_loop(0, nhead // LANES, put, 0)

    def add_one(i, _):
        w = plist[i >> 7, i & 127]
        r = pl.ds(w & 32767, 1)
        acc[r, :] = acc[r, :] + grad[pl.ds(w >> 15, 1), :]
        return 0

    def add_row(i, _):
        for j in range(0, LANES, ADDS):
            words = [plist[i, j + u] for u in range(ADDS)]
            rs = [w & 32767 for w in words]
            gs = [grad[pl.ds(w >> 15, 1), :] for w in words]
            outs = []
            for u in range(ADDS):
                v = acc[pl.ds(rs[u], 1), :] + gs[u]
                for t in range(u):
                    v = v + jnp.where(rs[t] == rs[u], gs[t], 0.0)
                outs.append(v)
            for u in range(ADDS):
                acc[pl.ds(rs[u], 1), :] = outs[u]
        return 0

    begin = nhead // LANES * LANES
    split = jnp.minimum((nhead + LANES - 1) // LANES * LANES, total)
    lax.fori_loop(begin, split, add_one, 0)
    lax.fori_loop((split + LANES - 1) // LANES, (total + LANES - 1) // LANES, add_row, 0)
    cr = rows // chunks

    def store(c):
        return pltpu.make_async_copy(acc.at[pl.ds(c * cr, cr), :], out_ref.at[pl.ds(c * cr, cr), :], sem.at[c])

    for c in range(chunks):
        store(c).start()
    for c in range(chunks):
        store(c).wait()
    for o in outs:
        o.wait()


def scatter(grads, plist, counts, rows, passed, parts):
    nr = plist.shape[0]
    npos = nr * LANES
    chunks = 8
    n = len(passed)
    dma = pltpu.SemaphoreType.DMA
    return pl.pallas_call(
        functools.partial(scatter_kernel, chunks),
        out_shape=(jax.ShapeDtypeStruct((rows, LANES), F32),) + tuple(jax.ShapeDtypeStruct(p.shape, p.dtype) for p in passed),
        in_specs=[SM, HB, HB] + [HB] * n,
        out_specs=(HB,) * (n + 1),
        scratch_shapes=[pltpu.VMEM(p.shape, p.dtype) for p in passed]
        + [pltpu.VMEM((rows, LANES), F32), pltpu.VMEM((npos, LANES), BF), pltpu.VMEM((npos + 8, LANES), F32), pltpu.SMEM((nr, LANES), I32), dma((chunks,)), dma, dma((parts,)), dma((n,)), dma((n,))],
        compiler_params=pltpu.CompilerParams(vmem_limit_bytes=VMEM_CAP),
        name="scatter_rows",
    )(counts, plist, grads, *passed)


MESHID = pl.DeviceIdType.MESH
CHIP_DIMS = (1, 2, 4)
SLOTS = tuple(range(8))
CORE_ORDER = (7, 3, 5, 6, 1, 2, 4, 0)
RS_BASE = (0, 4, 6)


def place():
    me = lax.axis_index("dp")
    core = lax.rem(me, 2)
    chip = me // 2
    sign = {d: 1 - 2 * lax.rem(chip // d, 2) for d in CHIP_DIMS}
    return me, core, chip, sign


def chip_at(chip, sign, s):
    for d in CHIP_DIMS:
        if s & d:
            chip = chip + d * sign[d]
    return chip


def enter(peers):
    barrier = pltpu.get_barrier_semaphore()
    for peer in peers:
        pl.semaphore_signal(barrier, inc=1, device_id=(peer,), device_id_type=MESHID)
    pl.semaphore_wait(barrier, len(peers))


def order_of(k):
    return tuple(CHIP_DIMS[(k + i) % 3] for i in range(3))


def thirds(rows, unit, a=0):
    base = rows // unit
    cuts = [(base * i // 3) * unit for i in range(4)]
    return [(a, cuts[i], cuts[i + 1] - cuts[i], i) for i in range(3)]


def remote(src, dst, send, recv, peer):
    return pltpu.make_async_remote_copy(src_ref=src, dst_ref=dst, send_sem=send, recv_sem=recv, device_id=(peer,), device_id_type=MESHID)


def stage_slots(order, t):
    dims = order_of(order)
    live = [s for s in SLOTS if all(not s & d for d in dims[:t])]
    return [(s, s ^ dims[t]) for s in live if s & dims[t]]


def rs_scratch(arrays, num):
    out = []
    for rows, width, dtype in arrays:
        out += [pltpu.VMEM((8, rows, width), dtype), pltpu.VMEM((8, rows, width), dtype), pltpu.VMEM((7, rows, width), dtype)]
    n = len(arrays)
    dma = pltpu.SemaphoreType.DMA
    return out + [dma((n, 8)), dma((n, 8)), dma((num, 7)), dma((num, 7))]


def reduce_scatter_steps(get, pieces, scratch, mine=None, produce=None):
    csend_s, crecv_s, send_s, recv_s = scratch[-4:]
    me, core, chip, sign = place()
    other = me + 1 - 2 * core
    num = len(pieces)
    arrays = range((len(scratch) - 4) // 3)
    crecv, acc, recv = ([scratch[3 * a + i] for a in arrays] for i in range(3))
    started = []

    def core_copy(s, a):
        return remote(get(2 * chip_at(chip, sign, s) + 1 - core, a), crecv[a].at[s], csend_s.at[a, s], crecv_s.at[a, s], other)

    def ici_copy(k, t, i, s):
        a, off, ln, order = pieces[k]
        slot = RS_BASE[t] + i
        peer = 2 * chip_at(chip, sign, order_of(order)[t]) + core
        return remote(acc[a].at[s, pl.ds(off, ln), :], recv[a].at[slot, pl.ds(off, ln), :], send_s.at[k, slot], recv_s.at[k, slot], peer)

    def go(c):
        c.start()
        started.append(c)

    def absorb(s):
        for a in arrays:
            core_copy(s, a).wait_recv()
            part = mine(s, a) if mine else get(2 * chip_at(chip, sign, s) + core, a)[...]
            acc[a][s] = part + crecv[a][s]
        for k in range(num):
            for i, (src, dst) in enumerate(stage_slots(pieces[k][3], 0)):
                if src == s:
                    go(ici_copy(k, 0, i, s))

    for n, s in enumerate(CORE_ORDER):
        if produce:
            produce(s)
        for a in arrays:
            go(core_copy(s, a))
        if produce and n:
            absorb(CORE_ORDER[n - 1])
    yield
    for s in CORE_ORDER[-1:] if produce else CORE_ORDER:
        absorb(s)
    yield
    for t in range(3):
        for i in reversed(range(4 >> t)):
            for k in range(num):
                a, off, ln, order = pieces[k]
                src, dst = stage_slots(order, t)[i]
                ici_copy(k, t, i, src).wait_recv()
                p = pl.ds(off, ln)
                acc[a][dst, p, :] = acc[a][dst, p, :] + recv[a][RS_BASE[t] + i, p, :]
                if t < 2:
                    for i2, (src2, dst2) in enumerate(stage_slots(order, t + 1)):
                        if src2 == dst:
                            go(ici_copy(k, t + 1, i2, dst))
        yield
    for c in started:
        c.wait_send()


def ag_scratch(num):
    return [pltpu.SemaphoreType.DMA((num, 8))] * 4


def all_gather_steps(own, out, pieces, scratch, landed=None):
    csend_s, crecv_s, send_s, recv_s = scratch
    me, core, chip, sign = place()
    other = me + 1 - 2 * core
    num = len(pieces)
    started = []

    def ref(k, s, c):
        a, off, ln, _ = pieces[k]
        return out(2 * chip_at(chip, sign, s) + c, a).at[pl.ds(off, ln), :]

    def source(k, s):
        a, off, ln, _ = pieces[k]
        return own(a).at[pl.ds(off, ln), :] if s == 0 else ref(k, s, core)

    def go(c):
        c.start()
        started.append(c)

    def core_send(k, s):
        go(remote(source(k, s), ref(k, s, core), csend_s.at[k, s], crecv_s.at[k, s], other))

    def send(k, t, s):
        d = order_of(pieces[k][3])[t]
        peer = 2 * chip_at(chip, sign, d) + core
        go(remote(source(k, s), ref(k, s, core), send_s.at[k, s ^ d], recv_s.at[k, s ^ d], peer))

    def arrive(k, s):
        there = ref(k, s, core)
        remote(there, there, send_s.at[k, s], recv_s.at[k, s], other).wait_recv()
        core_send(k, s)
        if landed:
            landed(k, s, 0)

    plan = (((), (0, 0)), ((), (1, 0)), ((1,), (1, 1)), ((), (2, 0)), ((), (2, 1)), ((2,), (2, 2)), ((3,), (2, 3)), ((4, 5, 6, 7), None))
    for i, (waits, sends) in enumerate(plan):
        for j in waits or (None,):
            for k in range(num):
                d = order_of(pieces[k][3])

                def slot(bits):
                    return sum(d[b] for b in range(3) if bits >> b & 1)

                if j is not None:
                    arrive(k, slot(j))
                if sends is not None:
                    send(k, sends[0], slot(sends[1]))
                if i == 0:
                    core_send(k, 0)
        yield
    for k in range(num):
        for s in SLOTS:
            there = ref(k, s, 1 - core)
            remote(there, there, csend_s.at[k, s], crecv_s.at[k, s], other).wait_recv()
            if landed:
                landed(k, s, 1)
    for c in started:
        c.wait_send()


def direct_scratch(rows, width):
    dma = pltpu.SemaphoreType.DMA
    return [pltpu.VMEM((8, rows, width), F32)] * 3 + [pltpu.VMEM((rows, width), F32), dma, dma, dma((8,)), dma((8,)), dma((8,)), dma((8,)), dma((8,)), dma((8,))]


def sum_direct_steps(src, out, scratch):
    crecv, acc, recv, tot, cs, cr, s1, r1, s2, r2, s3, r3 = scratch
    me, core, chip, sign = place()
    other = me + 1 - 2 * core
    first = remote(src.at[1 - core], crecv, cs, cr, other)
    first.start()
    yield
    first.wait_recv()
    acc[...] = src[core] + crecv[...]
    far = (7, 3, 5, 6, 1, 2, 4)

    def to(s):
        return 2 * chip_at(chip, sign, s) + core

    sends = [remote(acc.at[chip_at(chip, sign, s)], recv.at[s], s1.at[s], r1.at[s], to(s)) for s in far]
    for c in sends:
        c.start()
    yield
    for c in sends:
        c.wait_recv()
    total = acc[chip]
    for s in far:
        total = total + recv[s]
    tot[...] = total
    backs = [remote(tot, out.at[me], s2.at[s], r2.at[s], to(s)) for s in far]
    for c in backs:
        c.start()
    pair = [remote(tot, out.at[me], s3.at[0], r3.at[0], other)]
    pair[0].start()
    out[me] = total
    yield
    for s in reversed(far):
        there = out.at[to(s)]
        remote(there, there, s2.at[s], r2.at[s], other).wait_recv()
        c = remote(there, there, s3.at[s], r3.at[s], other)
        c.start()
        pair.append(c)
    yield
    for s in SLOTS:
        there = out.at[2 * chip_at(chip, sign, s) + 1 - core]
        remote(there, there, s3.at[s], r3.at[s], other).wait_recv()
    for c in [first] + sends + backs + pair:
        c.wait_send()


def drain(*steps):
    live = list(steps)
    while live:
        live = [g for g in live if next(g, StopIteration) is not StopIteration]


def kernel_call(body, name, cid, out_shape, scratch, *args, in_hbm=(), out_hbm=()):
    names = tuple(n for n, _ in scratch)

    def kernel(*refs):
        n = len(args) + len(jax.tree.leaves(out_shape))
        body(*refs[:n], dict(zip(names, refs[n:])))

    return pl.pallas_call(
        kernel,
        out_shape=out_shape,
        in_specs=[HB if i in in_hbm else VM for i in range(len(args))],
        out_specs=tuple(HB if i in out_hbm else VM for i in range(len(out_shape))),
        scratch_shapes=[s for _, s in scratch],
        compiler_params=pltpu.CompilerParams(collective_id=cid, has_side_effects=True, vmem_limit_bytes=VMEM_CAP),
        name=name,
    )(*args)


def grouped(name, items):
    return [(f"{name}.{i}", s) for i, s in enumerate(items)]


def group(scratch, name):
    return [v for k, v in scratch.items() if k.startswith(name + ".")]
LOG2E = 1.4426950408889634
GELU_C = math.sqrt(2.0 / math.pi)
GELU_A = 0.044715
ROW_BLK = 256
COL_BLK = 128


def gelu_both(x):
    x2 = x * x
    t = jnp.tanh(GELU_C * (x + GELU_A * (x2 * x)))
    half = 0.5 * (1.0 + t)
    return x * half, half + (0.5 * GELU_C) * x * (1.0 - t * t) * (1.0 + (3.0 * GELU_A) * x2)


def dot_nn(a, b):
    return jnp.dot(a, b, preferred_element_type=F32)


def dot_nt(a, b):
    return lax.dot_general(a, b, (((1,), (1,)), ((), ())), preferred_element_type=F32)


def turn(x):
    return x.astype(F32).T.astype(BF)


def row_blocks(rows, body):
    def blk(i, _):
        body(pl.ds(pl.multiple_of(i * ROW_BLK, ROW_BLK), ROW_BLK))
        return 0

    lax.fori_loop(0, rows // ROW_BLK, blk, 0)


def tower_into(rows, load, w_in, w_out, slope_ref, hid_ref, out_ref):
    def blk(s):
        act, slope = gelu_both(dot_nn(load(s), w_in[...]))
        slope_ref[s, :] = slope
        hid_ref[s, :] = act.astype(BF)
        out_ref[s, :] = dot_nn(hid_ref[s, :], w_out[...]).astype(BF)

    row_blocks(rows, blk)


def start_kernel(targ_ref, targ_out, v):
    me, core, chip, sign = place()
    peers = [2 * chip_at(chip, sign, s) + c for s in reversed(SLOTS) for c in ((core, 1 - core) if s else (1 - core,))]
    enter(peers)
    send_s, recv_s = v["sems.0"], v["sems.1"]
    targ_out[me] = targ_ref[...]
    copies = [remote(targ_ref, targ_out.at[me], send_s.at[i], recv_s.at[i], peer) for i, peer in enumerate(peers)]
    for c in copies:
        c.start()
    for c in copies:
        c.wait()


def start(targ, parts, cid):
    dma = pltpu.SemaphoreType.DMA
    outs = (jax.ShapeDtypeStruct((parts,) + targ.shape, I32),)
    return kernel_call(start_kernel, "start_step", cid, outs, grouped("sems", [dma((parts - 1,)), dma((parts - 1,))]), targ)[0]


def packed_grads(row_t, grad_t, pre_ref, hid_ref, loss, sums_ref):
    d_in = dot_nn(row_t, pre_ref[...])
    d_out = dot_nn(grad_t, hid_ref[...]).T
    parts = 2 * sums_ref.shape[1]
    n_in, n_out = d_in.shape[0] // parts, d_out.shape[0] // parts
    wide = d_in.shape[1] // LANES
    for dev in range(parts):
        part = sums_ref.at[dev % 2, dev // 2]
        for c in range(wide):
            part[c * n_in:(c + 1) * n_in, :] = d_in[dev * n_in:(dev + 1) * n_in, c * LANES:(c + 1) * LANES]
        part[wide * n_in:wide * n_in + n_out, :] = d_out[dev * n_out:(dev + 1) * n_out, :]
        part[wide * n_in + n_out:, :] = jnp.broadcast_to(loss if dev == 0 else 0.0 * loss, (8, LANES))


def unpack_grads(sums_ref, in_ref, out_ref, loss_ref):
    parts, n_in, width = in_ref.shape
    n_out = out_ref.shape[1]
    wide = width // LANES
    for dev in range(parts):
        for c in range(wide):
            in_ref[dev, :, c * LANES:(c + 1) * LANES] = sums_ref[dev, c * n_in:(c + 1) * n_in, :]
        out_ref[dev] = sums_ref[dev, wide * n_in:wide * n_in + n_out, :]
    loss_ref[...] = sums_ref[0, wide * n_in + n_out:, :]


def weight_grads(row_t, grad_t, pre_ref, hid_ref, in_ref, out_ref):
    parts, n_in, _ = in_ref.shape
    n_out = out_ref.shape[1]
    d_in = dot_nn(row_t, pre_ref[...])
    d_out = dot_nn(grad_t, hid_ref[...]).T
    for dev in range(parts):
        in_ref[dev] = d_in[dev * n_in:(dev + 1) * n_in, :]
        out_ref[dev] = d_out[dev * n_out:(dev + 1) * n_out, :]


def step_kernel(x_ref, tok_ref, w1, w2, wi1, wi2, cand_ref, logq_ref, targ_ref, rows_out, di_in_out, di_out_out, dq_in_out, dq_out_out, loss_out, v):
    parts, n_item, _ = x_ref.shape
    n_tok = tok_ref.shape[0]
    n_cand = n_item - n_tok
    total = float(n_tok * parts)
    scale = SCORE_GAIN / math.sqrt(LANES)
    me, core, chip, sign = place()
    x_chip = 2 * chip_at(chip, sign, 1)
    diag = 2 * chip_at(chip, sign, 6) + core
    rounds = ((me + 1 - 2 * core, x_chip + core, x_chip + 1 - core), (2 * chip_at(chip, sign, 2) + core, 2 * chip_at(chip, sign, 4) + core, diag))
    enter([me + 1 - 2 * core, x_chip + 1 - core] + [2 * chip_at(chip, sign, s) + core for s in SLOTS[1:]])
    x_mine, x_sem = v["x_mine"], v["x_sem"]

    def fetch(s):
        return pltpu.make_async_copy(x_ref.at[2 * chip_at(chip, sign, s) + core], x_mine.at[s], x_sem.at[s])

    def own_part(s, a):
        fetch(s).wait()
        return x_mine[s]

    rs_rows = reduce_scatter_steps(lambda dev, a: x_ref.at[dev], thirds(n_item, 16), group(v, "rs"), mine=own_part)
    next(rs_rows)
    for s in CORE_ORDER:
        fetch(s).start()
    tower_into(n_tok, lambda s: tok_ref[s, :], w1, w2, v["q_slope"], v["q_hid"], v["q_vec"])
    q_all = v["q_all"]
    q_all[me] = v["q_vec"][...]
    ag_q = all_gather_steps(lambda a: v["q_vec"], lambda dev, a: q_all.at[dev], thirds(n_tok, 16), group(v, "agq"))
    next(ag_q)
    next(rs_rows)
    next(ag_q)
    n_sub = n_cand // LANES
    for r in range(n_sub):
        s = pl.ds(r * LANES, LANES)
        row = pl.ds(me * n_sub + r, 1)
        v["lq"][s, :] = jnp.broadcast_to(logq_ref[row, :] * LOG2E, (LANES, LANES)).T
        v["ids"][s, :] = jnp.broadcast_to(cand_ref[row, :].astype(F32), (LANES, LANES)).T
    drain(rs_rows, ag_q)
    raw = v["rs.1"].at[0]
    tower_into(n_item, lambda s: raw[s, :], wi1, wi2, v["i_slope"], v["i_hid"], v["i_vec"])
    vec = v["i_vec"]
    z_ref, top_ref, den_ref, own_ref = v["z"], v["top"], v["den"], v["own"]
    own = pl.ds(me, 1)
    targ_vec = vec[pl.ds(n_cand, n_tok), :]
    q_own = v["q_vec"][...]
    eye = lax.broadcasted_iota(I32, (n_tok, n_tok), 0) == lax.broadcasted_iota(I32, (n_tok, n_tok), 1)
    z_own = jnp.sum(jnp.where(eye, dot_nt(targ_vec, q_own), 0.0), axis=0, keepdims=True) * (scale * LOG2E)
    own_ref[...] = jnp.full(own_ref.shape, -jnp.inf, F32)
    own_ref[own, :] = z_own

    def pass_one(t, _):
        q_t = q_all[t]
        targ = jnp.concatenate([targ_ref[t, pl.ds(i, 1), :] for i in range(n_tok // LANES)], axis=1).astype(F32)
        z_t = own_ref[pl.ds(t, 1), :]
        top8 = jnp.broadcast_to(z_t, (8, n_tok))
        for j in range(n_cand // COL_BLK):
            s = pl.ds(j * COL_BLK, COL_BLK)
            lq = jnp.concatenate([v["lq"][s, :]] * (n_tok // LANES), axis=1)
            ids = jnp.concatenate([v["ids"][s, :]] * (n_tok // LANES), axis=1)
            z = dot_nt(vec[s, :], q_t) * (scale * LOG2E) - lq
            z = jnp.where(ids == targ, HIT_VALUE * LOG2E, z)
            z_ref[t, s, :] = z
            top8 = jnp.maximum(top8, jnp.max(z.reshape(COL_BLK // 8, 8, n_tok), axis=0))
        top = jnp.max(top8, axis=0, keepdims=True)
        den8 = jnp.zeros((8, n_tok), F32)
        for j in range(n_cand // COL_BLK):
            e = jnp.exp2(z_ref[t, pl.ds(j * COL_BLK, COL_BLK), :] - top)
            den8 = den8 + jnp.sum(e.reshape(COL_BLK // 8, 8, n_tok), axis=0)
        top_ref[pl.ds(t, 1), :] = top
        den_ref[pl.ds(t, 1), :] = jnp.sum(den8, axis=0, keepdims=True) + jnp.exp2(z_t - top)
        return 0

    lax.fori_loop(0, parts, pass_one, 0)
    held, got, st_send, st_recv = group(v, "st")
    held[0, 0] = top_ref[...]
    held[0, 1] = den_ref[...]
    for r, peers in enumerate(rounds):
        copies = [remote(held.at[r], got.at[r, i], st_send.at[r, i], st_recv.at[r, i], peer) for i, peer in enumerate(peers)]
        for c in copies:
            c.start()
        for c in copies:
            c.wait()
        tops = [held[r, 0]] + [got[r, i, 0] for i in range(3)]
        dens = [held[r, 1]] + [got[r, i, 1] for i in range(3)]
        top = jnp.maximum(jnp.maximum(tops[0], tops[1]), jnp.maximum(tops[2], tops[3]))
        held[r + 1, 0] = top
        held[r + 1, 1] = sum(d * jnp.exp2(m - top) for m, d in zip(tops, dens))
    norm = v["norm"]
    norm[...] = held[2, 0] + jnp.log2(held[2, 1] * total)
    top_ref[...] = held[2, 0]
    den_ref[...] = held[2, 1]
    lse = top_ref[own, :] + jnp.log2(den_ref[own, :])
    loss = jnp.sum(lse - z_own, axis=1, keepdims=True) * (1.0 / (LOG2E * total))
    dz_row = ((jnp.exp2(z_own - top_ref[own, :]) / den_ref[own, :] - 1.0) * (1.0 / total)).astype(BF).astype(F32)
    dz_col = jnp.sum(jnp.where(eye, dz_row, 0.0), axis=1, keepdims=True)
    grad = v["i_grad"]
    grad[pl.ds(n_cand, n_tok), :] = (scale * dz_col * q_own.astype(F32)).astype(BF)
    vec_t = v["vec_t"]
    vec_t[...] = turn(vec[:n_cand, :])
    d_acc, dz_s, dh = v["d_acc"], v["dz"], v["dh"]
    d_acc[...] = jnp.zeros_like(d_acc)

    def pass_two(t, _):
        shift = norm[pl.ds(t, 1), :]
        for j in range(n_cand // COL_BLK):
            s = pl.ds(j * COL_BLK, COL_BLK)
            dz_s[s, :] = jnp.exp2(z_ref[t, s, :] - shift).astype(BF)
        d_acc[...] += dot_nn(dz_s[...], q_all[t])
        dh[t] = dot_nn(vec_t[...], dz_s[...])
        return 0

    def both(s):
        lax.fori_loop(0, 2, lambda c, _: pass_two(2 * chip_at(chip, sign, s) + c, 0), 0)

    rs_dh = reduce_scatter_steps(lambda dev, a: dh.at[dev], thirds(LANES, 8), group(v, "rsd"), produce=both)
    next(rs_dh)
    grad[pl.ds(0, n_cand), :] = (d_acc[...] * scale).astype(BF)
    i_pre, i_slope = v["i_pre"], v["i_slope"]

    def pre_grad(s):
        i_pre[s, :] = (i_slope[s, :] * dot_nt(grad[s, :], wi2[...])).astype(BF)

    row_blocks(n_item, pre_grad)
    next(rs_dh)
    rows_v, row_sem = v["rows"], v["row_sem"]
    mine = rows_v.at[me]
    row_cuts = thirds(n_item, 16)

    def leave(k, s, other):
        dev = 2 * chip_at(chip, sign, s) + (1 - core if other else core)
        p = pl.ds(row_cuts[k][1], row_cuts[k][2])
        return pltpu.make_async_copy(rows_v.at[dev, p, :], rows_out.at[dev, p, :], row_sem.at[k, s, other])

    def input_grad(s):
        mine[s, :] = dot_nt(i_pre[s, :], wi1[...]).astype(BF)

    row_blocks(n_item, input_grad)
    next(rs_dh)
    ag_rows = all_gather_steps(lambda a: mine, lambda dev, a: rows_v.at[dev], row_cuts, group(v, "agr"), landed=lambda k, s, o: leave(k, s, o).start())
    next(ag_rows)
    for k in range(3):
        leave(k, 0, 0).start()
    weight_grads(turn(raw[...]), turn(grad[...]), i_pre, v["i_hid"], v["di_in"], v["di_out"])
    next(rs_dh)
    next(ag_rows)

    def sum_all(name, parts_in, orders, outs):
        pieces = [(a, 0, r.shape[1], o) for a, (r, o) in enumerate(zip(parts_in, orders))]
        refs = group(v, name)
        sums = [refs[3 * a + 1].at[0] for a in range(len(parts_in))]
        first = reduce_scatter_steps(lambda dev, a: parts_in[a].at[dev], pieces, refs[:-4])
        yield from (x for _, x in zip(range(5), first))
        for a, out in enumerate(outs):
            out[me] = sums[a][...]
        yield from all_gather_steps(lambda a: sums[a], lambda dev, a: outs[a].at[dev], pieces, refs[-4:])
        for _ in first:
            pass

    ar_i = sum_all("ai", (v["di_in"], v["di_out"]), (0, 1), (di_in_out, di_out_out))
    next(ar_i)
    next(rs_dh)
    d_query = ((dz_col * targ_vec.astype(F32) + v["rsd.1"][0].T) * scale).astype(BF)
    q_pre = v["q_pre"]
    q_pre[...] = (v["q_slope"][...] * dot_nt(d_query, w2[...])).astype(BF)
    packed_grads(turn(tok_ref[...]), turn(d_query), q_pre, v["q_hid"], loss, v["q_part"])
    ar_q = sum_direct_steps(v["q_part"], v["q_sum"], group(v, "aq"))
    drain(ar_q, ar_i, ag_rows, rs_dh)
    unpack_grads(v["q_sum"], dq_in_out, dq_out_out, loss_out)
    for k in range(3):
        for s in SLOTS:
            for other in range(2):
                leave(k, s, other).wait()


def step(x, tokens, weights, cand, logq, targ, cid):
    parts, n_item, _ = x.shape
    n_tok = tokens.shape[0]
    n_cand = n_item - n_tok
    ff = weights[0].shape[1]
    dma = pltpu.SemaphoreType.DMA
    n_in, n_out = LANES // parts, ff // parts
    w_parts = [(n_in, ff, F32), (n_out, LANES, F32)]
    spec = grouped("rs", rs_scratch([(n_item, LANES, BF)], 3))
    spec += grouped("st", [pltpu.VMEM((3, 2, parts, n_tok), F32), pltpu.VMEM((2, 3, 2, parts, n_tok), F32), dma((2, 3)), dma((2, 3))])
    spec += grouped("rsd", rs_scratch([(LANES, n_tok, F32)], 3))
    spec += grouped("agr", ag_scratch(3))
    spec += grouped("ai", rs_scratch(w_parts, 2) + ag_scratch(2))
    q_rows = n_in * (ff // LANES) + n_out + 8
    spec += grouped("aq", direct_scratch(q_rows, LANES))
    spec += grouped("agq", ag_scratch(3))
    spec += [("x_sem", dma((8,))), ("row_sem", dma((3, 8, 2)))]

    def add(name, shape, dtype=F32):
        spec.append((name, pltpu.VMEM(shape, dtype)))

    for n, pre in ((n_tok, "q"), (n_item, "i")):
        add(pre + "_slope", (n, ff))
        add(pre + "_hid", (n, ff), BF)
        add(pre + "_pre", (n, ff), BF)
        add(pre + "_vec", (n, LANES), BF)
    add("i_grad", (n_item, LANES), BF)
    add("di_in", (parts, n_in, ff))
    add("di_out", (parts, n_out, LANES))
    add("q_part", (2, parts // 2, q_rows, LANES))
    add("q_sum", (parts, q_rows, LANES))
    add("x_mine", (8, n_item, LANES), BF)
    add("rows", (parts, n_item, LANES), BF)
    add("q_all", (parts, n_tok, LANES), BF)
    for name in ("lq", "ids", "d_acc"):
        add(name, (n_cand, LANES))
    add("z", (parts, n_cand, n_tok))
    for name in ("top", "den", "norm", "own"):
        add(name, (parts, n_tok))
    add("vec_t", (LANES, n_cand), BF)
    add("dz", (n_cand, n_tok), BF)
    add("dh", (parts, LANES, n_tok))
    sums = (jax.ShapeDtypeStruct((parts, n_in, ff), F32), jax.ShapeDtypeStruct((parts, n_out, LANES), F32))
    outs = (jax.ShapeDtypeStruct((parts, n_item, LANES), BF),) + sums + sums + (jax.ShapeDtypeStruct((8, LANES), F32),)
    return kernel_call(step_kernel, "softmax_step", cid, outs, spec, x, tokens, *weights, cand, logq, targ, in_hbm=(0,), out_hbm=(0,))


def solution(mesh):
    num_dev = mesh.shape["dp"]

    def local_step(tokens, w_one, w_two, wi_one, wi_two, table_loc, cand_ids, log_q, targ_loc):
        rows_loc, dim = table_loc.shape
        n_item = cand_ids.shape[0] // num_dev + tokens.shape[0]
        cand = cand_ids.reshape(-1, LANES)
        targ = start(targ_loc.reshape(-1, LANES), num_dev, 1)
        owned, plist, counts = gather(table_loc, cand, targ)
        back, *sums = step(owned.reshape(num_dev, n_item, dim), tokens, (w_one, w_two, wi_one, wi_two), cand, log_q.reshape(-1, LANES), targ, 2)
        d_table, di_in, di_out, dq_in, dq_out, loss = scatter(back.reshape(-1, dim), plist, counts, rows_loc, sums, num_dev)
        shaped = [g.reshape(w.shape) for g, w in zip((dq_in, dq_out, di_in, di_out), (w_one, w_two, wi_one, wi_two))]
        return (loss[0, 0], d_table) + tuple(shaped)

    return jax.shard_map(local_step, mesh=mesh, in_specs=(P("dp", None), P(), P(), P(), P(), P("dp", None), P(), P(), P("dp")), out_specs=(P(), P("dp", None), P(), P(), P(), P()), check_vma=False)
```

```python
import functools
import math
import jax
import jax.numpy as jnp
from jax import lax
from jax.experimental import pallas as pl
from jax.experimental.pallas import tpu as pltpu
from jax.sharding import PartitionSpec as P

SCORE_GAIN = 3.0
HIT_VALUE = -1e9
LANES = 128
VMEM_CAP = 60 * 1024 * 1024
BF = jnp.bfloat16
F32 = jnp.float32
I32 = jnp.int32
VM = pl.BlockSpec(memory_space=pltpu.VMEM)
SM = pl.BlockSpec(memory_space=pltpu.SMEM)
HB = pl.BlockSpec(memory_space=pl.ANY)
BLK = 256


def compact(loc, num_rows, parts, head):
    nr = loc.shape[0]
    own = jnp.where((loc >= 0) & (loc < num_rows), 1.0, 0.0)
    own16 = own.astype(BF)
    tri = jnp.where(lax.broadcasted_iota(I32, (LANES, LANES), 0) < lax.broadcasted_iota(I32, (LANES, LANES), 1), 1.0, 0.0).astype(BF)
    within = jnp.dot(own16, tri, preferred_element_type=F32)
    low = jnp.where(lax.broadcasted_iota(I32, (nr, nr), 1) < lax.broadcasted_iota(I32, (nr, nr), 0), 1.0, 0.0).astype(BF)
    before = jnp.sum(jnp.dot(low, own16, preferred_element_type=F32), axis=1, keepdims=True)
    lane = lax.broadcasted_iota(I32, (nr, LANES), 1)
    flat = lax.broadcasted_iota(I32, (nr, LANES), 0) * LANES + lane
    disp = flat - (within + before).astype(I32)
    n_head, n_tail = head // parts, (nr * LANES - head) // parts
    late = flat - head
    pos = jnp.where(flat < head, flat + flat // n_head * n_tail, late + (late // n_tail + 1) * n_head)
    val = jnp.where(own > 0, pos * 32768 + loc, -1)
    total = jnp.sum(own).astype(I32)

    def back(x, s):
        if s >= LANES:
            return pltpu.roll(x, nr - s // LANES, axis=0)
        here = pltpu.roll(x, LANES - s, axis=1)
        return jnp.where(lane < LANES - s, here, pltpu.roll(here, nr - 1, axis=0))

    bit = 0
    while (1 << bit) < nr * LANES:
        val_b, disp_b = back(val, 1 << bit), back(disp, 1 << bit)
        take = (val_b >= 0) & (((disp_b >> bit) & 1) == 1)
        stay = ((disp >> bit) & 1) == 0
        val = jnp.where(take, val_b, jnp.where(stay, val, -1))
        disp = jnp.where(take, disp_b, disp)
        bit += 1
    return jnp.where(flat < total, val, nr * LANES * 32768), own, total


def gather_kernel(chunks, cand_ref, targ_ref, table_ref, out_ref, list_ref, cnt_ref, ids_ref, stage, tab, dense, plist, packed_rows, sem, psem, osem):
    rows = tab.shape[0]
    npos = out_ref.shape[0]
    cr = rows // chunks

    def load(c):
        return pltpu.make_async_copy(table_ref.at[pl.ds(c * cr, cr), :], stage.at[pl.ds(c * cr, cr), :], sem.at[c])

    for c in range(chunks):
        load(c).start()
    parts, sub, _ = targ_ref.shape
    n_head = cand_ref.shape[0]
    head = n_head * LANES
    ids_ref[:n_head, :] = cand_ref[...]
    for d in range(parts):
        ids_ref[n_head + d * sub:n_head + (d + 1) * sub, :] = targ_ref[d]
    packed, own, total = compact(ids_ref[...] - lax.axis_index("dp") * rows, rows, parts, head)
    list_ref[...] = packed
    cnt_ref[0] = jnp.sum(own[:head // LANES]).astype(I32)
    cnt_ref[1] = total
    to_smem = pltpu.make_async_copy(list_ref, plist, psem)
    to_smem.start()

    def zero(i, _):
        dense[pl.ds(pl.multiple_of(i * BLK, BLK), BLK), :] = jnp.zeros((BLK, LANES), F32)
        return 0

    lax.fori_loop(0, npos // BLK, zero, 0)
    for c in range(chunks):
        load(c).wait()

        def conv(i, _, c=c):
            s = pl.ds(pl.multiple_of(c * cr + i * BLK, BLK), BLK)
            tab[s, :] = stage[s, :].astype(F32)
            return 0

        lax.fori_loop(0, cr // BLK, conv, 0)
    to_smem.wait()

    def pick(i, _):
        vals = []
        for u in range(LANES):
            w = plist[i, u]
            vals.append((w >> 15, tab[pl.ds(w & 32767, 1), :]))
        for p, v in vals:
            dense[pl.ds(p, 1), :] = v
        return 0

    lax.fori_loop(0, (total + LANES - 1) // LANES, pick, 0)

    part = npos // parts

    def leave(d):
        s = pl.ds(d * part, part)
        return pltpu.make_async_copy(packed_rows.at[s, :], out_ref.at[s, :], osem.at[d])

    for d in range(parts):
        packed_rows[pl.ds(d * part, part), :] = dense[pl.ds(d * part, part), :].astype(BF)
        leave(d).start()
    for d in range(parts):
        leave(d).wait()


def gather(table, cand, targ):
    rows = table.shape[0]
    nr = cand.shape[0] + targ.shape[0] * targ.shape[1]
    npos = nr * LANES
    chunks = 8
    return pl.pallas_call(
        functools.partial(gather_kernel, chunks),
        out_shape=(jax.ShapeDtypeStruct((npos, LANES), BF), jax.ShapeDtypeStruct((nr, LANES), I32), jax.ShapeDtypeStruct((2,), I32)),
        in_specs=[VM, VM, HB],
        out_specs=(HB, VM, SM),
        scratch_shapes=[pltpu.VMEM((nr, LANES), I32), pltpu.VMEM((rows, LANES), BF), pltpu.VMEM((rows, LANES), F32), pltpu.VMEM((npos + 8, LANES), F32), pltpu.SMEM((nr, LANES), I32), pltpu.VMEM((npos, LANES), BF), pltpu.SemaphoreType.DMA((chunks,)), pltpu.SemaphoreType.DMA, pltpu.SemaphoreType.DMA((targ.shape[0],))],
        compiler_params=pltpu.CompilerParams(vmem_limit_bytes=VMEM_CAP),
        name="gather_rows",
    )(cand, targ, table)


ADDS = 4


def scatter_kernel(chunks, cnt_ref, list_ref, grad_ref, *refs):
    n = (len(refs) - 10) // 3
    passed, (out_ref, *refs) = refs[:n], refs[n:]
    kept, held, (acc, raw, grad, plist, sem, psem, gsem, isem, osem) = refs[:n], refs[n:2 * n], refs[2 * n:]
    parts = gsem.shape[0]
    part = grad_ref.shape[0] // parts

    def arrive(d):
        s = pl.ds(d * part, part)
        return pltpu.make_async_copy(grad_ref.at[s, :], raw.at[s, :], gsem.at[d])

    for d in range(parts):
        arrive(d).start()
    ins = [pltpu.make_async_copy(src, dst, isem.at[i]) for i, (src, dst) in enumerate(zip(passed, held))]
    outs = [pltpu.make_async_copy(src, dst, osem.at[i]) for i, (src, dst) in enumerate(zip(held, kept))]
    for c in ins:
        c.start()
    rows = out_ref.shape[0]
    npos = grad_ref.shape[0]
    to_smem = pltpu.make_async_copy(list_ref, plist, psem)
    to_smem.start()

    def zero(i, _):
        acc[pl.ds(pl.multiple_of(i * BLK, BLK), BLK), :] = jnp.zeros((BLK, LANES), F32)
        return 0

    lax.fori_loop(0, rows // BLK, zero, 0)

    for d in range(parts):
        arrive(d).wait()
        s = pl.ds(d * part, part)
        grad[s, :] = raw[s, :].astype(F32)
    for i, o in zip(ins, outs):
        i.wait()
        o.start()
    grad[npos:, :] = jnp.zeros((8, LANES), F32)
    to_smem.wait()
    nhead = cnt_ref[0]
    total = cnt_ref[1]

    def put(i, _):
        vals = []
        for u in range(LANES):
            w = plist[i, u]
            vals.append((w & 32767, grad[pl.ds(w >> 15, 1), :]))
        for r, v in vals:
            acc[pl.ds(r, 1), :] = v
        return 0

    lax.fori_loop(0, nhead // LANES, put, 0)

    def add_one(i, _):
        w = plist[i >> 7, i & 127]
        r = pl.ds(w & 32767, 1)
        acc[r, :] = acc[r, :] + grad[pl.ds(w >> 15, 1), :]
        return 0

    def add_row(i, _):
        for j in range(0, LANES, ADDS):
            words = [plist[i, j + u] for u in range(ADDS)]
            rs = [w & 32767 for w in words]
            gs = [grad[pl.ds(w >> 15, 1), :] for w in words]
            outs = []
            for u in range(ADDS):
                v = acc[pl.ds(rs[u], 1), :] + gs[u]
                for t in range(u):
                    v = v + jnp.where(rs[t] == rs[u], gs[t], 0.0)
                outs.append(v)
            for u in range(ADDS):
                acc[pl.ds(rs[u], 1), :] = outs[u]
        return 0

    begin = nhead // LANES * LANES
    split = jnp.minimum((nhead + LANES - 1) // LANES * LANES, total)
    lax.fori_loop(begin, split, add_one, 0)
    lax.fori_loop((split + LANES - 1) // LANES, (total + LANES - 1) // LANES, add_row, 0)
    cr = rows // chunks

    def store(c):
        return pltpu.make_async_copy(acc.at[pl.ds(c * cr, cr), :], out_ref.at[pl.ds(c * cr, cr), :], sem.at[c])

    for c in range(chunks):
        store(c).start()
    for c in range(chunks):
        store(c).wait()
    for o in outs:
        o.wait()


def scatter(grads, plist, counts, rows, passed, parts):
    nr = plist.shape[0]
    npos = nr * LANES
    chunks = 8
    n = len(passed)
    dma = pltpu.SemaphoreType.DMA
    return pl.pallas_call(
        functools.partial(scatter_kernel, chunks),
        out_shape=(jax.ShapeDtypeStruct((rows, LANES), F32),) + tuple(jax.ShapeDtypeStruct(p.shape, p.dtype) for p in passed),
        in_specs=[SM, HB, HB] + [HB] * n,
        out_specs=(HB,) * (n + 1),
        scratch_shapes=[pltpu.VMEM(p.shape, p.dtype) for p in passed]
        + [pltpu.VMEM((rows, LANES), F32), pltpu.VMEM((npos, LANES), BF), pltpu.VMEM((npos + 8, LANES), F32), pltpu.SMEM((nr, LANES), I32), dma((chunks,)), dma, dma((parts,)), dma((n,)), dma((n,))],
        compiler_params=pltpu.CompilerParams(vmem_limit_bytes=VMEM_CAP),
        name="scatter_rows",
    )(counts, plist, grads, *passed)


MESHID = pl.DeviceIdType.MESH
CHIP_DIMS = (1, 2, 4)
SLOTS = tuple(range(8))
CORE_ORDER = (7, 3, 5, 6, 1, 2, 4, 0)
RS_BASE = (0, 4, 6)


def place():
    me = lax.axis_index("dp")
    core = lax.rem(me, 2)
    chip = me // 2
    sign = {d: 1 - 2 * lax.rem(chip // d, 2) for d in CHIP_DIMS}
    return me, core, chip, sign


def chip_at(chip, sign, s):
    for d in CHIP_DIMS:
        if s & d:
            chip = chip + d * sign[d]
    return chip


def enter(peers):
    barrier = pltpu.get_barrier_semaphore()
    for peer in peers:
        pl.semaphore_signal(barrier, inc=1, device_id=(peer,), device_id_type=MESHID)
    pl.semaphore_wait(barrier, len(peers))


def order_of(k):
    return tuple(CHIP_DIMS[(k + i) % 3] for i in range(3))


def thirds(rows, unit, first=0):
    base = rows // unit
    cuts = [(base * i // 3) * unit for i in range(4)]
    return [(0, first + cuts[i], cuts[i + 1] - cuts[i], i) for i in range(3)]


def remote(src, dst, send, recv, peer):
    return pltpu.make_async_remote_copy(src_ref=src, dst_ref=dst, send_sem=send, recv_sem=recv, device_id=(peer,), device_id_type=MESHID)


def stage_slots(order, t):
    dims = order_of(order)
    live = [s for s in SLOTS if all(not s & d for d in dims[:t])]
    return [(s, s ^ dims[t]) for s in live if s & dims[t]]


def rs_scratch(arrays, num):
    out = []
    for rows, width, dtype in arrays:
        out += [pltpu.VMEM((8, rows, width), dtype), pltpu.VMEM((8, rows, width), dtype), pltpu.VMEM((7, rows, width), dtype)]
    n = len(arrays)
    dma = pltpu.SemaphoreType.DMA
    return out + [dma((n, 8)), dma((n, 8)), dma((num, 7)), dma((num, 7))]


def reduce_scatter_steps(get, pieces, scratch, mine=None, produce=None):
    csend_s, crecv_s, send_s, recv_s = scratch[-4:]
    me, core, chip, sign = place()
    other = me + 1 - 2 * core
    num = len(pieces)
    arrays = range((len(scratch) - 4) // 3)
    crecv, acc, recv = ([scratch[3 * a + i] for a in arrays] for i in range(3))
    started = []

    def core_copy(s, a):
        return remote(get(2 * chip_at(chip, sign, s) + 1 - core, a), crecv[a].at[s], csend_s.at[a, s], crecv_s.at[a, s], other)

    def ici_copy(k, t, i, s):
        a, off, ln, order = pieces[k]
        slot = RS_BASE[t] + i
        peer = 2 * chip_at(chip, sign, order_of(order)[t]) + core
        return remote(acc[a].at[s, pl.ds(off, ln), :], recv[a].at[slot, pl.ds(off, ln), :], send_s.at[k, slot], recv_s.at[k, slot], peer)

    def go(c):
        c.start()
        started.append(c)

    def absorb(s):
        for a in arrays:
            core_copy(s, a).wait_recv()
            part = mine(s, a) if mine else get(2 * chip_at(chip, sign, s) + core, a)[...]
            acc[a][s] = part + crecv[a][s]
        for k in range(num):
            for i, (src, dst) in enumerate(stage_slots(pieces[k][3], 0)):
                if src == s:
                    go(ici_copy(k, 0, i, s))

    for n, s in enumerate(CORE_ORDER):
        if produce:
            produce(s)
        for a in arrays:
            go(core_copy(s, a))
        if produce and n:
            absorb(CORE_ORDER[n - 1])
    yield
    for s in CORE_ORDER[-1:] if produce else CORE_ORDER:
        absorb(s)
    yield
    for t in range(3):
        for i in reversed(range(4 >> t)):
            for k in range(num):
                a, off, ln, order = pieces[k]
                src, dst = stage_slots(order, t)[i]
                ici_copy(k, t, i, src).wait_recv()
                p = pl.ds(off, ln)
                acc[a][dst, p, :] = acc[a][dst, p, :] + recv[a][RS_BASE[t] + i, p, :]
                if t < 2:
                    for i2, (src2, dst2) in enumerate(stage_slots(order, t + 1)):
                        if src2 == dst:
                            go(ici_copy(k, t + 1, i2, dst))
        yield
    for c in started:
        c.wait_send()


def ag_scratch(num):
    return [pltpu.SemaphoreType.DMA((num, 8))] * 4


def all_gather_steps(own, out, pieces, scratch, landed=None):
    csend_s, crecv_s, send_s, recv_s = scratch
    me, core, chip, sign = place()
    other = me + 1 - 2 * core
    num = len(pieces)
    started = []

    def ref(k, s, c):
        a, off, ln, _ = pieces[k]
        return out(2 * chip_at(chip, sign, s) + c, a).at[pl.ds(off, ln), :]

    def source(k, s):
        a, off, ln, _ = pieces[k]
        return own(a).at[pl.ds(off, ln), :] if s == 0 else ref(k, s, core)

    def go(c):
        c.start()
        started.append(c)

    def core_send(k, s):
        go(remote(source(k, s), ref(k, s, core), csend_s.at[k, s], crecv_s.at[k, s], other))

    def send(k, t, s):
        d = order_of(pieces[k][3])[t]
        peer = 2 * chip_at(chip, sign, d) + core
        go(remote(source(k, s), ref(k, s, core), send_s.at[k, s ^ d], recv_s.at[k, s ^ d], peer))

    def arrive(k, s):
        there = ref(k, s, core)
        remote(there, there, send_s.at[k, s], recv_s.at[k, s], other).wait_recv()
        core_send(k, s)
        if landed:
            landed(k, s, 0)

    plan = (((), (0, 0)), ((), (1, 0)), ((), (2, 0)), ((1,), (1, 1)), ((), (2, 1)), ((2,), (2, 2)), ((3,), (2, 3)), ((4, 5, 6, 7), None))
    for i, (waits, sends) in enumerate(plan):
        for j in waits or (None,):
            for k in range(num):
                d = order_of(pieces[k][3])

                def slot(bits):
                    return sum(d[b] for b in range(3) if bits >> b & 1)

                if j is not None:
                    arrive(k, slot(j))
                if sends is not None:
                    send(k, sends[0], slot(sends[1]))
                if i == 0:
                    core_send(k, 0)
        yield
    for k in range(num):
        for s in SLOTS:
            there = ref(k, s, 1 - core)
            remote(there, there, csend_s.at[k, s], crecv_s.at[k, s], other).wait_recv()
            if landed:
                landed(k, s, 1)
    for c in started:
        c.wait_send()


def direct_scratch(rows, width):
    dma = pltpu.SemaphoreType.DMA
    return [pltpu.VMEM((8, rows, width), F32)] * 3 + [pltpu.VMEM((rows, width), F32), dma, dma, dma((8,)), dma((8,)), dma((8,)), dma((8,)), dma((8,)), dma((8,))]


def sum_direct_steps(src, out, scratch):
    crecv, acc, recv, tot, cs, cr, s1, r1, s2, r2, s3, r3 = scratch
    me, core, chip, sign = place()
    other = me + 1 - 2 * core
    first = remote(src.at[1 - core], crecv, cs, cr, other)
    first.start()
    yield
    first.wait_recv()
    acc[...] = src[core] + crecv[...]
    far = (7, 3, 5, 6, 1, 2, 4)

    def to(s):
        return 2 * chip_at(chip, sign, s) + core

    sends = [remote(acc.at[chip_at(chip, sign, s)], recv.at[s], s1.at[s], r1.at[s], to(s)) for s in far]
    for c in sends:
        c.start()
    yield
    for c in sends:
        c.wait_recv()
    total = acc[chip]
    for s in far:
        total = total + recv[s]
    tot[...] = total
    backs = [remote(tot, out.at[me], s2.at[s], r2.at[s], to(s)) for s in far]
    for c in backs:
        c.start()
    pair = [remote(tot, out.at[me], s3.at[0], r3.at[0], other)]
    pair[0].start()
    out[me] = total
    yield
    for s in reversed(far):
        there = out.at[to(s)]
        remote(there, there, s2.at[s], r2.at[s], other).wait_recv()
        c = remote(there, there, s3.at[s], r3.at[s], other)
        c.start()
        pair.append(c)
    yield
    for s in SLOTS:
        there = out.at[2 * chip_at(chip, sign, s) + 1 - core]
        remote(there, there, s3.at[s], r3.at[s], other).wait_recv()
    for c in [first] + sends + backs + pair:
        c.wait_send()


def drain(*steps):
    live = list(steps)
    while live:
        live = [g for g in live if next(g, StopIteration) is not StopIteration]


def kernel_call(body, name, cid, out_shape, scratch, *args, in_hbm=(), out_hbm=()):
    names = tuple(n for n, _ in scratch)

    def kernel(*refs):
        n = len(args) + len(jax.tree.leaves(out_shape))
        body(*refs[:n], dict(zip(names, refs[n:])))

    return pl.pallas_call(
        kernel,
        out_shape=out_shape,
        in_specs=[HB if i in in_hbm else VM for i in range(len(args))],
        out_specs=tuple(HB if i in out_hbm else VM for i in range(len(out_shape))),
        scratch_shapes=[s for _, s in scratch],
        compiler_params=pltpu.CompilerParams(collective_id=cid, has_side_effects=True, vmem_limit_bytes=VMEM_CAP),
        name=name,
    )(*args)


def grouped(name, items):
    return [(f"{name}.{i}", s) for i, s in enumerate(items)]


def group(scratch, name):
    return [v for k, v in scratch.items() if k.startswith(name + ".")]
LOG2E = 1.4426950408889634
GELU_C = math.sqrt(2.0 / math.pi)
GELU_A = 0.044715
ROW_BLK = 256
COL_BLK = 128


def gelu_both(x):
    x2 = x * x
    t = jnp.tanh(GELU_C * (x + GELU_A * (x2 * x)))
    half = 0.5 * (1.0 + t)
    return x * half, half + (0.5 * GELU_C) * x * (1.0 - t * t) * (1.0 + (3.0 * GELU_A) * x2)


def dot_nn(a, b):
    return jnp.dot(a, b, preferred_element_type=F32)


def dot_nt(a, b):
    return lax.dot_general(a, b, (((1,), (1,)), ((), ())), preferred_element_type=F32)


def turn(x):
    return x.astype(F32).T.astype(BF)


def row_blocks(rows, body):
    def blk(i, _):
        body(pl.ds(pl.multiple_of(i * ROW_BLK, ROW_BLK), ROW_BLK))
        return 0

    lax.fori_loop(0, rows // ROW_BLK, blk, 0)


def tower_into(rows, load, w_in, w_out, slope_ref, hid_ref, out_ref):
    def blk(s):
        act, slope = gelu_both(dot_nn(load(s), w_in[...]))
        slope_ref[s, :] = slope
        hid_ref[s, :] = act.astype(BF)
        out_ref[s, :] = dot_nn(hid_ref[s, :], w_out[...]).astype(BF)

    row_blocks(rows, blk)


def start_kernel(targ_ref, targ_out, v):
    me, core, chip, sign = place()
    peers = [2 * chip_at(chip, sign, s) + c for s in reversed(SLOTS) for c in ((core, 1 - core) if s else (1 - core,))]
    enter(peers)
    send_s, recv_s = v["sems.0"], v["sems.1"]
    targ_out[me] = targ_ref[...]
    copies = [remote(targ_ref, targ_out.at[me], send_s.at[i], recv_s.at[i], peer) for i, peer in enumerate(peers)]
    for c in copies:
        c.start()
    for c in copies:
        c.wait()


def start(targ, parts, cid):
    dma = pltpu.SemaphoreType.DMA
    outs = (jax.ShapeDtypeStruct((parts,) + targ.shape, I32),)
    return kernel_call(start_kernel, "start_step", cid, outs, grouped("sems", [dma((parts - 1,)), dma((parts - 1,))]), targ)[0]


def packed_grads(row_t, grad_t, pre_ref, hid_ref, loss, sums_ref):
    d_in = dot_nn(row_t, pre_ref[...])
    d_out = dot_nn(grad_t, hid_ref[...]).T
    parts = 2 * sums_ref.shape[1]
    n_in, n_out = d_in.shape[0] // parts, d_out.shape[0] // parts
    wide = d_in.shape[1] // LANES
    for dev in range(parts):
        part = sums_ref.at[dev % 2, dev // 2]
        for c in range(wide):
            part[c * n_in:(c + 1) * n_in, :] = d_in[dev * n_in:(dev + 1) * n_in, c * LANES:(c + 1) * LANES]
        part[wide * n_in:wide * n_in + n_out, :] = d_out[dev * n_out:(dev + 1) * n_out, :]
        part[wide * n_in + n_out:, :] = jnp.broadcast_to(loss if dev == 0 else 0.0 * loss, (8, LANES))


def unpack_grads(sums_ref, in_ref, out_ref, loss_ref):
    parts, n_in, width = in_ref.shape
    n_out = out_ref.shape[1]
    wide = width // LANES
    for dev in range(parts):
        for c in range(wide):
            in_ref[dev, :, c * LANES:(c + 1) * LANES] = sums_ref[dev, c * n_in:(c + 1) * n_in, :]
        out_ref[dev] = sums_ref[dev, wide * n_in:wide * n_in + n_out, :]
    loss_ref[...] = sums_ref[0, wide * n_in + n_out:, :]


def weight_grads(row_t, grad_t, pre_ref, hid_ref, in_ref, out_ref):
    parts, n_in, _ = in_ref.shape
    n_out = out_ref.shape[1]
    d_in = dot_nn(row_t, pre_ref[...])
    d_out = dot_nn(grad_t, hid_ref[...]).T
    for dev in range(parts):
        in_ref[dev] = d_in[dev * n_in:(dev + 1) * n_in, :]
        out_ref[dev] = d_out[dev * n_out:(dev + 1) * n_out, :]


def step_kernel(x_ref, tok_ref, w1, w2, wi1, wi2, cand_ref, logq_ref, targ_ref, rows_out, di_in_out, di_out_out, dq_in_out, dq_out_out, loss_out, v):
    parts, n_item, _ = x_ref.shape
    n_tok = tok_ref.shape[0]
    n_cand = n_item - n_tok
    total = float(n_tok * parts)
    scale = SCORE_GAIN / math.sqrt(LANES)
    me, core, chip, sign = place()
    x_chip = 2 * chip_at(chip, sign, 1)
    diag = 2 * chip_at(chip, sign, 6) + core
    rounds = ((me + 1 - 2 * core, x_chip + core, x_chip + 1 - core), (2 * chip_at(chip, sign, 2) + core, 2 * chip_at(chip, sign, 4) + core, diag))
    enter([me + 1 - 2 * core, x_chip + 1 - core] + [2 * chip_at(chip, sign, s) + core for s in SLOTS[1:]])
    x_mine, x_sem = v["x_mine"], v["x_sem"]

    def fetch(s):
        return pltpu.make_async_copy(x_ref.at[2 * chip_at(chip, sign, s) + core], x_mine.at[s], x_sem.at[s])

    def own_part(s, a):
        fetch(s).wait()
        return x_mine[s]

    rs_rows = reduce_scatter_steps(lambda dev, a: x_ref.at[dev], thirds(n_item, 16), group(v, "rs"), mine=own_part)
    next(rs_rows)
    for s in CORE_ORDER:
        fetch(s).start()
    tower_into(n_tok, lambda s: tok_ref[s, :], w1, w2, v["q_slope"], v["q_hid"], v["q_vec"])
    q_all = v["q_all"]
    q_all[me] = v["q_vec"][...]
    q_send, q_recv, q_csend, q_crecv = group(v, "agq")
    q_sent = []

    def q_tile(s, c):
        return q_all.at[2 * chip_at(chip, sign, s) + c]

    def q_go(s, d):
        src = v["q_vec"] if s == 0 else q_tile(s, core)
        if d:
            c = remote(src, q_tile(s, core), q_send.at[s ^ d], q_recv.at[s ^ d], 2 * chip_at(chip, sign, d) + core)
        else:
            c = remote(src, q_tile(s, core), q_csend.at[s], q_crecv.at[s], me + 1 - 2 * core)
        c.start()
        q_sent.append(c)

    def q_have(s, onward):
        remote(q_tile(s, core), q_tile(s, core), q_send.at[s], q_recv.at[s], me + 1 - 2 * core).wait_recv()
        for d in onward:
            q_go(s, d)
        q_go(s, 0)

    def q_other(s):
        there = q_tile(s, 1 - core)
        remote(there, there, q_csend.at[s], q_crecv.at[s], me + 1 - 2 * core).wait_recv()

    for d in (1, 2, 4, 0):
        q_go(0, d)
    next(rs_rows)
    n_sub = n_cand // LANES
    for r in range(n_sub):
        s = pl.ds(r * LANES, LANES)
        row = pl.ds(me * n_sub + r, 1)
        v["lq"][s, :] = jnp.broadcast_to(logq_ref[row, :] * LOG2E, (LANES, LANES)).T
        v["ids"][s, :] = jnp.broadcast_to(cand_ref[row, :].astype(F32), (LANES, LANES)).T
    drain(rs_rows)
    raw = v["rs.1"].at[0]
    q_have(1, (2, 4))
    q_have(2, (4,))
    q_have(4, ())
    tower_into(n_item, lambda s: raw[s, :], wi1, wi2, v["i_slope"], v["i_hid"], v["i_vec"])
    q_have(3, (4,))
    vec = v["i_vec"]
    z_ref, top_ref, den_ref, own_ref = v["z"], v["top"], v["den"], v["own"]
    own = pl.ds(me, 1)
    targ_vec = vec[pl.ds(n_cand, n_tok), :]
    q_own = v["q_vec"][...]
    eye = lax.broadcasted_iota(I32, (n_tok, n_tok), 0) == lax.broadcasted_iota(I32, (n_tok, n_tok), 1)
    z_own = jnp.sum(jnp.where(eye, dot_nt(targ_vec, q_own), 0.0), axis=0, keepdims=True) * (scale * LOG2E)
    own_ref[...] = jnp.full(own_ref.shape, -jnp.inf, F32)
    own_ref[own, :] = z_own

    def pass_one(i, upper):
        t = 2 * (chip + sign[1] * lax.rem(i // 2, 2) + 2 * sign[2] * (i // 4) + upper * 4 * sign[4]) + lax.rem(i, 2)
        q_t = q_all[t]
        targ = jnp.concatenate([targ_ref[t, pl.ds(i, 1), :] for i in range(n_tok // LANES)], axis=1).astype(F32)
        z_t = own_ref[pl.ds(t, 1), :]
        top8 = jnp.broadcast_to(z_t, (8, n_tok))
        for j in range(n_cand // COL_BLK):
            s = pl.ds(j * COL_BLK, COL_BLK)
            lq = jnp.concatenate([v["lq"][s, :]] * (n_tok // LANES), axis=1)
            ids = jnp.concatenate([v["ids"][s, :]] * (n_tok // LANES), axis=1)
            z = dot_nt(vec[s, :], q_t) * (scale * LOG2E) - lq
            z = jnp.where(ids == targ, HIT_VALUE * LOG2E, z)
            z_ref[t, s, :] = z
            top8 = jnp.maximum(top8, jnp.max(z.reshape(COL_BLK // 8, 8, n_tok), axis=0))
        top = jnp.max(top8, axis=0, keepdims=True)
        den8 = jnp.zeros((8, n_tok), F32)
        for j in range(n_cand // COL_BLK):
            e = jnp.exp2(z_ref[t, pl.ds(j * COL_BLK, COL_BLK), :] - top)
            den8 = den8 + jnp.sum(e.reshape(COL_BLK // 8, 8, n_tok), axis=0)
        top_ref[pl.ds(t, 1), :] = top
        den_ref[pl.ds(t, 1), :] = jnp.sum(den8, axis=0, keepdims=True) + jnp.exp2(z_t - top)
        return upper

    for s in (0, 1, 2, 3):
        q_other(s)
    lax.fori_loop(0, parts // 2, pass_one, 0)
    for s in (5, 6, 7):
        q_have(s, ())
    for s in (4, 5, 6, 7):
        q_other(s)
    lax.fori_loop(0, parts // 2, pass_one, 1)
    for c in q_sent:
        c.wait_send()
    held, got, st_send, st_recv = group(v, "st")
    held[0, 0] = top_ref[...]
    held[0, 1] = den_ref[...]
    for r, peers in enumerate(rounds):
        copies = [remote(held.at[r], got.at[r, i], st_send.at[r, i], st_recv.at[r, i], peer) for i, peer in enumerate(peers)]
        for c in copies:
            c.start()
        for c in copies:
            c.wait()
        tops = [held[r, 0]] + [got[r, i, 0] for i in range(3)]
        dens = [held[r, 1]] + [got[r, i, 1] for i in range(3)]
        top = jnp.maximum(jnp.maximum(tops[0], tops[1]), jnp.maximum(tops[2], tops[3]))
        held[r + 1, 0] = top
        held[r + 1, 1] = sum(d * jnp.exp2(m - top) for m, d in zip(tops, dens))
    norm = v["norm"]
    norm[...] = held[2, 0] + jnp.log2(held[2, 1] * total)
    top_ref[...] = held[2, 0]
    den_ref[...] = held[2, 1]
    lse = top_ref[own, :] + jnp.log2(den_ref[own, :])
    loss = jnp.sum(lse - z_own, axis=1, keepdims=True) * (1.0 / (LOG2E * total))
    dz_row = ((jnp.exp2(z_own - top_ref[own, :]) / den_ref[own, :] - 1.0) * (1.0 / total)).astype(BF).astype(F32)
    dz_col = jnp.sum(jnp.where(eye, dz_row, 0.0), axis=1, keepdims=True)
    grad = v["i_grad"]
    grad[pl.ds(n_cand, n_tok), :] = (scale * dz_col * q_own.astype(F32)).astype(BF)
    i_pre, i_slope = v["i_pre"], v["i_slope"]
    rows_v, row_sem = v["rows"], v["row_sem"]
    mine = rows_v.at[me]

    def item_back(first, rows):
        for r in range(first, first + rows, ROW_BLK):
            s = pl.ds(r, ROW_BLK)
            i_pre[s, :] = (i_slope[s, :] * dot_nt(grad[s, :], wi2[...])).astype(BF)
            mine[s, :] = dot_nt(i_pre[s, :], wi1[...]).astype(BF)

    def send_back(n, first, rows):
        cuts = thirds(rows, 16, first)

        def leave(k, s, o):
            dev = 2 * chip_at(chip, sign, s) + (1 - core if o else core)
            p = pl.ds(cuts[k][1], cuts[k][2])
            return pltpu.make_async_copy(rows_v.at[dev, p, :], rows_out.at[dev, p, :], row_sem.at[3 * n + k, s, o])

        for k in range(3):
            leave(k, 0, 0).start()
        yield from all_gather_steps(lambda a: mine, lambda dev, a: rows_v.at[dev], cuts, group(v, f"agr{n}"), landed=lambda k, s, o: leave(k, s, o).start())
        for k in range(3):
            for s in SLOTS:
                for o in range(2):
                    leave(k, s, o).wait()

    item_back(n_cand, n_tok)
    back_t = send_back(0, n_cand, n_tok)
    for _ in range(3):
        next(back_t)
    vec_t = v["vec_t"]
    vec_t[...] = turn(vec[:n_cand, :])
    d_acc, dz_s, dh = v["d_acc"], v["dz"], v["dh"]
    d_acc[...] = jnp.zeros_like(d_acc)
    half = n_cand // 2

    def pass_two(t, first):
        shift = norm[pl.ds(t, 1), :]
        for j in range(half // COL_BLK):
            dz_s[pl.ds(j * COL_BLK, COL_BLK), :] = jnp.exp2(z_ref[t, pl.ds(first + j * COL_BLK, COL_BLK), :] - shift).astype(BF)
        d_acc[pl.ds(first, half), :] += dot_nn(dz_s[...], q_all[t])
        part = dot_nn(vec_t[:, first:first + half], dz_s[...])
        dh[t] = part if first == 0 else dh[t] + part

    def upper_half(t, _):
        pass_two(t, 0)
        return 0

    def cand_back(first):
        grad[pl.ds(first, half), :] = (d_acc[pl.ds(first, half), :] * scale).astype(BF)
        item_back(first, half)

    lax.fori_loop(0, parts // 2, upper_half, 0)
    next(back_t)
    next(back_t)
    lax.fori_loop(parts // 2, parts, upper_half, 0)
    next(back_t)
    cand_back(0)
    next(back_t)
    back_a = send_back(1, 0, half)
    for _ in range(3):
        next(back_a)

    def both(s):
        def one(c, _):
            pass_two(2 * chip_at(chip, sign, s) + c, half)
            return 0

        lax.fori_loop(0, 2, one, 0)

    rs_dh = reduce_scatter_steps(lambda dev, a: dh.at[dev], thirds(LANES, 8), group(v, "rsd"), produce=both)
    next(rs_dh)
    next(back_a)
    next(rs_dh)
    cand_back(half)
    next(rs_dh)
    next(back_a)
    next(back_t)
    back_b = send_back(2, half, half)
    next(back_b)
    weight_grads(turn(raw[...]), turn(grad[...]), i_pre, v["i_hid"], v["di_in"], v["di_out"])
    next(rs_dh)
    next(back_a)
    next(back_b)

    def sum_all(name, parts_in, orders, outs):
        pieces = [(a, 0, r.shape[1], o) for a, (r, o) in enumerate(zip(parts_in, orders))]
        refs = group(v, name)
        sums = [refs[3 * a + 1].at[0] for a in range(len(parts_in))]
        first = reduce_scatter_steps(lambda dev, a: parts_in[a].at[dev], pieces, refs[:-4])
        yield from (x for _, x in zip(range(5), first))
        for a, out in enumerate(outs):
            out[me] = sums[a][...]
        yield from all_gather_steps(lambda a: sums[a], lambda dev, a: outs[a].at[dev], pieces, refs[-4:])
        for _ in first:
            pass

    ar_i = sum_all("ai", (v["di_in"], v["di_out"]), (0, 1), (di_in_out, di_out_out))
    next(ar_i)
    next(rs_dh)
    d_query = ((dz_col * targ_vec.astype(F32) + v["rsd.1"][0].T) * scale).astype(BF)
    q_pre = v["q_pre"]
    q_pre[...] = (v["q_slope"][...] * dot_nt(d_query, w2[...])).astype(BF)
    packed_grads(turn(tok_ref[...]), turn(d_query), q_pre, v["q_hid"], loss, v["q_part"])
    ar_q = sum_direct_steps(v["q_part"], v["q_sum"], group(v, "aq"))
    drain(ar_q, ar_i, back_a, back_b, back_t, rs_dh)
    unpack_grads(v["q_sum"], dq_in_out, dq_out_out, loss_out)


def step(x, tokens, weights, cand, logq, targ, cid):
    parts, n_item, _ = x.shape
    n_tok = tokens.shape[0]
    n_cand = n_item - n_tok
    ff = weights[0].shape[1]
    dma = pltpu.SemaphoreType.DMA
    n_in, n_out = LANES // parts, ff // parts
    w_parts = [(n_in, ff, F32), (n_out, LANES, F32)]
    spec = grouped("rs", rs_scratch([(n_item, LANES, BF)], 3))
    spec += grouped("st", [pltpu.VMEM((3, 2, parts, n_tok), F32), pltpu.VMEM((2, 3, 2, parts, n_tok), F32), dma((2, 3)), dma((2, 3))])
    spec += grouped("rsd", rs_scratch([(LANES, n_tok, F32)], 3))
    for n in range(3):
        spec += grouped(f"agr{n}", ag_scratch(3))
    spec += grouped("ai", rs_scratch(w_parts, 2) + ag_scratch(2))
    q_rows = n_in * (ff // LANES) + n_out + 8
    spec += grouped("aq", direct_scratch(q_rows, LANES))
    spec += grouped("agq", [dma((8,))] * 4)
    spec += [("x_sem", dma((8,))), ("row_sem", dma((9, 8, 2)))]

    def add(name, shape, dtype=F32):
        spec.append((name, pltpu.VMEM(shape, dtype)))

    for n, pre in ((n_tok, "q"), (n_item, "i")):
        add(pre + "_slope", (n, ff))
        add(pre + "_hid", (n, ff), BF)
        add(pre + "_pre", (n, ff), BF)
        add(pre + "_vec", (n, LANES), BF)
    add("i_grad", (n_item, LANES), BF)
    add("di_in", (parts, n_in, ff))
    add("di_out", (parts, n_out, LANES))
    add("q_part", (2, parts // 2, q_rows, LANES))
    add("q_sum", (parts, q_rows, LANES))
    add("x_mine", (8, n_item, LANES), BF)
    add("rows", (parts, n_item, LANES), BF)
    add("q_all", (parts, n_tok, LANES), BF)
    for name in ("lq", "ids", "d_acc"):
        add(name, (n_cand, LANES))
    add("z", (parts, n_cand, n_tok))
    for name in ("top", "den", "norm", "own"):
        add(name, (parts, n_tok))
    add("vec_t", (LANES, n_cand), BF)
    add("dz", (n_cand // 2, n_tok), BF)
    add("dh", (parts, LANES, n_tok))
    sums = (jax.ShapeDtypeStruct((parts, n_in, ff), F32), jax.ShapeDtypeStruct((parts, n_out, LANES), F32))
    outs = (jax.ShapeDtypeStruct((parts, n_item, LANES), BF),) + sums + sums + (jax.ShapeDtypeStruct((8, LANES), F32),)
    return kernel_call(step_kernel, "softmax_step", cid, outs, spec, x, tokens, *weights, cand, logq, targ, in_hbm=(0,), out_hbm=(0,))


def solution(mesh):
    num_dev = mesh.shape["dp"]

    def local_step(tokens, w_one, w_two, wi_one, wi_two, table_loc, cand_ids, log_q, targ_loc):
        rows_loc, dim = table_loc.shape
        n_item = cand_ids.shape[0] // num_dev + tokens.shape[0]
        cand = cand_ids.reshape(-1, LANES)
        targ = start(targ_loc.reshape(-1, LANES), num_dev, 1)
        owned, plist, counts = gather(table_loc, cand, targ)
        back, *sums = step(owned.reshape(num_dev, n_item, dim), tokens, (w_one, w_two, wi_one, wi_two), cand, log_q.reshape(-1, LANES), targ, 2)
        d_table, di_in, di_out, dq_in, dq_out, loss = scatter(back.reshape(-1, dim), plist, counts, rows_loc, sums, num_dev)
        shaped = [g.reshape(w.shape) for g, w in zip((dq_in, dq_out, di_in, di_out), (w_one, w_two, wi_one, wi_two))]
        return (loss[0, 0], d_table) + tuple(shaped)

    return jax.shard_map(local_step, mesh=mesh, in_specs=(P("dp", None), P(), P(), P(), P(), P("dp", None), P(), P(), P("dp")), out_specs=(P(), P("dp", None), P(), P(), P(), P()), check_vma=False)
```

```python
import functools
import math
import jax
import jax.numpy as jnp
from jax import lax
from jax.experimental import pallas as pl
from jax.experimental.pallas import tpu as pltpu
from jax.sharding import PartitionSpec as P

SCORE_GAIN = 3.0
HIT_VALUE = -1e9
LANES = 128
VMEM_CAP = 60 * 1024 * 1024
BF = jnp.bfloat16
F32 = jnp.float32
I32 = jnp.int32
VM = pl.BlockSpec(memory_space=pltpu.VMEM)
SM = pl.BlockSpec(memory_space=pltpu.SMEM)
HB = pl.BlockSpec(memory_space=pl.ANY)
BLK = 256


def compact(loc, num_rows, parts, head):
    nr = loc.shape[0]
    own = jnp.where((loc >= 0) & (loc < num_rows), 1.0, 0.0)
    own16 = own.astype(BF)
    tri = jnp.where(lax.broadcasted_iota(I32, (LANES, LANES), 0) < lax.broadcasted_iota(I32, (LANES, LANES), 1), 1.0, 0.0).astype(BF)
    within = jnp.dot(own16, tri, preferred_element_type=F32)
    low = jnp.where(lax.broadcasted_iota(I32, (nr, nr), 1) < lax.broadcasted_iota(I32, (nr, nr), 0), 1.0, 0.0).astype(BF)
    before = jnp.sum(jnp.dot(low, own16, preferred_element_type=F32), axis=1, keepdims=True)
    lane = lax.broadcasted_iota(I32, (nr, LANES), 1)
    flat = lax.broadcasted_iota(I32, (nr, LANES), 0) * LANES + lane
    disp = flat - (within + before).astype(I32)
    n_head, n_tail = head // parts, (nr * LANES - head) // parts
    late = flat - head
    pos = jnp.where(flat < head, flat + flat // n_head * n_tail, late + (late // n_tail + 1) * n_head)
    val = jnp.where(own > 0, pos * 32768 + loc, -1)
    total = jnp.sum(own).astype(I32)

    def back(x, s):
        if s >= LANES:
            return pltpu.roll(x, nr - s // LANES, axis=0)
        here = pltpu.roll(x, LANES - s, axis=1)
        return jnp.where(lane < LANES - s, here, pltpu.roll(here, nr - 1, axis=0))

    bit = 0
    while (1 << bit) < nr * LANES:
        val_b, disp_b = back(val, 1 << bit), back(disp, 1 << bit)
        take = (val_b >= 0) & (((disp_b >> bit) & 1) == 1)
        stay = ((disp >> bit) & 1) == 0
        val = jnp.where(take, val_b, jnp.where(stay, val, -1))
        disp = jnp.where(take, disp_b, disp)
        bit += 1
    return jnp.where(flat < total, val, nr * LANES * 32768), own, total


def gather_kernel(chunks, cand_ref, targ_ref, table_ref, out_ref, list_ref, cnt_ref, ids_ref, stage, tab, dense, plist, packed_rows, sem, psem, osem):
    rows = tab.shape[0]
    npos = out_ref.shape[0]
    cr = rows // chunks

    def load(c):
        return pltpu.make_async_copy(table_ref.at[pl.ds(c * cr, cr), :], stage.at[pl.ds(c * cr, cr), :], sem.at[c])

    for c in range(chunks):
        load(c).start()
    parts, sub, _ = targ_ref.shape
    n_head = cand_ref.shape[0]
    head = n_head * LANES
    ids_ref[:n_head, :] = cand_ref[...]
    for d in range(parts):
        ids_ref[n_head + d * sub:n_head + (d + 1) * sub, :] = targ_ref[d]
    packed, own, total = compact(ids_ref[...] - lax.axis_index("dp") * rows, rows, parts, head)
    list_ref[...] = packed
    cnt_ref[0] = jnp.sum(own[:head // LANES]).astype(I32)
    cnt_ref[1] = total
    to_smem = pltpu.make_async_copy(list_ref, plist, psem)
    to_smem.start()

    def zero(i, _):
        dense[pl.ds(pl.multiple_of(i * BLK, BLK), BLK), :] = jnp.zeros((BLK, LANES), F32)
        return 0

    lax.fori_loop(0, npos // BLK, zero, 0)
    for c in range(chunks):
        load(c).wait()

        def conv(i, _, c=c):
            s = pl.ds(pl.multiple_of(c * cr + i * BLK, BLK), BLK)
            tab[s, :] = stage[s, :].astype(F32)
            return 0

        lax.fori_loop(0, cr // BLK, conv, 0)
    to_smem.wait()

    def pick(i, _):
        vals = []
        for u in range(LANES):
            w = plist[i, u]
            vals.append((w >> 15, tab[pl.ds(w & 32767, 1), :]))
        for p, v in vals:
            dense[pl.ds(p, 1), :] = v
        return 0

    lax.fori_loop(0, (total + LANES - 1) // LANES, pick, 0)

    part = npos // parts

    def leave(d):
        s = pl.ds(d * part, part)
        return pltpu.make_async_copy(packed_rows.at[s, :], out_ref.at[s, :], osem.at[d])

    for d in range(parts):
        packed_rows[pl.ds(d * part, part), :] = dense[pl.ds(d * part, part), :].astype(BF)
        leave(d).start()
    for d in range(parts):
        leave(d).wait()


def gather(table, cand, targ):
    rows = table.shape[0]
    nr = cand.shape[0] + targ.shape[0] * targ.shape[1]
    npos = nr * LANES
    chunks = 8
    return pl.pallas_call(
        functools.partial(gather_kernel, chunks),
        out_shape=(jax.ShapeDtypeStruct((npos, LANES), BF), jax.ShapeDtypeStruct((nr, LANES), I32), jax.ShapeDtypeStruct((2,), I32)),
        in_specs=[VM, VM, HB],
        out_specs=(HB, VM, SM),
        scratch_shapes=[pltpu.VMEM((nr, LANES), I32), pltpu.VMEM((rows, LANES), BF), pltpu.VMEM((rows, LANES), F32), pltpu.VMEM((npos + 8, LANES), F32), pltpu.SMEM((nr, LANES), I32), pltpu.VMEM((npos, LANES), BF), pltpu.SemaphoreType.DMA((chunks,)), pltpu.SemaphoreType.DMA, pltpu.SemaphoreType.DMA((targ.shape[0],))],
        compiler_params=pltpu.CompilerParams(vmem_limit_bytes=VMEM_CAP),
        name="gather_rows",
    )(cand, targ, table)


ADDS = 4


def scatter_kernel(chunks, cnt_ref, list_ref, grad_ref, *refs):
    n = (len(refs) - 10) // 3
    passed, (out_ref, loss_ref, *refs) = refs[:n], refs[n:]
    kept, held, (acc, raw, grad, plist, sem, psem, gsem, isem, osem) = refs[:n - 1], refs[n - 1:2 * n - 1], refs[2 * n - 1:]
    parts = gsem.shape[0]
    part = grad_ref.shape[0] // parts

    def arrive(d):
        s = pl.ds(d * part, part)
        return pltpu.make_async_copy(grad_ref.at[s, :], raw.at[s, :], gsem.at[d])

    for d in range(parts):
        arrive(d).start()
    ins = [pltpu.make_async_copy(src, dst, isem.at[i]) for i, (src, dst) in enumerate(zip(passed, held))]
    outs = [pltpu.make_async_copy(src, dst, osem.at[i]) for i, (src, dst) in enumerate(zip(held[:-1], kept))]
    for c in ins:
        c.start()
    rows = out_ref.shape[0]
    npos = grad_ref.shape[0]
    to_smem = pltpu.make_async_copy(list_ref, plist, psem)
    to_smem.start()

    def zero(i, _):
        acc[pl.ds(pl.multiple_of(i * BLK, BLK), BLK), :] = jnp.zeros((BLK, LANES), F32)
        return 0

    lax.fori_loop(0, rows // BLK, zero, 0)

    for d in range(parts):
        arrive(d).wait()
        s = pl.ds(d * part, part)
        grad[s, :] = raw[s, :].astype(F32)
    for i in ins:
        i.wait()
    for o in outs:
        o.start()
    loss_ref[0] = jnp.sum(held[-1][0:1, 0:1])
    grad[npos:, :] = jnp.zeros((8, LANES), F32)
    to_smem.wait()
    nhead = cnt_ref[0]
    total = cnt_ref[1]

    def put(i, _):
        vals = []
        for u in range(LANES):
            w = plist[i, u]
            vals.append((w & 32767, grad[pl.ds(w >> 15, 1), :]))
        for r, v in vals:
            acc[pl.ds(r, 1), :] = v
        return 0

    lax.fori_loop(0, nhead // LANES, put, 0)

    def add_one(i, _):
        w = plist[i >> 7, i & 127]
        r = pl.ds(w & 32767, 1)
        acc[r, :] = acc[r, :] + grad[pl.ds(w >> 15, 1), :]
        return 0

    def add_row(i, _):
        for j in range(0, LANES, ADDS):
            words = [plist[i, j + u] for u in range(ADDS)]
            rs = [w & 32767 for w in words]
            gs = [grad[pl.ds(w >> 15, 1), :] for w in words]
            outs = []
            for u in range(ADDS):
                v = acc[pl.ds(rs[u], 1), :] + gs[u]
                for t in range(u):
                    v = v + jnp.where(rs[t] == rs[u], gs[t], 0.0)
                outs.append(v)
            for u in range(ADDS):
                acc[pl.ds(rs[u], 1), :] = outs[u]
        return 0

    begin = nhead // LANES * LANES
    split = jnp.minimum((nhead + LANES - 1) // LANES * LANES, total)
    lax.fori_loop(begin, split, add_one, 0)
    lax.fori_loop((split + LANES - 1) // LANES, (total + LANES - 1) // LANES, add_row, 0)
    cr = rows // chunks

    def store(c):
        return pltpu.make_async_copy(acc.at[pl.ds(c * cr, cr), :], out_ref.at[pl.ds(c * cr, cr), :], sem.at[c])

    for c in range(chunks):
        store(c).start()
    for c in range(chunks):
        store(c).wait()
    for o in outs:
        o.wait()


def scatter(grads, plist, counts, rows, passed, parts):
    nr = plist.shape[0]
    npos = nr * LANES
    chunks = 8
    n = len(passed)
    dma = pltpu.SemaphoreType.DMA
    return pl.pallas_call(
        functools.partial(scatter_kernel, chunks),
        out_shape=(jax.ShapeDtypeStruct((rows, LANES), F32), jax.ShapeDtypeStruct((1,), F32)) + tuple(jax.ShapeDtypeStruct(p.shape, p.dtype) for p in passed[:-1]),
        in_specs=[SM, HB, HB] + [HB] * n,
        out_specs=(HB, SM) + (HB,) * (n - 1),
        scratch_shapes=[pltpu.VMEM(p.shape, p.dtype) for p in passed]
        + [pltpu.VMEM((rows, LANES), F32), pltpu.VMEM((npos, LANES), BF), pltpu.VMEM((npos + 8, LANES), F32), pltpu.SMEM((nr, LANES), I32), dma((chunks,)), dma, dma((parts,)), dma((n,)), dma((n,))],
        compiler_params=pltpu.CompilerParams(vmem_limit_bytes=VMEM_CAP),
        name="scatter_rows",
    )(counts, plist, grads, *passed)


MESHID = pl.DeviceIdType.MESH
CHIP_DIMS = (1, 2, 4)
SLOTS = tuple(range(8))
CORE_ORDER = (7, 3, 5, 6, 1, 2, 4, 0)
RS_BASE = (0, 4, 6)


def place():
    me = lax.axis_index("dp")
    core = lax.rem(me, 2)
    chip = me // 2
    sign = {d: 1 - 2 * lax.rem(chip // d, 2) for d in CHIP_DIMS}
    return me, core, chip, sign


def chip_at(chip, sign, s):
    for d in CHIP_DIMS:
        if s & d:
            chip = chip + d * sign[d]
    return chip


def enter(peers):
    barrier = pltpu.get_barrier_semaphore()
    for peer in peers:
        pl.semaphore_signal(barrier, inc=1, device_id=(peer,), device_id_type=MESHID)
    pl.semaphore_wait(barrier, len(peers))


def order_of(k):
    return tuple(CHIP_DIMS[(k + i) % 3] for i in range(3))


def thirds(rows, unit, first=0):
    base = rows // unit
    cuts = [(base * i // 3) * unit for i in range(4)]
    return [(0, first + cuts[i], cuts[i + 1] - cuts[i], i) for i in range(3)]


def remote(src, dst, send, recv, peer):
    return pltpu.make_async_remote_copy(src_ref=src, dst_ref=dst, send_sem=send, recv_sem=recv, device_id=(peer,), device_id_type=MESHID)


def stage_slots(order, t):
    dims = order_of(order)
    live = [s for s in SLOTS if all(not s & d for d in dims[:t])]
    return [(s, s ^ dims[t]) for s in live if s & dims[t]]


def rs_scratch(arrays, num):
    out = []
    for rows, width, dtype in arrays:
        out += [pltpu.VMEM((8, rows, width), dtype), pltpu.VMEM((8, rows, width), dtype), pltpu.VMEM((7, rows, width), dtype)]
    n = len(arrays)
    dma = pltpu.SemaphoreType.DMA
    return out + [dma((n, 8)), dma((n, 8)), dma((num, 7)), dma((num, 7))]


def reduce_scatter_steps(get, pieces, scratch, mine=None, produce=None, fine=False):
    csend_s, crecv_s, send_s, recv_s = scratch[-4:]
    me, core, chip, sign = place()
    other = me + 1 - 2 * core
    num = len(pieces)
    arrays = range((len(scratch) - 4) // 3)
    crecv, acc, recv = ([scratch[3 * a + i] for a in arrays] for i in range(3))
    started = []

    def core_copy(s, a):
        return remote(get(2 * chip_at(chip, sign, s) + 1 - core, a), crecv[a].at[s], csend_s.at[a, s], crecv_s.at[a, s], other)

    def ici_copy(k, t, i, s):
        a, off, ln, order = pieces[k]
        slot = RS_BASE[t] + i
        peer = 2 * chip_at(chip, sign, order_of(order)[t]) + core
        return remote(acc[a].at[s, pl.ds(off, ln), :], recv[a].at[slot, pl.ds(off, ln), :], send_s.at[k, slot], recv_s.at[k, slot], peer)

    def go(c):
        c.start()
        started.append(c)

    def absorb(s):
        for a in arrays:
            core_copy(s, a).wait_recv()
            part = mine(s, a) if mine else get(2 * chip_at(chip, sign, s) + core, a)[...]
            acc[a][s] = part + crecv[a][s]
        for k in range(num):
            for i, (src, dst) in enumerate(stage_slots(pieces[k][3], 0)):
                if src == s:
                    go(ici_copy(k, 0, i, s))

    for n, s in enumerate(CORE_ORDER):
        if produce:
            produce(s)
        for a in arrays:
            go(core_copy(s, a))
        if produce and n:
            absorb(CORE_ORDER[n - 1])
    yield
    for s in CORE_ORDER[-1:] if produce else CORE_ORDER:
        absorb(s)
        if fine and s:
            yield
    yield
    for t in range(3):
        for i in reversed(range(4 >> t)):
            for k in range(num):
                a, off, ln, order = pieces[k]
                src, dst = stage_slots(order, t)[i]
                ici_copy(k, t, i, src).wait_recv()
                p = pl.ds(off, ln)
                acc[a][dst, p, :] = acc[a][dst, p, :] + recv[a][RS_BASE[t] + i, p, :]
                if t < 2:
                    for i2, (src2, dst2) in enumerate(stage_slots(order, t + 1)):
                        if src2 == dst:
                            go(ici_copy(k, t + 1, i2, dst))
        yield
    for c in started:
        c.wait_send()


def ag_scratch(num):
    return [pltpu.SemaphoreType.DMA((num, 8))] * 4


def all_gather_steps(own, out, pieces, scratch, landed=None):
    csend_s, crecv_s, send_s, recv_s = scratch
    me, core, chip, sign = place()
    other = me + 1 - 2 * core
    num = len(pieces)
    started = []

    def ref(k, s, c):
        a, off, ln, _ = pieces[k]
        return out(2 * chip_at(chip, sign, s) + c, a).at[pl.ds(off, ln), :]

    def source(k, s):
        a, off, ln, _ = pieces[k]
        return own(a).at[pl.ds(off, ln), :] if s == 0 else ref(k, s, core)

    def go(c):
        c.start()
        started.append(c)

    def core_send(k, s):
        go(remote(source(k, s), ref(k, s, core), csend_s.at[k, s], crecv_s.at[k, s], other))

    def send(k, t, s):
        d = order_of(pieces[k][3])[t]
        peer = 2 * chip_at(chip, sign, d) + core
        go(remote(source(k, s), ref(k, s, core), send_s.at[k, s ^ d], recv_s.at[k, s ^ d], peer))

    def arrive(k, s):
        there = ref(k, s, core)
        remote(there, there, send_s.at[k, s], recv_s.at[k, s], other).wait_recv()
        core_send(k, s)
        if landed:
            landed(k, s, 0)

    plan = (((), (0, 0)), ((), (1, 0)), ((), (2, 0)), ((1,), (1, 1)), ((), (2, 1)), ((2,), (2, 2)), ((3,), (2, 3)), ((4, 5, 6, 7), None))
    for i, (waits, sends) in enumerate(plan):
        for j in waits or (None,):
            for k in range(num):
                d = order_of(pieces[k][3])

                def slot(bits):
                    return sum(d[b] for b in range(3) if bits >> b & 1)

                if j is not None:
                    arrive(k, slot(j))
                if sends is not None:
                    send(k, sends[0], slot(sends[1]))
                if i == 0:
                    core_send(k, 0)
        yield
    for k in range(num):
        for s in SLOTS:
            there = ref(k, s, 1 - core)
            remote(there, there, csend_s.at[k, s], crecv_s.at[k, s], other).wait_recv()
            if landed:
                landed(k, s, 1)
    for c in started:
        c.wait_send()


def direct_scratch(rows, width):
    dma = pltpu.SemaphoreType.DMA
    return [pltpu.VMEM((8, rows, width), F32)] * 3 + [pltpu.VMEM((rows, width), F32), dma, dma, dma((8,)), dma((8,)), dma((8,)), dma((8,)), dma((8,)), dma((8,))]


def sum_direct_steps(src, out, scratch):
    crecv, acc, recv, tot, cs, cr, s1, r1, s2, r2, s3, r3 = scratch
    me, core, chip, sign = place()
    other = me + 1 - 2 * core
    first = remote(src.at[1 - core], crecv, cs, cr, other)
    first.start()
    yield
    first.wait_recv()
    acc[...] = src[core] + crecv[...]
    far = (7, 3, 5, 6, 1, 2, 4)

    def to(s):
        return 2 * chip_at(chip, sign, s) + core

    sends = [remote(acc.at[chip_at(chip, sign, s)], recv.at[s], s1.at[s], r1.at[s], to(s)) for s in far]
    for c in sends:
        c.start()
    yield
    for c in sends:
        c.wait_recv()
    total = acc[chip]
    for s in far:
        total = total + recv[s]
    tot[...] = total
    backs = [remote(tot, out.at[me], s2.at[s], r2.at[s], to(s)) for s in far]
    for c in backs:
        c.start()
    pair = [remote(tot, out.at[me], s3.at[0], r3.at[0], other)]
    pair[0].start()
    out[me] = total
    yield
    for s in reversed(far):
        there = out.at[to(s)]
        remote(there, there, s2.at[s], r2.at[s], other).wait_recv()
        c = remote(there, there, s3.at[s], r3.at[s], other)
        c.start()
        pair.append(c)
    yield
    for s in SLOTS:
        there = out.at[2 * chip_at(chip, sign, s) + 1 - core]
        remote(there, there, s3.at[s], r3.at[s], other).wait_recv()
    for c in [first] + sends + backs + pair:
        c.wait_send()


def drain(*steps):
    live = list(steps)
    while live:
        live = [g for g in live if next(g, StopIteration) is not StopIteration]


def kernel_call(body, name, cid, out_shape, scratch, *args, in_hbm=(), out_hbm=()):
    names = tuple(n for n, _ in scratch)

    def kernel(*refs):
        n = len(args) + len(jax.tree.leaves(out_shape))
        body(*refs[:n], dict(zip(names, refs[n:])))

    return pl.pallas_call(
        kernel,
        out_shape=out_shape,
        in_specs=[HB if i in in_hbm else VM for i in range(len(args))],
        out_specs=tuple(HB if i in out_hbm else VM for i in range(len(out_shape))),
        scratch_shapes=[s for _, s in scratch],
        compiler_params=pltpu.CompilerParams(collective_id=cid, has_side_effects=True, vmem_limit_bytes=VMEM_CAP),
        name=name,
    )(*args)


def grouped(name, items):
    return [(f"{name}.{i}", s) for i, s in enumerate(items)]


def group(scratch, name):
    return [v for k, v in scratch.items() if k.startswith(name + ".")]
LOG2E = 1.4426950408889634
GELU_C = math.sqrt(2.0 / math.pi)
GELU_A = 0.044715
ROW_BLK = 256
COL_BLK = 128


def gelu_both(x):
    x2 = x * x
    t = jnp.tanh(GELU_C * (x + GELU_A * (x2 * x)))
    half = 0.5 * (1.0 + t)
    return x * half, half + (0.5 * GELU_C) * x * (1.0 - t * t) * (1.0 + (3.0 * GELU_A) * x2)


def dot_nn(a, b):
    return jnp.dot(a, b, preferred_element_type=F32)


def dot_nt(a, b):
    return lax.dot_general(a, b, (((1,), (1,)), ((), ())), preferred_element_type=F32)


def turn(x):
    return x.astype(F32).T.astype(BF)


def tower_into(rows, load, w_in, w_out, slope_ref, hid_ref, out_ref, first=0):
    def blk(i, _):
        src = pl.ds(pl.multiple_of(i * ROW_BLK, ROW_BLK), ROW_BLK)
        s = pl.ds(pl.multiple_of(first + i * ROW_BLK, ROW_BLK), ROW_BLK)
        act, slope = gelu_both(dot_nn(load(src), w_in[...]))
        slope_ref[s, :] = slope
        hid_ref[s, :] = act.astype(BF)
        out_ref[s, :] = dot_nn(hid_ref[s, :], w_out[...]).astype(BF)
        return 0

    lax.fori_loop(0, rows // ROW_BLK, blk, 0)


def start_kernel(targ_ref, targ_out, v):
    me, core, chip, sign = place()
    peers = [2 * chip_at(chip, sign, s) + c for s in reversed(SLOTS) for c in ((core, 1 - core) if s else (1 - core,))]
    enter(peers)
    send_s, recv_s = v["sems.0"], v["sems.1"]
    targ_out[me] = targ_ref[...]
    copies = [remote(targ_ref, targ_out.at[me], send_s.at[i], recv_s.at[i], peer) for i, peer in enumerate(peers)]
    for c in copies:
        c.start()
    for c in copies:
        c.wait()


def start(targ, parts, cid):
    dma = pltpu.SemaphoreType.DMA
    outs = (jax.ShapeDtypeStruct((parts,) + targ.shape, I32),)
    return kernel_call(start_kernel, "start_step", cid, outs, grouped("sems", [dma((parts - 1,)), dma((parts - 1,))]), targ)[0]


def packed_grads(row_t, grad_t, pre_ref, hid_ref, loss, sums_ref):
    d_in = dot_nn(row_t, pre_ref[...])
    d_out = dot_nn(grad_t, hid_ref[...]).T
    parts = 2 * sums_ref.shape[1]
    n_in, n_out = d_in.shape[0] // parts, d_out.shape[0] // parts
    wide = d_in.shape[1] // LANES
    for dev in range(parts):
        part = sums_ref.at[dev % 2, dev // 2]
        for c in range(wide):
            part[c * n_in:(c + 1) * n_in, :] = d_in[dev * n_in:(dev + 1) * n_in, c * LANES:(c + 1) * LANES]
        part[wide * n_in:wide * n_in + n_out, :] = d_out[dev * n_out:(dev + 1) * n_out, :]
        part[wide * n_in + n_out:, :] = jnp.broadcast_to(loss if dev == 0 else 0.0 * loss, (8, LANES))


def unpack_grads(sums_ref, in_ref, out_ref, loss_ref):
    parts, n_in, width = in_ref.shape
    n_out = out_ref.shape[1]
    wide = width // LANES
    for dev in range(parts):
        for c in range(wide):
            in_ref[dev, :, c * LANES:(c + 1) * LANES] = sums_ref[dev, c * n_in:(c + 1) * n_in, :]
        out_ref[dev] = sums_ref[dev, wide * n_in:wide * n_in + n_out, :]
    loss_ref[...] = sums_ref[0, wide * n_in + n_out:, :]


def weight_grads(row_t, grad_t, pre_ref, hid_ref, in_ref, out_ref):
    parts, n_in, _ = in_ref.shape
    n_out = out_ref.shape[1]
    d_in = dot_nn(row_t, pre_ref[...])
    d_out = dot_nn(grad_t, hid_ref[...]).T
    for dev in range(parts):
        in_ref[dev] = d_in[dev * n_in:(dev + 1) * n_in, :]
        out_ref[dev] = d_out[dev * n_out:(dev + 1) * n_out, :]


def step_kernel(x_ref, *refs):
    (rows_out, *outs), v = refs[8:-1], refs[-1]
    ins = [pltpu.make_async_copy(src, v[f"in.{i}"], v["in_sem"].at[i]) for i, src in enumerate(refs[:8])]
    for c in ins:
        c.start()
    tok_ref, w1, w2, wi1, wi2, cand_ref, logq_ref, targ_ref = group(v, "in")
    di_in_out, di_out_out, dq_in_out, dq_out_out, loss_out = group(v, "out")
    leaves = [pltpu.make_async_copy(v[f"out.{i}"], dst, v["out_sem"].at[i]) for i, dst in enumerate(outs)]
    parts, n_item, _ = x_ref.shape
    n_tok = tok_ref.shape[0]
    n_cand = n_item - n_tok
    half = n_cand // 2
    total = float(n_tok * parts)
    scale = SCORE_GAIN / math.sqrt(LANES)
    me, core, chip, sign = place()
    x_chip = 2 * chip_at(chip, sign, 1)
    diag = 2 * chip_at(chip, sign, 6) + core
    rounds = ((me + 1 - 2 * core, x_chip + core, x_chip + 1 - core), (2 * chip_at(chip, sign, 2) + core, 2 * chip_at(chip, sign, 4) + core, diag))
    enter([me + 1 - 2 * core, x_chip + 1 - core] + [2 * chip_at(chip, sign, s) + core for s in SLOTS[1:]])
    x_mine, x_sem = v["x_mine"], v["x_sem"]

    def fetch(s):
        return pltpu.make_async_copy(x_ref.at[2 * chip_at(chip, sign, s) + core], x_mine.at[s], x_sem.at[s])

    fetched = set()

    def own_part(first, rows):
        def part(s, a):
            if s not in fetched:
                fetch(s).wait()
                fetched.add(s)
            return x_mine[s, pl.ds(first, rows), :]

        return part

    def row_sums(name, first, rows):
        p = pl.ds(first, rows)
        return reduce_scatter_steps(lambda dev, a: x_ref.at[dev, p, :], thirds(rows, 16), group(v, name), mine=own_part(first, rows), fine=True)

    rs_a, rs_b = row_sums("rsa", 0, half), row_sums("rsb", half, n_item - half)
    next(rs_a)
    next(rs_b)
    for s in CORE_ORDER:
        fetch(s).start()
    for c in ins[:3]:
        c.wait()
    tower_into(n_tok, lambda s: tok_ref[s, :], w1, w2, v["q_slope"], v["q_hid"], v["q_vec"])
    q_all = v["q_all"]
    q_all[me] = v["q_vec"][...]
    q_send, q_recv, q_csend, q_crecv = group(v, "agq")
    q_sent = []

    def q_tile(s, c):
        return q_all.at[2 * chip_at(chip, sign, s) + c]

    def q_go(s, d):
        src = v["q_vec"] if s == 0 else q_tile(s, core)
        if d:
            c = remote(src, q_tile(s, core), q_send.at[s ^ d], q_recv.at[s ^ d], 2 * chip_at(chip, sign, d) + core)
        else:
            c = remote(src, q_tile(s, core), q_csend.at[s], q_crecv.at[s], me + 1 - 2 * core)
        c.start()
        q_sent.append(c)

    def q_have(s, onward):
        remote(q_tile(s, core), q_tile(s, core), q_send.at[s], q_recv.at[s], me + 1 - 2 * core).wait_recv()
        for d in onward:
            q_go(s, d)
        q_go(s, 0)

    def q_other(s):
        there = q_tile(s, 1 - core)
        remote(there, there, q_csend.at[s], q_crecv.at[s], me + 1 - 2 * core).wait_recv()

    for d in (1, 2, 4, 0):
        q_go(0, d)
    for _ in range(8):
        next(rs_a)
    q_have(1, (2, 4))
    q_have(2, (4,))
    q_have(4, ())
    for c in ins[3:]:
        c.wait()
    n_sub = n_cand // LANES
    for r in range(n_sub):
        s = pl.ds(r * LANES, LANES)
        row = pl.ds(me * n_sub + r, 1)
        v["lq"][s, :] = jnp.broadcast_to(logq_ref[row, :] * LOG2E, (LANES, LANES)).T
        v["ids"][s, :] = jnp.broadcast_to(cand_ref[row, :].astype(F32), (LANES, LANES)).T
    for _ in range(2):
        next(rs_b)
    next(rs_a)
    for _ in range(6):
        next(rs_b)
    q_have(3, (4,))
    next(rs_a)
    for s in (5, 6, 7):
        q_have(s, ())
    next(rs_b)
    next(rs_a)
    raw_a, raw_b = v["rsa.1"].at[0], v["rsb.1"].at[0]
    tower_into(half, lambda s: raw_a[s, :], wi1, wi2, v["i_slope"], v["i_hid"], v["i_vec"])
    for s in SLOTS:
        q_other(s)
    next(rs_b)
    vec = v["i_vec"]
    z_ref, top_ref, den_ref, own_ref = v["z"], v["top"], v["den"], v["own"]
    def pass_one(t, first):
        q_t = q_all[t]
        row = pl.ds(t, 1)
        targ = jnp.concatenate([targ_ref[t, pl.ds(i, 1), :] for i in range(n_tok // LANES)], axis=1).astype(F32)
        if first:
            old_top, old_den, z_t = top_ref[row, :], den_ref[row, :], own_ref[row, :]
            top8 = jnp.broadcast_to(jnp.maximum(old_top, z_t), (8, n_tok))
        else:
            top8 = jnp.full((8, n_tok), -jnp.inf, F32)
        for j in range(half // COL_BLK):
            s = pl.ds(first + j * COL_BLK, COL_BLK)
            lq = jnp.concatenate([v["lq"][s, :]] * (n_tok // LANES), axis=1)
            ids = jnp.concatenate([v["ids"][s, :]] * (n_tok // LANES), axis=1)
            z = dot_nt(vec[s, :], q_t) * (scale * LOG2E) - lq
            z = jnp.where(ids == targ, HIT_VALUE * LOG2E, z)
            z_ref[t, s, :] = z
            top8 = jnp.maximum(top8, jnp.max(z.reshape(COL_BLK // 8, 8, n_tok), axis=0))
        top = jnp.max(top8, axis=0, keepdims=True)
        den8 = jnp.zeros((8, n_tok), F32)
        for j in range(half // COL_BLK):
            e = jnp.exp2(z_ref[t, pl.ds(first + j * COL_BLK, COL_BLK), :] - top)
            den8 = den8 + jnp.sum(e.reshape(COL_BLK // 8, 8, n_tok), axis=0)
        den = jnp.sum(den8, axis=0, keepdims=True)
        top_ref[row, :] = top
        den_ref[row, :] = den + old_den * jnp.exp2(old_top - top) + jnp.exp2(z_t - top) if first else den

    def lower(t, _):
        pass_one(t, 0)
        return 0

    def higher(t, _):
        pass_one(t, half)
        return 0

    lax.fori_loop(0, parts // 2, lower, 0)
    next(rs_b)
    lax.fori_loop(parts // 2, parts, lower, 0)
    tower_into(n_item - half, lambda s: raw_b[s, :], wi1, wi2, v["i_slope"], v["i_hid"], v["i_vec"], half)
    own = pl.ds(me, 1)
    targ_vec = vec[pl.ds(n_cand, n_tok), :]
    q_own = v["q_vec"][...]
    eye = lax.broadcasted_iota(I32, (n_tok, n_tok), 0) == lax.broadcasted_iota(I32, (n_tok, n_tok), 1)
    z_own = jnp.sum(jnp.where(eye, dot_nt(targ_vec, q_own), 0.0), axis=0, keepdims=True) * (scale * LOG2E)
    own_ref[...] = jnp.full(own_ref.shape, -jnp.inf, F32)
    own_ref[own, :] = z_own
    lax.fori_loop(0, parts, higher, 0)
    drain(rs_a, rs_b)
    for c in q_sent:
        c.wait_send()
    held, got, st_send, st_recv = group(v, "st")
    held[0, 0] = top_ref[...]
    held[0, 1] = den_ref[...]
    for r, peers in enumerate(rounds):
        copies = [remote(held.at[r], got.at[r, i], st_send.at[r, i], st_recv.at[r, i], peer) for i, peer in enumerate(peers)]
        for c in copies:
            c.start()
        for c in copies:
            c.wait()
        tops = [held[r, 0]] + [got[r, i, 0] for i in range(3)]
        dens = [held[r, 1]] + [got[r, i, 1] for i in range(3)]
        top = jnp.maximum(jnp.maximum(tops[0], tops[1]), jnp.maximum(tops[2], tops[3]))
        held[r + 1, 0] = top
        held[r + 1, 1] = sum(d * jnp.exp2(m - top) for m, d in zip(tops, dens))
    norm = v["norm"]
    norm[...] = held[2, 0] + jnp.log2(held[2, 1] * total)
    top_ref[...] = held[2, 0]
    den_ref[...] = held[2, 1]
    lse = top_ref[own, :] + jnp.log2(den_ref[own, :])
    loss = jnp.sum(lse - z_own, axis=1, keepdims=True) * (1.0 / (LOG2E * total))
    dz_row = ((jnp.exp2(z_own - top_ref[own, :]) / den_ref[own, :] - 1.0) * (1.0 / total)).astype(BF).astype(F32)
    dz_col = jnp.sum(jnp.where(eye, dz_row, 0.0), axis=1, keepdims=True)
    grad = v["i_grad"]
    grad[pl.ds(n_cand, n_tok), :] = (scale * dz_col * q_own.astype(F32)).astype(BF)
    i_pre, i_slope = v["i_pre"], v["i_slope"]
    rows_v, row_sem = v["rows"], v["row_sem"]
    mine = rows_v.at[me]

    def item_back(first, rows):
        for r in range(first, first + rows, ROW_BLK):
            s = pl.ds(r, ROW_BLK)
            i_pre[s, :] = (i_slope[s, :] * dot_nt(grad[s, :], wi2[...])).astype(BF)
            mine[s, :] = dot_nt(i_pre[s, :], wi1[...]).astype(BF)

    def send_back(n, first, rows):
        cuts = thirds(rows, 16, first)

        def leave(k, s, o):
            dev = 2 * chip_at(chip, sign, s) + (1 - core if o else core)
            p = pl.ds(cuts[k][1], cuts[k][2])
            return pltpu.make_async_copy(rows_v.at[dev, p, :], rows_out.at[dev, p, :], row_sem.at[3 * n + k, s, o])

        for k in range(3):
            leave(k, 0, 0).start()
        yield from all_gather_steps(lambda a: mine, lambda dev, a: rows_v.at[dev], cuts, group(v, f"agr{n}"), landed=lambda k, s, o: leave(k, s, o).start())
        for k in range(3):
            for s in SLOTS:
                for o in range(2):
                    leave(k, s, o).wait()

    item_back(n_cand, n_tok)
    back_t = send_back(0, n_cand, n_tok)
    for _ in range(3):
        next(back_t)
    vec_t = v["vec_t"]
    vec_t[...] = turn(vec[:n_cand, :])
    d_acc, dz_s, dh = v["d_acc"], v["dz"], v["dh"]
    d_acc[...] = jnp.zeros_like(d_acc)
    def pass_two(t, first):
        shift = norm[pl.ds(t, 1), :]
        for j in range(half // COL_BLK):
            dz_s[pl.ds(j * COL_BLK, COL_BLK), :] = jnp.exp2(z_ref[t, pl.ds(first + j * COL_BLK, COL_BLK), :] - shift).astype(BF)
        d_acc[pl.ds(first, half), :] += dot_nn(dz_s[...], q_all[t])
        part = dot_nn(vec_t[:, first:first + half], dz_s[...])
        dh[t] = part if first == 0 else dh[t] + part

    def upper_half(t, _):
        pass_two(t, 0)
        return 0

    def cand_back(first):
        grad[pl.ds(first, half), :] = (d_acc[pl.ds(first, half), :] * scale).astype(BF)
        item_back(first, half)

    lax.fori_loop(0, parts // 2, upper_half, 0)
    next(back_t)
    next(back_t)
    lax.fori_loop(parts // 2, parts, upper_half, 0)
    next(back_t)
    cand_back(0)
    next(back_t)
    back_a = send_back(1, 0, half)
    for _ in range(3):
        next(back_a)

    def both(s):
        def one(c, _):
            pass_two(2 * chip_at(chip, sign, s) + c, half)
            return 0

        lax.fori_loop(0, 2, one, 0)

    rs_dh = reduce_scatter_steps(lambda dev, a: dh.at[dev], thirds(LANES, 8), group(v, "rsd"), produce=both)
    next(rs_dh)
    next(back_a)
    next(rs_dh)
    cand_back(half)
    next(rs_dh)
    next(back_a)
    next(back_t)
    back_b = send_back(2, half, half)
    next(back_b)
    weight_grads(turn(jnp.concatenate([raw_a[...], raw_b[...]])), turn(grad[...]), i_pre, v["i_hid"], v["di_in"], v["di_out"])
    next(rs_dh)
    next(back_a)
    next(back_b)

    def sum_all(name, parts_in, orders, outs):
        pieces = [(a, 0, r.shape[1], o) for a, (r, o) in enumerate(zip(parts_in, orders))]
        refs = group(v, name)
        sums = [refs[3 * a + 1].at[0] for a in range(len(parts_in))]
        first = reduce_scatter_steps(lambda dev, a: parts_in[a].at[dev], pieces, refs[:-4])
        yield from (x for _, x in zip(range(5), first))
        for a, out in enumerate(outs):
            out[me] = sums[a][...]
        yield from all_gather_steps(lambda a: sums[a], lambda dev, a: outs[a].at[dev], pieces, refs[-4:])
        for _ in first:
            pass

    ar_i = sum_all("ai", (v["di_in"], v["di_out"]), (0, 1), (di_in_out, di_out_out))
    next(ar_i)
    next(rs_dh)
    d_query = ((dz_col * targ_vec.astype(F32) + v["rsd.1"][0].T) * scale).astype(BF)
    q_pre = v["q_pre"]
    q_pre[...] = (v["q_slope"][...] * dot_nt(d_query, w2[...])).astype(BF)
    packed_grads(turn(tok_ref[...]), turn(d_query), q_pre, v["q_hid"], loss, v["q_part"])
    ar_q = sum_direct_steps(v["q_part"], v["q_sum"], group(v, "aq"))
    drain(ar_q, ar_i, back_a, back_b, back_t, rs_dh)
    for c in leaves[:2]:
        c.start()
    unpack_grads(v["q_sum"], dq_in_out, dq_out_out, loss_out)
    for c in leaves[2:]:
        c.start()
    for c in leaves:
        c.wait()


def step(x, tokens, weights, cand, logq, targ, cid):
    parts, n_item, _ = x.shape
    n_tok = tokens.shape[0]
    n_cand = n_item - n_tok
    ff = weights[0].shape[1]
    dma = pltpu.SemaphoreType.DMA
    n_in, n_out = LANES // parts, ff // parts
    w_parts = [(n_in, ff, F32), (n_out, LANES, F32)]
    half = n_cand // 2
    spec = grouped("rsa", rs_scratch([(half, LANES, BF)], 3)) + grouped("rsb", rs_scratch([(n_item - half, LANES, BF)], 3))
    spec += grouped("st", [pltpu.VMEM((3, 2, parts, n_tok), F32), pltpu.VMEM((2, 3, 2, parts, n_tok), F32), dma((2, 3)), dma((2, 3))])
    spec += grouped("rsd", rs_scratch([(LANES, n_tok, F32)], 3))
    for n in range(3):
        spec += grouped(f"agr{n}", ag_scratch(3))
    spec += grouped("ai", rs_scratch(w_parts, 2) + ag_scratch(2))
    q_rows = n_in * (ff // LANES) + n_out + 8
    spec += grouped("aq", direct_scratch(q_rows, LANES))
    spec += grouped("agq", [dma((8,))] * 4)
    spec += [("x_sem", dma((8,))), ("row_sem", dma((9, 8, 2)))]

    def add(name, shape, dtype=F32):
        spec.append((name, pltpu.VMEM(shape, dtype)))

    for n, pre in ((n_tok, "q"), (n_item, "i")):
        add(pre + "_slope", (n, ff))
        add(pre + "_hid", (n, ff), BF)
        add(pre + "_pre", (n, ff), BF)
        add(pre + "_vec", (n, LANES), BF)
    add("i_grad", (n_item, LANES), BF)
    add("di_in", (parts, n_in, ff))
    add("di_out", (parts, n_out, LANES))
    add("q_part", (2, parts // 2, q_rows, LANES))
    add("q_sum", (parts, q_rows, LANES))
    add("x_mine", (8, n_item, LANES), BF)
    add("rows", (parts, n_item, LANES), BF)
    add("q_all", (parts, n_tok, LANES), BF)
    for name in ("lq", "ids", "d_acc"):
        add(name, (n_cand, LANES))
    add("z", (parts, n_cand, n_tok))
    for name in ("top", "den", "norm", "own"):
        add(name, (parts, n_tok))
    add("vec_t", (LANES, n_cand), BF)
    add("dz", (n_cand // 2, n_tok), BF)
    add("dh", (parts, LANES, n_tok))
    sums = (jax.ShapeDtypeStruct((parts, n_in, ff), F32), jax.ShapeDtypeStruct((parts, n_out, LANES), F32))
    outs = (jax.ShapeDtypeStruct((parts, n_item, LANES), BF),) + sums + sums + (jax.ShapeDtypeStruct((8, LANES), F32),)
    args = (tokens, *weights, cand, logq, targ)
    spec += grouped("in", [pltpu.VMEM(a.shape, a.dtype) for a in args]) + grouped("out", [pltpu.VMEM(o.shape, o.dtype) for o in outs[1:]])
    spec += [("in_sem", dma((8,))), ("out_sem", dma((5,)))]
    return kernel_call(step_kernel, "softmax_step", cid, outs, spec, x, *args, in_hbm=range(9), out_hbm=range(6))


def solution(mesh):
    num_dev = mesh.shape["dp"]

    def local_step(tokens, w_one, w_two, wi_one, wi_two, table_loc, cand_ids, log_q, targ_loc):
        rows_loc, dim = table_loc.shape
        n_item = cand_ids.shape[0] // num_dev + tokens.shape[0]
        cand = cand_ids.reshape(-1, LANES)
        targ = start(targ_loc.reshape(-1, LANES), num_dev, 1)
        owned, plist, counts = gather(table_loc, cand, targ)
        back, *sums = step(owned.reshape(num_dev, n_item, dim), tokens, (w_one, w_two, wi_one, wi_two), cand, log_q.reshape(-1, LANES), targ, 2)
        d_table, loss, di_in, di_out, dq_in, dq_out = scatter(back.reshape(-1, dim), plist, counts, rows_loc, sums, num_dev)
        shaped = [g.reshape(w.shape) for g, w in zip((dq_in, dq_out, di_in, di_out), (w_one, w_two, wi_one, wi_two))]
        return (loss.reshape(()), d_table) + tuple(shaped)

    return jax.shard_map(local_step, mesh=mesh, in_specs=(P("dp", None), P(), P(), P(), P(), P("dp", None), P(), P(), P("dp")), out_specs=(P(), P("dp", None), P(), P(), P(), P()), check_vma=False)
```

```python
import functools
import math
import jax
import jax.numpy as jnp
from jax import lax
from jax.experimental import pallas as pl
from jax.experimental.pallas import tpu as pltpu
from jax.sharding import PartitionSpec as P

SCORE_GAIN = 3.0
HIT_VALUE = -1e9
LANES = 128
VMEM_CAP = 60 * 1024 * 1024
BF = jnp.bfloat16
F32 = jnp.float32
I32 = jnp.int32
VM = pl.BlockSpec(memory_space=pltpu.VMEM)
SM = pl.BlockSpec(memory_space=pltpu.SMEM)
HB = pl.BlockSpec(memory_space=pl.ANY)
BLK = 256


def compact(loc, num_rows, parts, head):
    nr = loc.shape[0]
    own = jnp.where((loc >= 0) & (loc < num_rows), 1.0, 0.0)
    own16 = own.astype(BF)
    tri = jnp.where(lax.broadcasted_iota(I32, (LANES, LANES), 0) < lax.broadcasted_iota(I32, (LANES, LANES), 1), 1.0, 0.0).astype(BF)
    within = jnp.dot(own16, tri, preferred_element_type=F32)
    low = jnp.where(lax.broadcasted_iota(I32, (nr, nr), 1) < lax.broadcasted_iota(I32, (nr, nr), 0), 1.0, 0.0).astype(BF)
    before = jnp.sum(jnp.dot(low, own16, preferred_element_type=F32), axis=1, keepdims=True)
    lane = lax.broadcasted_iota(I32, (nr, LANES), 1)
    flat = lax.broadcasted_iota(I32, (nr, LANES), 0) * LANES + lane
    disp = flat - (within + before).astype(I32)
    n_head, n_tail = head // parts, (nr * LANES - head) // parts
    late = flat - head
    pos = jnp.where(flat < head, flat + flat // n_head * n_tail, late + (late // n_tail + 1) * n_head)
    val = jnp.where(own > 0, pos * 32768 + loc, -1)
    total = jnp.sum(own).astype(I32)

    def back(x, s):
        if s >= LANES:
            return pltpu.roll(x, nr - s // LANES, axis=0)
        here = pltpu.roll(x, LANES - s, axis=1)
        return jnp.where(lane < LANES - s, here, pltpu.roll(here, nr - 1, axis=0))

    bit = 0
    while (1 << bit) < nr * LANES:
        val_b, disp_b = back(val, 1 << bit), back(disp, 1 << bit)
        take = (val_b >= 0) & (((disp_b >> bit) & 1) == 1)
        stay = ((disp >> bit) & 1) == 0
        val = jnp.where(take, val_b, jnp.where(stay, val, -1))
        disp = jnp.where(take, disp_b, disp)
        bit += 1
    return jnp.where(flat < total, val, nr * LANES * 32768), own, total


def gather_kernel(chunks, cand_ref, targ_ref, table_ref, out_ref, list_ref, cnt_ref, ids_ref, stage, tab, dense, plist, packed_rows, sem, psem, osem):
    rows = tab.shape[0]
    npos = out_ref.shape[0]
    cr = rows // chunks

    def load(c):
        return pltpu.make_async_copy(table_ref.at[pl.ds(c * cr, cr), :], stage.at[pl.ds(c * cr, cr), :], sem.at[c])

    for c in range(chunks):
        load(c).start()
    parts, sub, _ = targ_ref.shape
    n_head = cand_ref.shape[0]
    head = n_head * LANES
    ids_ref[:n_head, :] = cand_ref[...]
    for d in range(parts):
        ids_ref[n_head + d * sub:n_head + (d + 1) * sub, :] = targ_ref[d]
    packed, own, total = compact(ids_ref[...] - lax.axis_index("dp") * rows, rows, parts, head)
    list_ref[...] = packed
    cnt_ref[0] = jnp.sum(own[:head // LANES]).astype(I32)
    cnt_ref[1] = total
    to_smem = pltpu.make_async_copy(list_ref, plist, psem)
    to_smem.start()

    def zero(i, _):
        dense[pl.ds(pl.multiple_of(i * BLK, BLK), BLK), :] = jnp.zeros((BLK, LANES), F32)
        return 0

    lax.fori_loop(0, npos // BLK, zero, 0)
    for c in range(chunks):
        load(c).wait()

        def conv(i, _, c=c):
            s = pl.ds(pl.multiple_of(c * cr + i * BLK, BLK), BLK)
            tab[s, :] = stage[s, :].astype(F32)
            return 0

        lax.fori_loop(0, cr // BLK, conv, 0)
    to_smem.wait()

    def pick(i, _):
        vals = []
        for u in range(LANES):
            w = plist[i, u]
            vals.append((w >> 15, tab[pl.ds(w & 32767, 1), :]))
        for p, v in vals:
            dense[pl.ds(p, 1), :] = v
        return 0

    lax.fori_loop(0, (total + LANES - 1) // LANES, pick, 0)

    part = npos // parts

    def leave(d):
        s = pl.ds(d * part, part)
        return pltpu.make_async_copy(packed_rows.at[s, :], out_ref.at[s, :], osem.at[d])

    for d in range(parts):
        packed_rows[pl.ds(d * part, part), :] = dense[pl.ds(d * part, part), :].astype(BF)
        leave(d).start()
    for d in range(parts):
        leave(d).wait()


def gather(table, cand, targ):
    rows = table.shape[0]
    nr = cand.shape[0] + targ.shape[0] * targ.shape[1]
    npos = nr * LANES
    chunks = 8
    return pl.pallas_call(
        functools.partial(gather_kernel, chunks),
        out_shape=(jax.ShapeDtypeStruct((npos, LANES), BF), jax.ShapeDtypeStruct((nr, LANES), I32), jax.ShapeDtypeStruct((2,), I32)),
        in_specs=[VM, VM, HB],
        out_specs=(HB, VM, SM),
        scratch_shapes=[pltpu.VMEM((nr, LANES), I32), pltpu.VMEM((rows, LANES), BF), pltpu.VMEM((rows, LANES), F32), pltpu.VMEM((npos + 8, LANES), F32), pltpu.SMEM((nr, LANES), I32), pltpu.VMEM((npos, LANES), BF), pltpu.SemaphoreType.DMA((chunks,)), pltpu.SemaphoreType.DMA, pltpu.SemaphoreType.DMA((targ.shape[0],))],
        compiler_params=pltpu.CompilerParams(vmem_limit_bytes=VMEM_CAP),
        name="gather_rows",
    )(cand, targ, table)


ADDS = 4


def scatter_kernel(chunks, cnt_ref, list_ref, grad_ref, *refs):
    n = (len(refs) - 10) // 3
    passed, (out_ref, loss_ref, *refs) = refs[:n], refs[n:]
    kept, held, (acc, raw, grad, plist, sem, psem, gsem, isem, osem) = refs[:n - 1], refs[n - 1:2 * n - 1], refs[2 * n - 1:]
    parts = gsem.shape[0]
    part = grad_ref.shape[0] // parts

    def arrive(d):
        s = pl.ds(d * part, part)
        return pltpu.make_async_copy(grad_ref.at[s, :], raw.at[s, :], gsem.at[d])

    for d in range(parts):
        arrive(d).start()
    ins = [pltpu.make_async_copy(src, dst, isem.at[i]) for i, (src, dst) in enumerate(zip(passed, held))]
    outs = [pltpu.make_async_copy(src, dst, osem.at[i]) for i, (src, dst) in enumerate(zip(held[:-1], kept))]
    for c in ins:
        c.start()
    rows = out_ref.shape[0]
    npos = grad_ref.shape[0]
    to_smem = pltpu.make_async_copy(list_ref, plist, psem)
    to_smem.start()

    def zero(i, _):
        acc[pl.ds(pl.multiple_of(i * BLK, BLK), BLK), :] = jnp.zeros((BLK, LANES), F32)
        return 0

    lax.fori_loop(0, rows // BLK, zero, 0)

    for d in range(parts):
        arrive(d).wait()
        s = pl.ds(d * part, part)
        grad[s, :] = raw[s, :].astype(F32)
    for i in ins:
        i.wait()
    for o in outs:
        o.start()
    loss_ref[0] = jnp.sum(held[-1][0:1, 0:1])
    grad[npos:, :] = jnp.zeros((8, LANES), F32)
    to_smem.wait()
    nhead = cnt_ref[0]
    total = cnt_ref[1]

    def put(i, _):
        vals = []
        for u in range(LANES):
            w = plist[i, u]
            vals.append((w & 32767, grad[pl.ds(w >> 15, 1), :]))
        for r, v in vals:
            acc[pl.ds(r, 1), :] = v
        return 0

    lax.fori_loop(0, nhead // LANES, put, 0)

    def add_one(i, _):
        w = plist[i >> 7, i & 127]
        r = pl.ds(w & 32767, 1)
        acc[r, :] = acc[r, :] + grad[pl.ds(w >> 15, 1), :]
        return 0

    def add_row(i, _):
        for j in range(0, LANES, ADDS):
            words = [plist[i, j + u] for u in range(ADDS)]
            rs = [w & 32767 for w in words]
            gs = [grad[pl.ds(w >> 15, 1), :] for w in words]
            outs = []
            for u in range(ADDS):
                v = acc[pl.ds(rs[u], 1), :] + gs[u]
                for t in range(u):
                    v = v + jnp.where(rs[t] == rs[u], gs[t], 0.0)
                outs.append(v)
            for u in range(ADDS):
                acc[pl.ds(rs[u], 1), :] = outs[u]
        return 0

    begin = nhead // LANES * LANES
    split = jnp.minimum((nhead + LANES - 1) // LANES * LANES, total)
    lax.fori_loop(begin, split, add_one, 0)
    lax.fori_loop((split + LANES - 1) // LANES, (total + LANES - 1) // LANES, add_row, 0)
    cr = rows // chunks

    def store(c):
        return pltpu.make_async_copy(acc.at[pl.ds(c * cr, cr), :], out_ref.at[pl.ds(c * cr, cr), :], sem.at[c])

    for c in range(chunks):
        store(c).start()
    for c in range(chunks):
        store(c).wait()
    for o in outs:
        o.wait()


def scatter(grads, plist, counts, rows, passed, parts):
    nr = plist.shape[0]
    npos = nr * LANES
    chunks = 8
    n = len(passed)
    dma = pltpu.SemaphoreType.DMA
    return pl.pallas_call(
        functools.partial(scatter_kernel, chunks),
        out_shape=(jax.ShapeDtypeStruct((rows, LANES), F32), jax.ShapeDtypeStruct((1,), F32)) + tuple(jax.ShapeDtypeStruct(p.shape, p.dtype) for p in passed[:-1]),
        in_specs=[SM, HB, HB] + [HB] * n,
        out_specs=(HB, SM) + (HB,) * (n - 1),
        scratch_shapes=[pltpu.VMEM(p.shape, p.dtype) for p in passed]
        + [pltpu.VMEM((rows, LANES), F32), pltpu.VMEM((npos, LANES), BF), pltpu.VMEM((npos + 8, LANES), F32), pltpu.SMEM((nr, LANES), I32), dma((chunks,)), dma, dma((parts,)), dma((n,)), dma((n,))],
        compiler_params=pltpu.CompilerParams(vmem_limit_bytes=VMEM_CAP),
        name="scatter_rows",
    )(counts, plist, grads, *passed)


MESHID = pl.DeviceIdType.MESH
CHIP_DIMS = (1, 2, 4)
SLOTS = tuple(range(8))
CORE_ORDER = (7, 3, 5, 6, 1, 2, 4, 0)
RS_BASE = (0, 4, 6)


def place():
    me = lax.axis_index("dp")
    core = lax.rem(me, 2)
    chip = me // 2
    sign = {d: 1 - 2 * lax.rem(chip // d, 2) for d in CHIP_DIMS}
    return me, core, chip, sign


def chip_at(chip, sign, s):
    for d in CHIP_DIMS:
        if s & d:
            chip = chip + d * sign[d]
    return chip


def locate():
    me, core, chip, sign = place()
    return me, core, 1 - core, chip, sign, lambda s, c: 2 * chip_at(chip, sign, s) + c


def enter(peers):
    barrier = pltpu.get_barrier_semaphore()
    for peer in peers:
        pl.semaphore_signal(barrier, inc=1, device_id=(peer,), device_id_type=MESHID)
    pl.semaphore_wait(barrier, len(peers))


def order_of(k):
    return tuple(CHIP_DIMS[(k + i) % 3] for i in range(3))


def thirds(rows, unit, first=0):
    base = rows // unit
    cuts = [(base * i // 3) * unit for i in range(4)]
    return [(0, first + cuts[i], cuts[i + 1] - cuts[i], i) for i in range(3)]


def remote(src, dst, send, recv, peer):
    return pltpu.make_async_remote_copy(src_ref=src, dst_ref=dst, send_sem=send, recv_sem=recv, device_id=(peer,), device_id_type=MESHID)


def stage_slots(order, t):
    dims = order_of(order)
    live = [s for s in SLOTS if all(not s & d for d in dims[:t])]
    return [(s, s ^ dims[t]) for s in live if s & dims[t]]


def rs_scratch(rows, width, dtype):
    dma = pltpu.SemaphoreType.DMA
    return [pltpu.VMEM((8, rows, width), dtype), pltpu.VMEM((8, rows, width), dtype), pltpu.VMEM((7, rows, width), dtype), dma, dma((8,)), dma, dma((7,))]


def reduce_scatter_steps(get, pieces, scratch, mine=None, produce=None):
    crecv, acc, recv, csend_s, crecv_s, send_s, recv_s = scratch
    me, core, away, chip, sign, at = locate()
    other = at(0, away)

    def core_copy(s):
        return remote(get(at(s, away)), crecv.at[s], csend_s, crecv_s.at[s], other)

    def send(k, t, i, s):
        _, off, ln, order = pieces[k]
        slot = RS_BASE[t] + i
        peer = at(order_of(order)[t], core)
        remote(acc.at[s, pl.ds(off, ln), :], recv.at[slot, pl.ds(off, ln), :], send_s, recv_s.at[slot], peer).start()

    def forward(k, t, s):
        for i, (src, _) in enumerate(stage_slots(pieces[k][3], t)):
            if src == s:
                send(k, t, i, s)

    def absorb(s):
        core_copy(s).wait_recv()
        acc[s] = (mine(s) if mine else get(at(s, core))[...]) + crecv[s]
        for k in range(3):
            forward(k, 0, s)

    for n, s in enumerate(CORE_ORDER):
        if produce:
            produce(s)
        core_copy(s).start()
        if produce and n:
            absorb(CORE_ORDER[n - 1])
    yield
    for s in CORE_ORDER[-1:] if produce else CORE_ORDER:
        absorb(s)
    yield
    for t in range(3):
        for i in reversed(range(4 >> t)):
            slot = RS_BASE[t] + i
            remote(recv.at[slot], recv.at[slot], send_s, recv_s.at[slot], other).wait_recv()
            for k in range(3):
                _, off, ln, order = pieces[k]
                dst = stage_slots(order, t)[i][1]
                p = pl.ds(off, ln)
                acc[dst, p, :] = acc[dst, p, :] + recv[slot, p, :]
                if t < 2:
                    forward(k, t + 1, dst)
        yield
    remote(crecv, crecv, csend_s, crecv_s.at[0], other).wait_send()
    remote(recv, recv, send_s, recv_s.at[0], other).wait_send()


def ag_scratch():
    dma = pltpu.SemaphoreType.DMA
    return [dma, dma, dma, dma((8,))]


def all_gather_steps(own, out, pieces, scratch, landed=None):
    csend_s, crecv_s, send_s, recv_s = scratch
    me, core, away, chip, sign, at = locate()
    other = at(0, away)
    begin = pieces[0][1]
    whole = pl.ds(begin, sum(p[2] for p in pieces))

    def device(s):
        return at(s, core)

    def slot(k, bits):
        d = order_of(pieces[k][3])
        return sum(d[b] for b in range(3) if bits >> b & 1)

    def ends(k, s):
        p = pl.ds(pieces[k][1], pieces[k][2])
        there = out.at[device(s), p, :]
        return (own.at[p, :] if s == 0 else there), there

    def core_send(k, s):
        src, there = ends(k, s)
        remote(src, there, csend_s, crecv_s, other).start()

    def send(k, t, bits):
        src, there = ends(k, slot(k, bits))
        remote(src, there, send_s, recv_s.at[bits | 1 << t], at(order_of(pieces[k][3])[t], core)).start()

    plan = (((), (0, 0)), ((), (1, 0)), ((), (2, 0)), ((1,), (1, 1)), ((), (2, 1)), ((2,), (2, 2)), ((3,), (2, 3)), ((4, 5, 6, 7), None))
    for n, (waits, step) in enumerate(plan):
        for bits in waits:
            remote(out.at[me, whole, :], out.at[me, whole, :], send_s, recv_s.at[bits], other).wait_recv()
            for k in range(len(pieces)):
                core_send(k, slot(k, bits))
                if landed:
                    landed(device(slot(k, bits)), pieces[k][1], pieces[k][2])
        for k in range(len(pieces)):
            if step:
                send(k, *step)
            if n == 0:
                core_send(k, 0)
        yield
    half = out.at[pl.ds(0, 8), whole, :]
    remote(half, half, csend_s, crecv_s, other).wait()
    sent = out.at[pl.ds(0, 7), whole, :]
    remote(sent, sent, send_s, recv_s.at[0], other).wait_send()
    if landed:
        for s in SLOTS:
            landed(at(s, away), begin, whole.size)


def direct_scratch(rows, width):
    dma = pltpu.SemaphoreType.DMA
    return [pltpu.VMEM((8, rows, width), F32)] * 3 + [pltpu.VMEM((rows, width), F32)] + [dma] * 8


def sum_direct_steps(src, out, scratch):
    crecv, acc, recv, tot, cs, cr, s1, r1, s2, r2, s3, r3 = scratch
    me, core, away, chip, sign, at = locate()
    other = at(0, away)
    first = remote(src.at[away], crecv, cs, cr, other)
    first.start()
    yield
    first.wait()
    acc[...] = src[core] + crecv[...]
    far = (7, 3, 5, 6, 1, 2, 4)

    def to(s):
        return at(s, core)

    for s in far:
        remote(acc.at[chip_at(chip, sign, s)], recv.at[s], s1, r1, to(s)).start()
    yield
    seven = recv.at[pl.ds(1, 7)]
    remote(seven, seven, s1, r1, other).wait()
    total = acc[chip]
    for s in far:
        total = total + recv[s]
    tot[...] = total
    for s in far:
        remote(tot, out.at[me], s2, r2, to(s)).start()
    remote(tot, out.at[me], s3, r3, other).start()
    out[me] = total
    yield
    seven = out.at[pl.ds(0, 7)]
    remote(seven, seven, s2, r2, other).wait()
    for s in far:
        remote(out.at[to(s)], out.at[to(s)], s3, r3, other).start()
    yield
    eight = out.at[pl.ds(0, 8)]
    remote(eight, eight, s3, r3, other).wait()


def drain(*steps):
    live = list(steps)
    while live:
        live = [g for g in live if next(g, StopIteration) is not StopIteration]


def kernel_call(body, name, cid, out_shape, scratch, *args, in_hbm=(), out_hbm=()):
    names = tuple(n for n, _ in scratch)

    def kernel(*refs):
        n = len(args) + len(jax.tree.leaves(out_shape))
        body(*refs[:n], dict(zip(names, refs[n:])))

    return pl.pallas_call(
        kernel,
        out_shape=out_shape,
        in_specs=[HB if i in in_hbm else VM for i in range(len(args))],
        out_specs=tuple(HB if i in out_hbm else VM for i in range(len(out_shape))),
        scratch_shapes=[s for _, s in scratch],
        compiler_params=pltpu.CompilerParams(collective_id=cid, has_side_effects=True, vmem_limit_bytes=VMEM_CAP),
        name=name,
    )(*args)


def grouped(name, items):
    return [(f"{name}.{i}", s) for i, s in enumerate(items)]


def group(scratch, name):
    return [v for k, v in scratch.items() if k.startswith(name + ".")]
LOG2E = 1.4426950408889634
GELU_C = math.sqrt(2.0 / math.pi)
GELU_A = 0.044715
ROW_BLK = 256
COL_BLK = 128


def gelu_both(x):
    x2 = x * x
    t = jnp.tanh(GELU_C * (x + GELU_A * (x2 * x)))
    half = 0.5 * (1.0 + t)
    return x * half, half + (0.5 * GELU_C) * x * (1.0 - t * t) * (1.0 + (3.0 * GELU_A) * x2)


def dot_nn(a, b):
    return jnp.dot(a, b, preferred_element_type=F32)


def dot_nt(a, b):
    return lax.dot_general(a, b, (((1,), (1,)), ((), ())), preferred_element_type=F32)


def turn(x):
    return x.astype(F32).T.astype(BF)


def tower_into(rows, load, w_in, w_out, slope_ref, hid_ref, out_ref):
    def blk(i, _):
        s = pl.ds(pl.multiple_of(i * ROW_BLK, ROW_BLK), ROW_BLK)
        act, slope = gelu_both(dot_nn(load(s), w_in[...]))
        slope_ref[s, :] = slope
        hid_ref[s, :] = act.astype(BF)
        out_ref[s, :] = dot_nn(hid_ref[s, :], w_out[...]).astype(BF)

        return 0

    lax.fori_loop(0, rows // ROW_BLK, blk, 0)


def start_kernel(targ_ref, targ_out, v):
    me, core, away, chip, sign, at = locate()
    peers = [at(s, c) for s in reversed(SLOTS) for c in ((core, away) if s else (away,))]
    enter(peers)
    send_s, recv_s = v["sems.0"], v["sems.1"]
    targ_out[me] = targ_ref[...]
    for peer in peers:
        remote(targ_ref, targ_out.at[me], send_s, recv_s, peer).start()
    most = targ_out.at[pl.ds(0, len(peers))]
    remote(most, most, send_s, recv_s, peers[-1]).wait()


def start(targ, parts, cid):
    dma = pltpu.SemaphoreType.DMA
    outs = (jax.ShapeDtypeStruct((parts,) + targ.shape, I32),)
    return kernel_call(start_kernel, "start_step", cid, outs, grouped("sems", [dma, dma]), targ)[0]


def packed_grads(row_t, grad_t, pre_ref, hid_ref, loss, part_of):
    d_in = dot_nn(row_t, pre_ref[...])
    d_out = dot_nn(grad_t, hid_ref[...]).T
    wide = d_in.shape[1] // LANES
    parts = 16
    n_in, n_out = d_in.shape[0] // parts, d_out.shape[0] // parts
    for dev in range(parts):
        part = part_of(dev)
        for c in range(wide):
            part[c * n_in:(c + 1) * n_in, :] = d_in[dev * n_in:(dev + 1) * n_in, c * LANES:(c + 1) * LANES]
        part[wide * n_in:wide * n_in + n_out, :] = d_out[dev * n_out:(dev + 1) * n_out, :]
        if loss is not None:
            part[wide * n_in + n_out:, :] = jnp.broadcast_to(loss if dev == 0 else 0.0 * loss, (8, LANES))


def unpack_grads(sums_ref, in_ref, out_ref, loss_ref):
    parts, n_in, width = in_ref.shape
    n_out = out_ref.shape[1]
    wide = width // LANES
    for dev in range(parts):
        for c in range(wide):
            in_ref[dev, :, c * LANES:(c + 1) * LANES] = sums_ref[dev, c * n_in:(c + 1) * n_in, :]
        out_ref[dev] = sums_ref[dev, wide * n_in:wide * n_in + n_out, :]
    if loss_ref is not None:
        loss_ref[...] = sums_ref[0, wide * n_in + n_out:, :]


def step_kernel(x_ref, *refs):
    (rows_out, *outs), v = refs[8:-1], refs[-1]
    ins = [pltpu.make_async_copy(src, v[f"in.{i}"], v["in_sem"].at[i]) for i, src in enumerate(refs[:8])]
    for c in ins:
        c.start()
    tok_ref, w1, w2, wi1, wi2, cand_ref, logq_ref, targ_ref = group(v, "in")
    di_in_out, di_out_out, dq_in_out, dq_out_out, loss_out = group(v, "out")
    leaves = [pltpu.make_async_copy(v[f"out.{i}"], dst, v["out_sem"].at[i]) for i, dst in enumerate(outs)]
    parts, n_item, _ = x_ref.shape
    n_tok = tok_ref.shape[0]
    n_cand = n_item - n_tok
    total = float(n_tok * parts)
    scale = SCORE_GAIN / math.sqrt(LANES)
    me, core, away, chip, sign, at = locate()
    other = at(0, away)
    diag = at(6, core)
    rounds = ((other, at(1, core), at(1, away)), (at(2, core), at(4, core), diag))
    enter([other, at(1, away)] + [at(s, core) for s in SLOTS[1:]])
    x_mine, x_sem = v["x_mine"], v["x_sem"]

    def fetch(s):
        return pltpu.make_async_copy(x_ref.at[at(s, core)], x_mine.at[s], x_sem.at[s])

    def own_part(s):
        fetch(s).wait()
        return x_mine[s]

    rs_rows = reduce_scatter_steps(lambda dev: x_ref.at[dev], thirds(n_item, 16), group(v, "rs"), mine=own_part)
    next(rs_rows)
    for s in CORE_ORDER:
        fetch(s).start()
    for c in ins[:3]:
        c.wait()
    tower_into(n_tok, lambda s: tok_ref[s, :], w1, w2, v["q_slope"], v["q_hid"], v["q_vec"])
    q_all = v["q_all"]
    q_all[me] = v["q_vec"][...]
    q_send, q_recv, q_csend, q_crecv = group(v, "agq")

    def q_tile(s, c):
        return q_all.at[at(s, c)]

    def q_go(s, d):
        src = v["q_vec"] if s == 0 else q_tile(s, core)
        if d:
            c = remote(src, q_tile(s, core), q_send, q_recv.at[s ^ d], at(d, core))
        else:
            c = remote(src, q_tile(s, core), q_csend, q_crecv.at[s // 4], other)
        c.start()

    def q_have(s, onward):
        remote(q_tile(s, core), q_tile(s, core), q_send, q_recv.at[s], other).wait_recv()
        for d in onward:
            q_go(s, d)
        q_go(s, 0)

    def q_other(upper):
        four = q_all.at[pl.ds(0, 4)]
        remote(four, four, q_csend, q_crecv.at[upper], other).wait_recv()

    for d in (1, 2, 4, 0):
        q_go(0, d)
    next(rs_rows)
    for c in ins[3:]:
        c.wait()
    n_sub = n_cand // LANES
    for r in range(n_sub):
        s = pl.ds(r * LANES, LANES)
        row = pl.ds(me * n_sub + r, 1)
        v["lq"][s, :] = jnp.broadcast_to(logq_ref[row, :] * LOG2E, (LANES, LANES)).T
        v["ids"][s, :] = jnp.broadcast_to(cand_ref[row, :].astype(F32), (LANES, LANES)).T
    drain(rs_rows)
    raw = v["rs.1"].at[0]
    q_have(1, (2, 4))
    q_have(2, (4,))
    q_have(4, ())
    tower_into(n_item, lambda s: raw[s, :], wi1, wi2, v["i_slope"], v["i_hid"], v["i_vec"])
    q_have(3, (4,))
    vec = v["i_vec"]
    z_ref, top_ref, den_ref, own_ref = v["z"], v["top"], v["den"], v["own"]
    own = pl.ds(me, 1)
    targ_vec = vec[pl.ds(n_cand, n_tok), :]
    q_own = v["q_vec"][...]
    eye = lax.broadcasted_iota(I32, (n_tok, n_tok), 0) == lax.broadcasted_iota(I32, (n_tok, n_tok), 1)
    z_own = jnp.sum(jnp.where(eye, dot_nt(targ_vec, q_own), 0.0), axis=0, keepdims=True) * (scale * LOG2E)
    own_ref[...] = jnp.full(own_ref.shape, -jnp.inf, F32)
    own_ref[own, :] = z_own

    def pass_one(i, upper):
        t = 2 * (chip + sign[1] * lax.rem(i // 2, 2) + 2 * sign[2] * (i // 4) + upper * 4 * sign[4]) + lax.rem(i, 2)
        q_t = q_all[t]
        targ = jnp.concatenate([targ_ref[t, pl.ds(i, 1), :] for i in range(n_tok // LANES)], axis=1).astype(F32)
        z_t = own_ref[pl.ds(t, 1), :]
        top8 = jnp.broadcast_to(z_t, (8, n_tok))
        for j in range(n_cand // COL_BLK):
            s = pl.ds(j * COL_BLK, COL_BLK)
            lq = jnp.concatenate([v["lq"][s, :]] * (n_tok // LANES), axis=1)
            ids = jnp.concatenate([v["ids"][s, :]] * (n_tok // LANES), axis=1)
            z = dot_nt(vec[s, :], q_t) * (scale * LOG2E) - lq
            z = jnp.where(ids == targ, HIT_VALUE * LOG2E, z)
            z_ref[t, s, :] = z
            top8 = jnp.maximum(top8, jnp.max(z.reshape(COL_BLK // 8, 8, n_tok), axis=0))
        top = jnp.max(top8, axis=0, keepdims=True)
        den8 = jnp.zeros((8, n_tok), F32)
        for j in range(n_cand // COL_BLK):
            e = jnp.exp2(z_ref[t, pl.ds(j * COL_BLK, COL_BLK), :] - top)
            den8 = den8 + jnp.sum(e.reshape(COL_BLK // 8, 8, n_tok), axis=0)
        top_ref[pl.ds(t, 1), :] = top
        den_ref[pl.ds(t, 1), :] = jnp.sum(den8, axis=0, keepdims=True) + jnp.exp2(z_t - top)
        return upper

    q_other(0)
    lax.fori_loop(0, parts // 2, pass_one, 0)
    for s in (5, 6, 7):
        q_have(s, ())
    q_other(1)
    lax.fori_loop(0, parts // 2, pass_one, 1)
    for sem, tiles in ((q_send, 7), (q_csend, 8)):
        some = q_all.at[pl.ds(0, tiles)]
        remote(some, some, sem, q_recv.at[0], other).wait_send()
    held, got, st_send, st_recv = group(v, "st")
    held[0, 0] = top_ref[...]
    held[0, 1] = den_ref[...]
    for r, peers in enumerate(rounds):
        for i, peer in enumerate(peers):
            remote(held.at[r], got.at[r, i], st_send.at[r], st_recv.at[r], peer).start()
        remote(got.at[r], got.at[r], st_send.at[r], st_recv.at[r], other).wait()
        tops = [held[r, 0]] + [got[r, i, 0] for i in range(3)]
        dens = [held[r, 1]] + [got[r, i, 1] for i in range(3)]
        top = jnp.maximum(jnp.maximum(tops[0], tops[1]), jnp.maximum(tops[2], tops[3]))
        held[r + 1, 0] = top
        held[r + 1, 1] = sum(d * jnp.exp2(m - top) for m, d in zip(tops, dens))
    norm = v["norm"]
    norm[...] = held[2, 0] + jnp.log2(held[2, 1] * total)
    top_ref[...] = held[2, 0]
    den_ref[...] = held[2, 1]
    lse = top_ref[own, :] + jnp.log2(den_ref[own, :])
    loss = jnp.sum(lse - z_own, axis=1, keepdims=True) * (1.0 / (LOG2E * total))
    dz_row = ((jnp.exp2(z_own - top_ref[own, :]) / den_ref[own, :] - 1.0) * (1.0 / total)).astype(BF).astype(F32)
    dz_col = jnp.sum(jnp.where(eye, dz_row, 0.0), axis=1, keepdims=True)
    grad = v["i_grad"]
    grad[pl.ds(n_cand, n_tok), :] = (scale * dz_col * q_own.astype(F32)).astype(BF)
    i_pre, i_slope = v["i_pre"], v["i_slope"]
    rows_v, row_sem = v["rows"], v["row_sem"]
    mine = rows_v.at[me]

    def item_back(first, rows):
        for r in range(first, first + rows, ROW_BLK):
            s = pl.ds(r, ROW_BLK)
            i_pre[s, :] = (i_slope[s, :] * dot_nt(grad[s, :], wi2[...])).astype(BF)
            mine[s, :] = dot_nt(i_pre[s, :], wi1[...]).astype(BF)

    def send_back(n, first, rows):
        p = pl.ds(first, rows)

        def leave(dev, begin, num):
            q = pl.ds(begin, num)
            pltpu.make_async_copy(rows_v.at[dev, q, :], rows_out.at[dev, q, :], row_sem.at[n]).start()

        leave(me, first, rows)
        yield from all_gather_steps(mine, rows_v, thirds(rows, 16, first), group(v, f"agr{n}"), leave)
        pltpu.make_async_copy(rows_v.at[:, p, :], rows_out.at[:, p, :], row_sem.at[n]).wait()

    item_back(n_cand, n_tok)
    back_t = send_back(0, n_cand, n_tok)
    for _ in range(3):
        next(back_t)
    vec_t = v["vec_t"]
    vec_t[...] = turn(vec[:n_cand, :])
    d_acc, dz_s, dh = v["d_acc"], v["dz"], v["dh"]
    d_acc[...] = jnp.zeros_like(d_acc)
    half = n_cand // 2

    def pass_two(t, first):
        shift = norm[pl.ds(t, 1), :]
        for j in range(half // COL_BLK):
            dz_s[pl.ds(j * COL_BLK, COL_BLK), :] = jnp.exp2(z_ref[t, pl.ds(first + j * COL_BLK, COL_BLK), :] - shift).astype(BF)
        d_acc[pl.ds(first, half), :] += dot_nn(dz_s[...], q_all[t])
        part = dot_nn(vec_t[:, first:first + half], dz_s[...])
        dh[t] = part if first == 0 else dh[t] + part

    def upper_half(t, _):
        pass_two(t, 0)
        return 0

    def cand_back(first):
        grad[pl.ds(first, half), :] = (d_acc[pl.ds(first, half), :] * scale).astype(BF)
        item_back(first, half)

    lax.fori_loop(0, parts // 2, upper_half, 0)
    next(back_t)
    next(back_t)
    lax.fori_loop(parts // 2, parts, upper_half, 0)
    next(back_t)
    cand_back(0)
    next(back_t)
    back_a = send_back(1, 0, half)
    for _ in range(3):
        next(back_a)

    def both(s):
        def one(c, _):
            pass_two(at(s, c), half)
            return 0

        lax.fori_loop(0, 2, one, 0)

    rs_dh = reduce_scatter_steps(lambda dev: dh.at[dev], thirds(LANES, 8), group(v, "rsd"), produce=both)
    next(rs_dh)
    next(back_a)
    next(rs_dh)
    cand_back(half)
    next(rs_dh)
    next(back_a)
    next(back_t)
    back_b = send_back(2, half, half)
    next(back_b)
    packed_grads(turn(raw[...]), turn(grad[...]), i_pre, v["i_hid"], None, lambda dev: v["i_part"].at[dev])
    next(rs_dh)
    next(back_a)
    next(back_b)

    def sum_items(part, out, refs):
        first = reduce_scatter_steps(lambda dev: part.at[dev], thirds(part.shape[1], 8), refs[:-4])
        for _ in range(5):
            next(first)
            yield
        tot = refs[1].at[0]
        out[me] = tot[...]
        yield from all_gather_steps(tot, out, thirds(part.shape[1], 8), refs[-4:])
        drain(first)

    ar_i = sum_items(v["i_part"], v["i_sum"], group(v, "ai"))
    next(ar_i)
    next(rs_dh)
    d_query = ((dz_col * targ_vec.astype(F32) + v["rsd.1"][0].T) * scale).astype(BF)
    q_pre = v["q_pre"]
    q_pre[...] = (v["q_slope"][...] * dot_nt(d_query, w2[...])).astype(BF)
    packed_grads(turn(tok_ref[...]), turn(d_query), q_pre, v["q_hid"], loss, lambda dev: v["q_part"].at[dev % 2, dev // 2])
    ar_q = sum_direct_steps(v["q_part"], v["q_sum"], group(v, "aq"))
    drain(ar_q, ar_i, back_a, back_b, back_t, rs_dh)
    unpack_grads(v["i_sum"], di_in_out, di_out_out, None)
    unpack_grads(v["q_sum"], dq_in_out, dq_out_out, loss_out)
    for c in leaves:
        c.start()
    for c in leaves:
        c.wait()


def step(x, tokens, weights, cand, logq, targ, cid):
    parts, n_item, _ = x.shape
    n_tok = tokens.shape[0]
    n_cand = n_item - n_tok
    ff = weights[0].shape[1]
    dma = pltpu.SemaphoreType.DMA
    n_in, n_out = LANES // parts, ff // parts
    spec = grouped("rs", rs_scratch(n_item, LANES, BF))
    spec += grouped("st", [pltpu.VMEM((3, 2, parts, n_tok), F32), pltpu.VMEM((2, 3, 2, parts, n_tok), F32), dma((2,)), dma((2,))])
    spec += grouped("rsd", rs_scratch(LANES, n_tok, F32))
    for n in range(3):
        spec += grouped(f"agr{n}", ag_scratch())
    i_rows = n_in * (ff // LANES) + n_out
    q_rows = i_rows + 8
    spec += grouped("ai", rs_scratch(i_rows, LANES, F32) + ag_scratch())
    spec += grouped("aq", direct_scratch(q_rows, LANES))
    spec += grouped("agq", [dma, dma((8,)), dma, dma((2,))])
    spec += [("x_sem", dma((8,))), ("row_sem", dma((3,)))]

    def add(name, shape, dtype=F32):
        spec.append((name, pltpu.VMEM(shape, dtype)))

    for n, pre in ((n_tok, "q"), (n_item, "i")):
        add(pre + "_slope", (n, ff))
        add(pre + "_hid", (n, ff), BF)
        add(pre + "_pre", (n, ff), BF)
        add(pre + "_vec", (n, LANES), BF)
    add("i_grad", (n_item, LANES), BF)
    add("i_part", (parts, i_rows, LANES))
    add("i_sum", (parts, i_rows, LANES))
    add("q_part", (2, parts // 2, q_rows, LANES))
    add("q_sum", (parts, q_rows, LANES))
    add("x_mine", (8, n_item, LANES), BF)
    add("rows", (parts, n_item, LANES), BF)
    add("q_all", (parts, n_tok, LANES), BF)
    for name in ("lq", "ids", "d_acc"):
        add(name, (n_cand, LANES))
    add("z", (parts, n_cand, n_tok))
    for name in ("top", "den", "norm", "own"):
        add(name, (parts, n_tok))
    add("vec_t", (LANES, n_cand), BF)
    add("dz", (n_cand // 2, n_tok), BF)
    add("dh", (parts, LANES, n_tok))
    sums = (jax.ShapeDtypeStruct((parts, n_in, ff), F32), jax.ShapeDtypeStruct((parts, n_out, LANES), F32))
    outs = (jax.ShapeDtypeStruct((parts, n_item, LANES), BF),) + sums + sums + (jax.ShapeDtypeStruct((8, LANES), F32),)
    args = (tokens, *weights, cand, logq, targ)
    spec += grouped("in", [pltpu.VMEM(a.shape, a.dtype) for a in args]) + grouped("out", [pltpu.VMEM(o.shape, o.dtype) for o in outs[1:]])
    spec += [("in_sem", dma((8,))), ("out_sem", dma((5,)))]
    return kernel_call(step_kernel, "softmax_step", cid, outs, spec, x, *args, in_hbm=range(9), out_hbm=range(6))


def solution(mesh):
    num_dev = mesh.shape["dp"]

    def local_step(tokens, w_one, w_two, wi_one, wi_two, table_loc, cand_ids, log_q, targ_loc):
        rows_loc, dim = table_loc.shape
        n_item = cand_ids.shape[0] // num_dev + tokens.shape[0]
        cand = cand_ids.reshape(-1, LANES)
        targ = start(targ_loc.reshape(-1, LANES), num_dev, 1)
        owned, plist, counts = gather(table_loc, cand, targ)
        back, *sums = step(owned.reshape(num_dev, n_item, dim), tokens, (w_one, w_two, wi_one, wi_two), cand, log_q.reshape(-1, LANES), targ, 2)
        d_table, loss, di_in, di_out, dq_in, dq_out = scatter(back.reshape(-1, dim), plist, counts, rows_loc, sums, num_dev)
        shaped = [g.reshape(w.shape) for g, w in zip((dq_in, dq_out, di_in, di_out), (w_one, w_two, wi_one, wi_two))]
        return (loss.reshape(()), d_table) + tuple(shaped)

    return jax.shard_map(local_step, mesh=mesh, in_specs=(P("dp", None), P(), P(), P(), P(), P("dp", None), P(), P(), P("dp")), out_specs=(P(), P("dp", None), P(), P(), P(), P()), check_vma=False)
```

```python
import functools
import math
import jax
import jax.numpy as jnp
from jax import lax
from jax.experimental import pallas as pl
from jax.experimental.pallas import tpu as pltpu
from jax.sharding import PartitionSpec as P

SCORE_GAIN = 3.0
HIT_VALUE = -1e9
LANES = 128
VMEM_CAP = 60 * 1024 * 1024
BF = jnp.bfloat16
F32 = jnp.float32
I32 = jnp.int32
VM = pl.BlockSpec(memory_space=pltpu.VMEM)
SM = pl.BlockSpec(memory_space=pltpu.SMEM)
HB = pl.BlockSpec(memory_space=pl.ANY)
BLK = 256


def compact(loc, num_rows, parts, head):
    nr = loc.shape[0]
    own = jnp.where((loc >= 0) & (loc < num_rows), 1.0, 0.0)
    own16 = own.astype(BF)
    tri = jnp.where(lax.broadcasted_iota(I32, (LANES, LANES), 0) < lax.broadcasted_iota(I32, (LANES, LANES), 1), 1.0, 0.0).astype(BF)
    within = jnp.dot(own16, tri, preferred_element_type=F32)
    low = jnp.where(lax.broadcasted_iota(I32, (nr, nr), 1) < lax.broadcasted_iota(I32, (nr, nr), 0), 1.0, 0.0).astype(BF)
    before = jnp.sum(jnp.dot(low, own16, preferred_element_type=F32), axis=1, keepdims=True)
    lane = lax.broadcasted_iota(I32, (nr, LANES), 1)
    flat = lax.broadcasted_iota(I32, (nr, LANES), 0) * LANES + lane
    disp = flat - (within + before).astype(I32)
    n_head, n_tail = head // parts, (nr * LANES - head) // parts
    late = flat - head
    pos = jnp.where(flat < head, flat + flat // n_head * n_tail, late + (late // n_tail + 1) * n_head)
    val = jnp.where(own > 0, pos * 32768 + loc, -1)
    total = jnp.sum(own).astype(I32)

    def back(x, s):
        if s >= LANES:
            return pltpu.roll(x, nr - s // LANES, axis=0)
        here = pltpu.roll(x, LANES - s, axis=1)
        return jnp.where(lane < LANES - s, here, pltpu.roll(here, nr - 1, axis=0))

    bit = 0
    while (1 << bit) < nr * LANES:
        val_b, disp_b = back(val, 1 << bit), back(disp, 1 << bit)
        take = (val_b >= 0) & (((disp_b >> bit) & 1) == 1)
        stay = ((disp >> bit) & 1) == 0
        val = jnp.where(take, val_b, jnp.where(stay, val, -1))
        disp = jnp.where(take, disp_b, disp)
        bit += 1
    return jnp.where(flat < total, val, nr * LANES * 32768), own, total


def gather_kernel(chunks, cand_ref, targ_ref, table_ref, out_ref, list_ref, cnt_ref, ids_ref, stage, tab, dense, plist, packed_rows, sem, psem, osem):
    rows = tab.shape[0]
    npos = out_ref.shape[0]
    cr = rows // chunks

    def load(c):
        return pltpu.make_async_copy(table_ref.at[pl.ds(c * cr, cr), :], stage.at[pl.ds(c * cr, cr), :], sem.at[c])

    for c in range(chunks):
        load(c).start()
    parts, sub, _ = targ_ref.shape
    n_head = cand_ref.shape[0]
    head = n_head * LANES
    ids_ref[:n_head, :] = cand_ref[...]
    for d in range(parts):
        ids_ref[n_head + d * sub:n_head + (d + 1) * sub, :] = targ_ref[d]
    packed, own, total = compact(ids_ref[...] - lax.axis_index("dp") * rows, rows, parts, head)
    list_ref[...] = packed
    cnt_ref[0] = jnp.sum(own[:head // LANES]).astype(I32)
    cnt_ref[1] = total
    to_smem = pltpu.make_async_copy(list_ref, plist, psem)
    to_smem.start()

    def zero(i, _):
        dense[pl.ds(pl.multiple_of(i * BLK, BLK), BLK), :] = jnp.zeros((BLK, LANES), F32)
        return 0

    lax.fori_loop(0, npos // BLK, zero, 0)
    for c in range(chunks):
        load(c).wait()

        def conv(i, _, c=c):
            s = pl.ds(pl.multiple_of(c * cr + i * BLK, BLK), BLK)
            tab[s, :] = stage[s, :].astype(F32)
            return 0

        lax.fori_loop(0, cr // BLK, conv, 0)
    to_smem.wait()

    def pick(i, _):
        vals = []
        for u in range(LANES):
            w = plist[i, u]
            vals.append((w >> 15, tab[pl.ds(w & 32767, 1), :]))
        for p, v in vals:
            dense[pl.ds(p, 1), :] = v
        return 0

    lax.fori_loop(0, (total + LANES - 1) // LANES, pick, 0)

    part = npos // parts

    def leave(d):
        s = pl.ds(d * part, part)
        return pltpu.make_async_copy(packed_rows.at[s, :], out_ref.at[s, :], osem.at[d])

    for d in range(parts):
        packed_rows[pl.ds(d * part, part), :] = dense[pl.ds(d * part, part), :].astype(BF)
        leave(d).start()
    for d in range(parts):
        leave(d).wait()


def gather(table, cand, targ):
    rows = table.shape[0]
    nr = cand.shape[0] + targ.shape[0] * targ.shape[1]
    npos = nr * LANES
    chunks = 8
    return pl.pallas_call(
        functools.partial(gather_kernel, chunks),
        out_shape=(jax.ShapeDtypeStruct((npos, LANES), BF), jax.ShapeDtypeStruct((nr, LANES), I32), jax.ShapeDtypeStruct((2,), I32)),
        in_specs=[VM, VM, HB],
        out_specs=(HB, VM, SM),
        scratch_shapes=[pltpu.VMEM((nr, LANES), I32), pltpu.VMEM((rows, LANES), BF), pltpu.VMEM((rows, LANES), F32), pltpu.VMEM((npos + 8, LANES), F32), pltpu.SMEM((nr, LANES), I32), pltpu.VMEM((npos, LANES), BF), pltpu.SemaphoreType.DMA((chunks,)), pltpu.SemaphoreType.DMA, pltpu.SemaphoreType.DMA((targ.shape[0],))],
        compiler_params=pltpu.CompilerParams(vmem_limit_bytes=VMEM_CAP),
        name="gather_rows",
    )(cand, targ, table)


ADDS = 4


def scatter_kernel(chunks, cnt_ref, list_ref, grad_ref, *refs):
    n = (len(refs) - 10) // 3
    passed, (out_ref, loss_ref, *refs) = refs[:n], refs[n:]
    kept, held, (acc, raw, grad, plist, sem, psem, gsem, isem, osem) = refs[:n - 1], refs[n - 1:2 * n - 1], refs[2 * n - 1:]
    parts = gsem.shape[0]
    part = grad_ref.shape[0] // parts

    def arrive(d):
        s = pl.ds(d * part, part)
        return pltpu.make_async_copy(grad_ref.at[s, :], raw.at[s, :], gsem.at[d])

    for d in range(parts):
        arrive(d).start()
    ins = [pltpu.make_async_copy(src, dst, isem.at[i]) for i, (src, dst) in enumerate(zip(passed, held))]
    outs = [pltpu.make_async_copy(src, dst, osem.at[i]) for i, (src, dst) in enumerate(zip(held[:-1], kept))]
    for c in ins:
        c.start()
    rows = out_ref.shape[0]
    npos = grad_ref.shape[0]
    to_smem = pltpu.make_async_copy(list_ref, plist, psem)
    to_smem.start()

    def zero(i, _):
        acc[pl.ds(pl.multiple_of(i * BLK, BLK), BLK), :] = jnp.zeros((BLK, LANES), F32)
        return 0

    lax.fori_loop(0, rows // BLK, zero, 0)

    for d in range(parts):
        arrive(d).wait()
        s = pl.ds(d * part, part)
        grad[s, :] = raw[s, :].astype(F32)
    for i in ins:
        i.wait()
    for o in outs:
        o.start()
    loss_ref[0] = jnp.sum(held[-1][0:1, 0:1])
    grad[npos:, :] = jnp.zeros((8, LANES), F32)
    to_smem.wait()
    nhead = cnt_ref[0]
    total = cnt_ref[1]

    def put(i, _):
        vals = []
        for u in range(LANES):
            w = plist[i, u]
            vals.append((w & 32767, grad[pl.ds(w >> 15, 1), :]))
        for r, v in vals:
            acc[pl.ds(r, 1), :] = v
        return 0

    lax.fori_loop(0, nhead // LANES, put, 0)

    def add_one(i, _):
        w = plist[i >> 7, i & 127]
        r = pl.ds(w & 32767, 1)
        acc[r, :] = acc[r, :] + grad[pl.ds(w >> 15, 1), :]
        return 0

    def add_row(i, _):
        for j in range(0, LANES, ADDS):
            words = [plist[i, j + u] for u in range(ADDS)]
            rs = [w & 32767 for w in words]
            gs = [grad[pl.ds(w >> 15, 1), :] for w in words]
            outs = []
            for u in range(ADDS):
                v = acc[pl.ds(rs[u], 1), :] + gs[u]
                for t in range(u):
                    v = v + jnp.where(rs[t] == rs[u], gs[t], 0.0)
                outs.append(v)
            for u in range(ADDS):
                acc[pl.ds(rs[u], 1), :] = outs[u]
        return 0

    begin = nhead // LANES * LANES
    split = jnp.minimum((nhead + LANES - 1) // LANES * LANES, total)
    lax.fori_loop(begin, split, add_one, 0)
    lax.fori_loop((split + LANES - 1) // LANES, (total + LANES - 1) // LANES, add_row, 0)
    cr = rows // chunks

    def store(c):
        return pltpu.make_async_copy(acc.at[pl.ds(c * cr, cr), :], out_ref.at[pl.ds(c * cr, cr), :], sem.at[c])

    for c in range(chunks):
        store(c).start()
    for c in range(chunks):
        store(c).wait()
    for o in outs:
        o.wait()


def scatter(grads, plist, counts, rows, passed, parts):
    nr = plist.shape[0]
    npos = nr * LANES
    chunks = 8
    n = len(passed)
    dma = pltpu.SemaphoreType.DMA
    return pl.pallas_call(
        functools.partial(scatter_kernel, chunks),
        out_shape=(jax.ShapeDtypeStruct((rows, LANES), F32), jax.ShapeDtypeStruct((1,), F32)) + tuple(jax.ShapeDtypeStruct(p.shape, p.dtype) for p in passed[:-1]),
        in_specs=[SM, HB, HB] + [HB] * n,
        out_specs=(HB, SM) + (HB,) * (n - 1),
        scratch_shapes=[pltpu.VMEM(p.shape, p.dtype) for p in passed]
        + [pltpu.VMEM((rows, LANES), F32), pltpu.VMEM((npos, LANES), BF), pltpu.VMEM((npos + 8, LANES), F32), pltpu.SMEM((nr, LANES), I32), dma((chunks,)), dma, dma((parts,)), dma((n,)), dma((n,))],
        compiler_params=pltpu.CompilerParams(vmem_limit_bytes=VMEM_CAP),
        name="scatter_rows",
    )(counts, plist, grads, *passed)


MESHID = pl.DeviceIdType.MESH
CHIP_DIMS = (1, 2, 4)
SLOTS = tuple(range(8))
CORE_ORDER = (7, 3, 5, 6, 1, 2, 4, 0)
RS_BASE = (0, 4, 6)


def place():
    me = lax.axis_index("dp")
    core = lax.rem(me, 2)
    chip = me // 2
    sign = {d: 1 - 2 * lax.rem(chip // d, 2) for d in CHIP_DIMS}
    return me, core, chip, sign


def chip_at(chip, sign, s):
    for d in CHIP_DIMS:
        if s & d:
            chip = chip + d * sign[d]
    return chip


def locate():
    me, core, chip, sign = place()
    return me, core, 1 - core, chip, sign, lambda s, c: 2 * chip_at(chip, sign, s) + c


def enter(peers):
    barrier = pltpu.get_barrier_semaphore()
    for peer in peers:
        pl.semaphore_signal(barrier, inc=1, device_id=(peer,), device_id_type=MESHID)
    pl.semaphore_wait(barrier, len(peers))


def order_of(k):
    return tuple(CHIP_DIMS[(k + i) % 3] for i in range(3))


def thirds(rows, unit, first=0):
    base = rows // unit
    cuts = [(base * i // 3) * unit for i in range(4)]
    return [(0, first + cuts[i], cuts[i + 1] - cuts[i], i) for i in range(3)]


def remote(src, dst, send, recv, peer):
    return pltpu.make_async_remote_copy(src_ref=src, dst_ref=dst, send_sem=send, recv_sem=recv, device_id=(peer,), device_id_type=MESHID)


def stage_slots(order, t):
    dims = order_of(order)
    live = [s for s in SLOTS if all(not s & d for d in dims[:t])]
    return [(s, s ^ dims[t]) for s in live if s & dims[t]]


def rs_scratch(rows, width, dtype):
    dma = pltpu.SemaphoreType.DMA
    return [pltpu.VMEM((8, rows, width), dtype), pltpu.VMEM((8, rows, width), dtype), pltpu.VMEM((7, rows, width), dtype), dma, dma((8,)), dma, dma((7,))]


def reduce_scatter_steps(get, pieces, scratch, mine=None, produce=None):
    crecv, acc, recv, csend_s, crecv_s, send_s, recv_s = scratch
    me, core, away, chip, sign, at = locate()
    other = at(0, away)

    def core_copy(s):
        return remote(get(at(s, away)), crecv.at[s], csend_s, crecv_s.at[s], other)

    def send(k, t, i, s):
        _, off, ln, order = pieces[k]
        slot = RS_BASE[t] + i
        peer = at(order_of(order)[t], core)
        remote(acc.at[s, pl.ds(off, ln), :], recv.at[slot, pl.ds(off, ln), :], send_s, recv_s.at[slot], peer).start()

    def forward(k, t, s):
        for i, (src, _) in enumerate(stage_slots(pieces[k][3], t)):
            if src == s:
                send(k, t, i, s)

    def absorb(s):
        core_copy(s).wait_recv()
        acc[s] = (mine(s) if mine else get(at(s, core))[...]) + crecv[s]
        for k in range(3):
            forward(k, 0, s)

    for n, s in enumerate(CORE_ORDER):
        if produce:
            produce(s)
        core_copy(s).start()
        if produce and n:
            absorb(CORE_ORDER[n - 1])
    yield
    for s in CORE_ORDER[-1:] if produce else CORE_ORDER:
        absorb(s)
    yield
    for t in range(3):
        for i in reversed(range(4 >> t)):
            slot = RS_BASE[t] + i
            remote(recv.at[slot], recv.at[slot], send_s, recv_s.at[slot], other).wait_recv()
            for k in range(3):
                _, off, ln, order = pieces[k]
                dst = stage_slots(order, t)[i][1]
                p = pl.ds(off, ln)
                acc[dst, p, :] = acc[dst, p, :] + recv[slot, p, :]
                if t < 2:
                    forward(k, t + 1, dst)
        yield
    remote(crecv, crecv, csend_s, crecv_s.at[0], other).wait_send()
    remote(recv, recv, send_s, recv_s.at[0], other).wait_send()


def ag_scratch():
    dma = pltpu.SemaphoreType.DMA
    return [dma, dma, dma, dma((8,))]


def all_gather_steps(own, out, pieces, scratch, landed=None):
    csend_s, crecv_s, send_s, recv_s = scratch
    me, core, away, chip, sign, at = locate()
    other = at(0, away)
    begin = pieces[0][1]
    whole = pl.ds(begin, sum(p[2] for p in pieces))

    def device(s):
        return at(s, core)

    def slot(k, bits):
        d = order_of(pieces[k][3])
        return sum(d[b] for b in range(3) if bits >> b & 1)

    def ends(k, s):
        p = pl.ds(pieces[k][1], pieces[k][2])
        there = out.at[device(s), p, :]
        return (own.at[p, :] if s == 0 else there), there

    def core_send(k, s):
        src, there = ends(k, s)
        remote(src, there, csend_s, crecv_s, other).start()

    def send(k, t, bits):
        src, there = ends(k, slot(k, bits))
        remote(src, there, send_s, recv_s.at[bits | 1 << t], at(order_of(pieces[k][3])[t], core)).start()

    plan = (((), (0, 0)), ((), (1, 0)), ((), (2, 0)), ((1,), (1, 1)), ((), (2, 1)), ((2,), (2, 2)), ((3,), (2, 3)), ((4, 5, 6, 7), None))
    for n, (waits, step) in enumerate(plan):
        for bits in waits:
            remote(out.at[me, whole, :], out.at[me, whole, :], send_s, recv_s.at[bits], other).wait_recv()
            for k in range(len(pieces)):
                core_send(k, slot(k, bits))
                if landed:
                    landed(device(slot(k, bits)), pieces[k][1], pieces[k][2])
        for k in range(len(pieces)):
            if step:
                send(k, *step)
            if n == 0:
                core_send(k, 0)
        yield
    half = out.at[pl.ds(0, 8), whole, :]
    remote(half, half, csend_s, crecv_s, other).wait()
    sent = out.at[pl.ds(0, 7), whole, :]
    remote(sent, sent, send_s, recv_s.at[0], other).wait_send()
    if landed:
        for s in SLOTS:
            landed(at(s, away), begin, whole.size)


def direct_scratch(rows, width):
    dma = pltpu.SemaphoreType.DMA
    return [pltpu.VMEM((8, rows, width), F32)] * 3 + [pltpu.VMEM((rows, width), F32)] + [dma] * 8


def sum_direct_steps(src, out, scratch):
    crecv, acc, recv, tot, cs, cr, s1, r1, s2, r2, s3, r3 = scratch
    me, core, away, chip, sign, at = locate()
    other = at(0, away)
    first = remote(src.at[away], crecv, cs, cr, other)
    first.start()
    yield
    first.wait()
    acc[...] = src[core] + crecv[...]
    far = (7, 3, 5, 6, 1, 2, 4)

    def to(s):
        return at(s, core)

    for s in far:
        remote(acc.at[chip_at(chip, sign, s)], recv.at[s], s1, r1, to(s)).start()
    yield
    seven = recv.at[pl.ds(1, 7)]
    remote(seven, seven, s1, r1, other).wait()
    total = acc[chip]
    for s in far:
        total = total + recv[s]
    tot[...] = total
    for s in far:
        remote(tot, out.at[me], s2, r2, to(s)).start()
    remote(tot, out.at[me], s3, r3, other).start()
    out[me] = total
    yield
    seven = out.at[pl.ds(0, 7)]
    remote(seven, seven, s2, r2, other).wait()
    for s in far:
        remote(out.at[to(s)], out.at[to(s)], s3, r3, other).start()
    yield
    eight = out.at[pl.ds(0, 8)]
    remote(eight, eight, s3, r3, other).wait()


def drain(*steps):
    live = list(steps)
    while live:
        live = [g for g in live if next(g, StopIteration) is not StopIteration]


def kernel_call(body, name, cid, out_shape, scratch, *args, in_hbm=(), out_hbm=()):
    names = tuple(n for n, _ in scratch)

    def kernel(*refs):
        n = len(args) + len(jax.tree.leaves(out_shape))
        body(*refs[:n], dict(zip(names, refs[n:])))

    return pl.pallas_call(
        kernel,
        out_shape=out_shape,
        in_specs=[HB if i in in_hbm else VM for i in range(len(args))],
        out_specs=tuple(HB if i in out_hbm else VM for i in range(len(out_shape))),
        scratch_shapes=[s for _, s in scratch],
        compiler_params=pltpu.CompilerParams(collective_id=cid, has_side_effects=True, vmem_limit_bytes=VMEM_CAP),
        name=name,
    )(*args)


def grouped(name, items):
    return [(f"{name}.{i}", s) for i, s in enumerate(items)]


def group(scratch, name):
    return [v for k, v in scratch.items() if k.startswith(name + ".")]
LOG2E = 1.4426950408889634
GELU_C = math.sqrt(2.0 / math.pi)
GELU_A = 0.044715
ROW_BLK = 256
COL_BLK = 128


def gelu_both(x):
    x2 = x * x
    t = jnp.tanh(GELU_C * (x + GELU_A * (x2 * x)))
    half = 0.5 * (1.0 + t)
    return x * half, half + (0.5 * GELU_C) * x * (1.0 - t * t) * (1.0 + (3.0 * GELU_A) * x2)


def dot_nn(a, b):
    return jnp.dot(a, b, preferred_element_type=F32)


def dot_nt(a, b):
    return lax.dot_general(a, b, (((1,), (1,)), ((), ())), preferred_element_type=F32)


def turn(x):
    return x.astype(F32).T.astype(BF)


def tower_into(rows, load, w_in, w_out, slope_ref, hid_ref, out_ref):
    def blk(i, _):
        s = pl.ds(pl.multiple_of(i * ROW_BLK, ROW_BLK), ROW_BLK)
        act, slope = gelu_both(dot_nn(load(s), w_in[...]))
        slope_ref[s, :] = slope
        hid_ref[s, :] = act.astype(BF)
        out_ref[s, :] = dot_nn(hid_ref[s, :], w_out[...]).astype(BF)

        return 0

    lax.fori_loop(0, rows // ROW_BLK, blk, 0)


def start_kernel(targ_ref, targ_out, v):
    me, core, away, chip, sign, at = locate()
    peers = [at(s, c) for s in reversed(SLOTS) for c in ((core, away) if s else (away,))]
    enter(peers)
    send_s, recv_s = v["sems.0"], v["sems.1"]
    targ_out[me] = targ_ref[...]
    for peer in peers:
        remote(targ_ref, targ_out.at[me], send_s, recv_s, peer).start()
    most = targ_out.at[pl.ds(0, len(peers))]
    remote(most, most, send_s, recv_s, peers[-1]).wait()


def start(targ, parts, cid):
    dma = pltpu.SemaphoreType.DMA
    outs = (jax.ShapeDtypeStruct((parts,) + targ.shape, I32),)
    return kernel_call(start_kernel, "start_step", cid, outs, grouped("sems", [dma, dma]), targ)[0]


def packed_grads(row_t, grad_t, pre_ref, hid_ref, loss, part_of):
    d_in = dot_nn(row_t, pre_ref[...])
    d_out = dot_nn(grad_t, hid_ref[...]).T
    wide = d_in.shape[1] // LANES
    parts = 16
    n_in, n_out = d_in.shape[0] // parts, d_out.shape[0] // parts
    for dev in range(parts):
        part = part_of(dev)
        for c in range(wide):
            part[c * n_in:(c + 1) * n_in, :] = d_in[dev * n_in:(dev + 1) * n_in, c * LANES:(c + 1) * LANES]
        part[wide * n_in:wide * n_in + n_out, :] = d_out[dev * n_out:(dev + 1) * n_out, :]
        if loss is not None:
            part[wide * n_in + n_out:, :] = jnp.broadcast_to(loss if dev == 0 else 0.0 * loss, (8, LANES))


def unpack_grads(sums_ref, in_ref, out_ref, loss_ref):
    parts, n_in, width = in_ref.shape
    n_out = out_ref.shape[1]
    wide = width // LANES
    for dev in range(parts):
        for c in range(wide):
            in_ref[dev, :, c * LANES:(c + 1) * LANES] = sums_ref[dev, c * n_in:(c + 1) * n_in, :]
        out_ref[dev] = sums_ref[dev, wide * n_in:wide * n_in + n_out, :]
    if loss_ref is not None:
        loss_ref[...] = sums_ref[0, wide * n_in + n_out:, :]


def step_kernel(x_ref, *refs):
    (rows_out, *outs), v = refs[8:-1], refs[-1]
    ins = [pltpu.make_async_copy(src, v[f"in.{i}"], v["in_sem"].at[i]) for i, src in enumerate(refs[:8])]
    for c in ins:
        c.start()
    tok_ref, w1, w2, wi1, wi2, cand_ref, logq_ref, targ_ref = group(v, "in")
    di_in_out, di_out_out, dq_in_out, dq_out_out, loss_out = group(v, "out")
    leaves = [pltpu.make_async_copy(v[f"out.{i}"], dst, v["out_sem"].at[i]) for i, dst in enumerate(outs)]
    parts, n_item, _ = x_ref.shape
    n_tok = tok_ref.shape[0]
    n_cand = n_item - n_tok
    total = float(n_tok * parts)
    scale = SCORE_GAIN / math.sqrt(LANES)
    me, core, away, chip, sign, at = locate()
    other = at(0, away)
    diag = at(6, core)
    rounds = ((other, at(1, core), at(1, away)), (at(2, core), at(4, core), diag))
    enter([other, at(1, away)] + [at(s, core) for s in SLOTS[1:]])
    x_mine, x_sem = v["x_mine"], v["x_sem"]

    def fetch(s):
        return pltpu.make_async_copy(x_ref.at[at(s, core)], x_mine.at[s], x_sem.at[s])

    def own_part(s):
        fetch(s).wait()
        return x_mine[s]

    rs_rows = reduce_scatter_steps(lambda dev: x_ref.at[dev], thirds(n_item, 16), group(v, "rs"), mine=own_part)
    next(rs_rows)
    for s in CORE_ORDER:
        fetch(s).start()
    for c in ins[:3]:
        c.wait()
    tower_into(n_tok, lambda s: tok_ref[s, :], w1, w2, v["q_slope"], v["q_hid"], v["q_vec"])
    q_all = v["q_all"]
    q_all[me] = v["q_vec"][...]
    q_send, q_recv, q_csend, q_crecv = group(v, "agq")

    def q_tile(s, c):
        return q_all.at[at(s, c)]

    def q_go(s, d):
        src = v["q_vec"] if s == 0 else q_tile(s, core)
        if d:
            c = remote(src, q_tile(s, core), q_send, q_recv.at[s ^ d], at(d, core))
        else:
            c = remote(src, q_tile(s, core), q_csend, q_crecv.at[s // 4], other)
        c.start()

    def q_have(s, onward):
        remote(q_tile(s, core), q_tile(s, core), q_send, q_recv.at[s], other).wait_recv()
        for d in onward:
            q_go(s, d)
        q_go(s, 0)

    def q_other(upper):
        four = q_all.at[pl.ds(0, 4)]
        remote(four, four, q_csend, q_crecv.at[upper], other).wait_recv()

    for d in (1, 2, 4, 0):
        q_go(0, d)
    next(rs_rows)
    for c in ins[3:]:
        c.wait()
    n_sub = n_cand // LANES
    for r in range(n_sub):
        s = pl.ds(r * LANES, LANES)
        row = pl.ds(me * n_sub + r, 1)
        v["lq"][s, :] = jnp.broadcast_to(logq_ref[row, :] * LOG2E, (LANES, LANES)).T
        v["ids"][s, :] = jnp.broadcast_to(cand_ref[row, :].astype(F32), (LANES, LANES)).T
    drain(rs_rows)
    raw = v["rs.1"].at[0]
    q_have(1, (2, 4))
    q_have(2, (4,))
    q_have(4, ())
    tower_into(n_item, lambda s: raw[s, :], wi1, wi2, v["i_slope"], v["i_hid"], v["i_vec"])
    q_have(3, (4,))
    vec = v["i_vec"]
    z_ref, top_ref, den_ref, own_ref = v["z"], v["top"], v["den"], v["own"]
    own = pl.ds(me, 1)
    targ_vec = vec[pl.ds(n_cand, n_tok), :]
    q_own = v["q_vec"][...]
    eye = lax.broadcasted_iota(I32, (n_tok, n_tok), 0) == lax.broadcasted_iota(I32, (n_tok, n_tok), 1)
    z_own = jnp.sum(jnp.where(eye, dot_nt(targ_vec, q_own), 0.0), axis=0, keepdims=True) * (scale * LOG2E)
    own_ref[...] = jnp.full(own_ref.shape, -jnp.inf, F32)
    own_ref[own, :] = z_own

    def pass_one(i, upper):
        t = 2 * (chip + sign[1] * lax.rem(i // 2, 2) + 2 * sign[2] * (i // 4) + upper * 4 * sign[4]) + lax.rem(i, 2)
        q_t = q_all[t]
        targ = jnp.concatenate([targ_ref[t, pl.ds(i, 1), :] for i in range(n_tok // LANES)], axis=1).astype(F32)
        z_t = own_ref[pl.ds(t, 1), :]
        top8 = jnp.broadcast_to(z_t, (8, n_tok))
        for j in range(n_cand // COL_BLK):
            s = pl.ds(j * COL_BLK, COL_BLK)
            lq = jnp.concatenate([v["lq"][s, :]] * (n_tok // LANES), axis=1)
            ids = jnp.concatenate([v["ids"][s, :]] * (n_tok // LANES), axis=1)
            z = dot_nt(vec[s, :], q_t) * (scale * LOG2E) - lq
            z = jnp.where(ids == targ, HIT_VALUE * LOG2E, z)
            z_ref[t, s, :] = z
            top8 = jnp.maximum(top8, jnp.max(z.reshape(COL_BLK // 8, 8, n_tok), axis=0))
        top = jnp.max(top8, axis=0, keepdims=True)
        den8 = jnp.zeros((8, n_tok), F32)
        for j in range(n_cand // COL_BLK):
            e = jnp.exp2(z_ref[t, pl.ds(j * COL_BLK, COL_BLK), :] - top)
            den8 = den8 + jnp.sum(e.reshape(COL_BLK // 8, 8, n_tok), axis=0)
        top_ref[pl.ds(t, 1), :] = top
        den_ref[pl.ds(t, 1), :] = jnp.sum(den8, axis=0, keepdims=True) + jnp.exp2(z_t - top)
        return upper

    q_other(0)
    lax.fori_loop(0, parts // 2, pass_one, 0)
    for s in (5, 6, 7):
        q_have(s, ())
    q_other(1)
    lax.fori_loop(0, parts // 2, pass_one, 1)
    for sem, tiles in ((q_send, 7), (q_csend, 8)):
        some = q_all.at[pl.ds(0, tiles)]
        remote(some, some, sem, q_recv.at[0], other).wait_send()
    held, got, st_send, st_recv = group(v, "st")
    held[0] = top_ref[...] + jnp.log2(den_ref[...])
    for r, peers in enumerate(rounds):
        for i, peer in enumerate(peers):
            remote(held.at[r], got.at[r, i], st_send.at[r], st_recv.at[r], peer).start()
        remote(got.at[r], got.at[r], st_send.at[r], st_recv.at[r], other).wait()
        logs = [held[r]] + [got[r, i] for i in range(len(peers))]
        top = functools.reduce(jnp.maximum, logs)
        held[r + 1] = top + jnp.log2(sum(jnp.exp2(x - top) for x in logs))
    lse_ref, norm = held.at[len(rounds)], v["norm"]
    norm[...] = lse_ref[...] + math.log2(total)
    lse = lse_ref[own, :]
    loss = jnp.sum(lse - z_own, axis=1, keepdims=True) * (1.0 / (LOG2E * total))
    dz_row = ((jnp.exp2(z_own - lse) - 1.0) * (1.0 / total)).astype(BF).astype(F32)
    dz_col = jnp.sum(jnp.where(eye, dz_row, 0.0), axis=1, keepdims=True)
    grad = v["i_grad"]
    grad[pl.ds(n_cand, n_tok), :] = (scale * dz_col * q_own.astype(F32)).astype(BF)
    i_pre, i_slope = v["i_pre"], v["i_slope"]
    rows_v, row_sem = v["rows"], v["row_sem"]
    mine = rows_v.at[me]

    def item_back(first, rows):
        for r in range(first, first + rows, ROW_BLK):
            s = pl.ds(r, ROW_BLK)
            i_pre[s, :] = (i_slope[s, :] * dot_nt(grad[s, :], wi2[...])).astype(BF)
            mine[s, :] = dot_nt(i_pre[s, :], wi1[...]).astype(BF)

    def send_back(n, first, rows):
        p = pl.ds(first, rows)

        def leave(dev, begin, num):
            q = pl.ds(begin, num)
            pltpu.make_async_copy(rows_v.at[dev, q, :], rows_out.at[dev, q, :], row_sem.at[n]).start()

        leave(me, first, rows)
        yield from all_gather_steps(mine, rows_v, thirds(rows, 16, first), group(v, f"agr{n}"), leave)
        pltpu.make_async_copy(rows_v.at[:, p, :], rows_out.at[:, p, :], row_sem.at[n]).wait()

    item_back(n_cand, n_tok)
    back_t = send_back(0, n_cand, n_tok)
    for _ in range(3):
        next(back_t)
    vec_t = v["vec_t"]
    vec_t[...] = turn(vec[:n_cand, :])
    d_acc, dz_s, dh = v["d_acc"], v["dz"], v["dh"]
    d_acc[...] = jnp.zeros_like(d_acc)

    def pass_two(t):
        shift = norm[pl.ds(t, 1), :]
        for j in range(n_cand // COL_BLK):
            s = pl.ds(j * COL_BLK, COL_BLK)
            dz_s[s, :] = jnp.exp2(z_ref[t, s, :] - shift).astype(BF)
        d_acc[...] += dot_nn(dz_s[...], q_all[t])
        dh[t] = dot_nn(vec_t[...], dz_s[...])

    def both(s):
        def one(c, _):
            pass_two(at(s, c))
            return 0

        lax.fori_loop(0, 2, one, 0)
        if s not in CORE_ORDER[:2]:
            next(back_t, None)

    rs_dh = reduce_scatter_steps(lambda dev: dh.at[dev], thirds(LANES, 8), group(v, "rsd"), produce=both)
    next(rs_dh)
    next(rs_dh)
    grad[pl.ds(0, n_cand), :] = (d_acc[...] * scale).astype(BF)
    item_back(0, n_cand)
    next(rs_dh)
    back_c = send_back(1, 0, n_cand)
    next(back_c)
    packed_grads(turn(raw[...]), turn(grad[...]), i_pre, v["i_hid"], None, lambda dev: v["i_part"].at[dev % 2, dev // 2])
    next(rs_dh)
    next(back_c)
    ar_i = sum_direct_steps(v["i_part"], v["i_sum"], group(v, "ai"))
    next(back_c)
    next(ar_i)
    next(rs_dh)
    next(ar_i)
    next(back_c)
    next(back_c)
    d_query = ((dz_col * targ_vec.astype(F32) + v["rsd.1"][0].T) * scale).astype(BF)
    q_pre = v["q_pre"]
    q_pre[...] = (v["q_slope"][...] * dot_nt(d_query, w2[...])).astype(BF)
    packed_grads(turn(tok_ref[...]), turn(d_query), q_pre, v["q_hid"], loss, lambda dev: v["q_part"].at[dev % 2, dev // 2])
    ar_q = sum_direct_steps(v["q_part"], v["q_sum"], group(v, "aq"))
    drain(ar_q, ar_i, back_c, back_t, rs_dh)
    unpack_grads(v["i_sum"], di_in_out, di_out_out, None)
    unpack_grads(v["q_sum"], dq_in_out, dq_out_out, loss_out)
    for c in leaves:
        c.start()
    for c in leaves:
        c.wait()


def step(x, tokens, weights, cand, logq, targ, cid):
    parts, n_item, _ = x.shape
    n_tok = tokens.shape[0]
    n_cand = n_item - n_tok
    ff = weights[0].shape[1]
    dma = pltpu.SemaphoreType.DMA
    n_in, n_out = LANES // parts, ff // parts
    spec = grouped("rs", rs_scratch(n_item, LANES, BF))
    spec += grouped("st", [pltpu.VMEM((3, parts, n_tok), F32), pltpu.VMEM((2, 3, parts, n_tok), F32), dma((2,)), dma((2,))])
    spec += grouped("rsd", rs_scratch(LANES, n_tok, F32))
    for n in range(2):
        spec += grouped(f"agr{n}", ag_scratch())
    i_rows = n_in * (ff // LANES) + n_out
    q_rows = i_rows + 8
    spec += grouped("ai", direct_scratch(i_rows, LANES))
    spec += grouped("aq", direct_scratch(q_rows, LANES))
    spec += grouped("agq", [dma, dma((8,)), dma, dma((2,))])
    spec += [("x_sem", dma((8,))), ("row_sem", dma((2,)))]

    def add(name, shape, dtype=F32):
        spec.append((name, pltpu.VMEM(shape, dtype)))

    for n, pre in ((n_tok, "q"), (n_item, "i")):
        add(pre + "_slope", (n, ff))
        add(pre + "_hid", (n, ff), BF)
        add(pre + "_pre", (n, ff), BF)
        add(pre + "_vec", (n, LANES), BF)
    add("i_grad", (n_item, LANES), BF)
    add("i_part", (2, parts // 2, i_rows, LANES))
    add("i_sum", (parts, i_rows, LANES))
    add("q_part", (2, parts // 2, q_rows, LANES))
    add("q_sum", (parts, q_rows, LANES))
    add("x_mine", (8, n_item, LANES), BF)
    add("rows", (parts, n_item, LANES), BF)
    add("q_all", (parts, n_tok, LANES), BF)
    for name in ("lq", "ids", "d_acc"):
        add(name, (n_cand, LANES))
    add("z", (parts, n_cand, n_tok))
    for name in ("top", "den", "norm", "own"):
        add(name, (parts, n_tok))
    add("vec_t", (LANES, n_cand), BF)
    add("dz", (n_cand, n_tok), BF)
    add("dh", (parts, LANES, n_tok))
    sums = (jax.ShapeDtypeStruct((parts, n_in, ff), F32), jax.ShapeDtypeStruct((parts, n_out, LANES), F32))
    outs = (jax.ShapeDtypeStruct((parts, n_item, LANES), BF),) + sums + sums + (jax.ShapeDtypeStruct((8, LANES), F32),)
    args = (tokens, *weights, cand, logq, targ)
    spec += grouped("in", [pltpu.VMEM(a.shape, a.dtype) for a in args]) + grouped("out", [pltpu.VMEM(o.shape, o.dtype) for o in outs[1:]])
    spec += [("in_sem", dma((8,))), ("out_sem", dma((5,)))]
    return kernel_call(step_kernel, "softmax_step", cid, outs, spec, x, *args, in_hbm=range(9), out_hbm=range(6))


def solution(mesh):
    num_dev = mesh.shape["dp"]

    def local_step(tokens, w_one, w_two, wi_one, wi_two, table_loc, cand_ids, log_q, targ_loc):
        rows_loc, dim = table_loc.shape
        n_item = cand_ids.shape[0] // num_dev + tokens.shape[0]
        cand = cand_ids.reshape(-1, LANES)
        targ = start(targ_loc.reshape(-1, LANES), num_dev, 1)
        owned, plist, counts = gather(table_loc, cand, targ)
        back, *sums = step(owned.reshape(num_dev, n_item, dim), tokens, (w_one, w_two, wi_one, wi_two), cand, log_q.reshape(-1, LANES), targ, 2)
        d_table, loss, di_in, di_out, dq_in, dq_out = scatter(back.reshape(-1, dim), plist, counts, rows_loc, sums, num_dev)
        shaped = [g.reshape(w.shape) for g, w in zip((dq_in, dq_out, di_in, di_out), (w_one, w_two, wi_one, wi_two))]
        return (loss.reshape(()), d_table) + tuple(shaped)

    return jax.shard_map(local_step, mesh=mesh, in_specs=(P("dp", None), P(), P(), P(), P(), P("dp", None), P(), P(), P("dp")), out_specs=(P(), P("dp", None), P(), P(), P(), P()), check_vma=False)
```

```python
import functools
import math
import jax
import jax.numpy as jnp
from jax import lax
from jax.experimental import pallas as pl
from jax.experimental.pallas import tpu as pltpu
from jax.sharding import PartitionSpec as P

SCORE_GAIN = 3.0
HIT_VALUE = -1e9
LANES = 128
VMEM_CAP = 60 * 1024 * 1024
BF = jnp.bfloat16
F32 = jnp.float32
I32 = jnp.int32
VM = pl.BlockSpec(memory_space=pltpu.VMEM)
SM = pl.BlockSpec(memory_space=pltpu.SMEM)
HB = pl.BlockSpec(memory_space=pl.ANY)
BLK = 256


def compact(loc, num_rows, parts, head):
    nr = loc.shape[0]
    own = jnp.where((loc >= 0) & (loc < num_rows), 1.0, 0.0)
    own16 = own.astype(BF)
    tri = jnp.where(lax.broadcasted_iota(I32, (LANES, LANES), 0) < lax.broadcasted_iota(I32, (LANES, LANES), 1), 1.0, 0.0).astype(BF)
    within = jnp.dot(own16, tri, preferred_element_type=F32)
    low = jnp.where(lax.broadcasted_iota(I32, (nr, nr), 1) < lax.broadcasted_iota(I32, (nr, nr), 0), 1.0, 0.0).astype(BF)
    before = jnp.sum(jnp.dot(low, own16, preferred_element_type=F32), axis=1, keepdims=True)
    lane = lax.broadcasted_iota(I32, (nr, LANES), 1)
    flat = lax.broadcasted_iota(I32, (nr, LANES), 0) * LANES + lane
    disp = flat - (within + before).astype(I32)
    n_head, n_tail = head // parts, (nr * LANES - head) // parts
    late = flat - head
    pos = jnp.where(flat < head, flat + flat // n_head * n_tail, late + (late // n_tail + 1) * n_head)
    val = jnp.where(own > 0, pos * 32768 + loc, -1)
    total = jnp.sum(own).astype(I32)

    def back(x, s):
        if s >= LANES:
            return pltpu.roll(x, nr - s // LANES, axis=0)
        here = pltpu.roll(x, LANES - s, axis=1)
        return jnp.where(lane < LANES - s, here, pltpu.roll(here, nr - 1, axis=0))

    bit = 0
    while (1 << bit) < nr * LANES:
        val_b, disp_b = back(val, 1 << bit), back(disp, 1 << bit)
        take = (val_b >= 0) & (((disp_b >> bit) & 1) == 1)
        stay = ((disp >> bit) & 1) == 0
        val = jnp.where(take, val_b, jnp.where(stay, val, -1))
        disp = jnp.where(take, disp_b, disp)
        bit += 1
    return jnp.where(flat < total, val, nr * LANES * 32768), own, total


def gather_kernel(chunks, cand_ref, targ_ref, table_ref, out_ref, list_out, cnt_ref, list_ref, ids_ref, stage, tab, dense, plist, packed_rows, sem, psem, osem, lsem):
    rows = tab.shape[0]
    npos = out_ref.shape[0]
    cr = rows // chunks

    def load(c):
        return pltpu.make_async_copy(table_ref.at[pl.ds(c * cr, cr), :], stage.at[pl.ds(c * cr, cr), :], sem.at[c])

    for c in range(chunks):
        load(c).start()
    parts, sub, _ = targ_ref.shape
    n_head = cand_ref.shape[0]
    head = n_head * LANES
    ids_ref[:n_head, :] = cand_ref[...]
    for d in range(parts):
        ids_ref[n_head + d * sub:n_head + (d + 1) * sub, :] = targ_ref[d]
    packed, own, total = compact(ids_ref[...] - lax.axis_index("dp") * rows, rows, parts, head)
    list_ref[...] = packed
    cnt_ref[0] = jnp.sum(own[:head // LANES]).astype(I32)
    cnt_ref[1] = total
    to_smem = pltpu.make_async_copy(list_ref, plist, psem)
    to_smem.start()
    to_hbm = pltpu.make_async_copy(list_ref, list_out, lsem)
    to_hbm.start()

    def zero(i, _):
        dense[pl.ds(pl.multiple_of(i * BLK, BLK), BLK), :] = jnp.zeros((BLK, LANES), F32)
        return 0

    lax.fori_loop(0, npos // BLK, zero, 0)
    for c in range(chunks):
        load(c).wait()

        def conv(i, _, c=c):
            s = pl.ds(pl.multiple_of(c * cr + i * BLK, BLK), BLK)
            tab[s, :] = stage[s, :].astype(F32)
            return 0

        lax.fori_loop(0, cr // BLK, conv, 0)
    to_smem.wait()

    def pick(i, _):
        vals = []
        for u in range(LANES):
            w = plist[i, u]
            vals.append((w >> 15, tab[pl.ds(w & 32767, 1), :]))
        for p, v in vals:
            dense[pl.ds(p, 1), :] = v
        return 0

    lax.fori_loop(0, (total + LANES - 1) // LANES, pick, 0)

    part = npos // parts

    def leave(d):
        s = pl.ds(d * part, part)
        return pltpu.make_async_copy(packed_rows.at[s, :], out_ref.at[s, :], osem.at[d])

    for d in range(parts):
        packed_rows[pl.ds(d * part, part), :] = dense[pl.ds(d * part, part), :].astype(BF)
        leave(d).start()
    for d in range(parts):
        leave(d).wait()
    to_hbm.wait()


def gather(table, cand, targ):
    rows = table.shape[0]
    nr = cand.shape[0] + targ.shape[0] * targ.shape[1]
    npos = nr * LANES
    chunks = 8
    return pl.pallas_call(
        functools.partial(gather_kernel, chunks),
        out_shape=(jax.ShapeDtypeStruct((npos, LANES), BF), jax.ShapeDtypeStruct((nr, LANES), I32), jax.ShapeDtypeStruct((2,), I32)),
        in_specs=[VM, VM, HB],
        out_specs=(HB, HB, SM),
        scratch_shapes=[pltpu.VMEM((nr, LANES), I32), pltpu.VMEM((nr, LANES), I32), pltpu.VMEM((rows, LANES), BF), pltpu.VMEM((rows, LANES), F32), pltpu.VMEM((npos + 8, LANES), F32), pltpu.SMEM((nr, LANES), I32), pltpu.VMEM((npos, LANES), BF), pltpu.SemaphoreType.DMA((chunks,)), pltpu.SemaphoreType.DMA, pltpu.SemaphoreType.DMA((targ.shape[0],)), pltpu.SemaphoreType.DMA],
        compiler_params=pltpu.CompilerParams(vmem_limit_bytes=VMEM_CAP),
        name="gather_rows",
    )(cand, targ, table)


ADDS = 4


def scatter_kernel(chunks, cnt_ref, list_ref, grad_ref, *refs):
    n = (len(refs) - 10) // 3
    passed, (out_ref, loss_ref, *refs) = refs[:n], refs[n:]
    kept, held, (acc, raw, grad, plist, sem, psem, gsem, isem, osem) = refs[:n - 1], refs[n - 1:2 * n - 1], refs[2 * n - 1:]
    parts = gsem.shape[0]
    part = grad_ref.shape[0] // parts

    def arrive(d):
        s = pl.ds(d * part, part)
        return pltpu.make_async_copy(grad_ref.at[s, :], raw.at[s, :], gsem.at[d])

    for d in range(parts):
        arrive(d).start()
    ins = [pltpu.make_async_copy(src, dst, isem.at[i]) for i, (src, dst) in enumerate(zip(passed, held))]
    outs = [pltpu.make_async_copy(src, dst, osem.at[i]) for i, (src, dst) in enumerate(zip(held[:-1], kept))]
    for c in ins:
        c.start()
    rows = out_ref.shape[0]
    npos = grad_ref.shape[0]
    to_smem = pltpu.make_async_copy(list_ref, plist, psem)
    to_smem.start()

    def zero(i, _):
        acc[pl.ds(pl.multiple_of(i * BLK, BLK), BLK), :] = jnp.zeros((BLK, LANES), F32)
        return 0

    lax.fori_loop(0, rows // BLK, zero, 0)

    for d in range(parts):
        arrive(d).wait()
        s = pl.ds(d * part, part)
        grad[s, :] = raw[s, :].astype(F32)
    for i in ins:
        i.wait()
    for o in outs:
        o.start()
    loss_ref[0] = jnp.sum(held[-1][0:1, 0:1])
    grad[npos:, :] = jnp.zeros((8, LANES), F32)
    to_smem.wait()
    nhead = cnt_ref[0]
    total = cnt_ref[1]

    def put(i, _):
        vals = []
        for u in range(LANES):
            w = plist[i, u]
            vals.append((w & 32767, grad[pl.ds(w >> 15, 1), :]))
        for r, v in vals:
            acc[pl.ds(r, 1), :] = v
        return 0

    lax.fori_loop(0, nhead // LANES, put, 0)

    def add_one(i, _):
        w = plist[i >> 7, i & 127]
        r = pl.ds(w & 32767, 1)
        acc[r, :] = acc[r, :] + grad[pl.ds(w >> 15, 1), :]
        return 0

    def add_row(i, _):
        for j in range(0, LANES, ADDS):
            words = [plist[i, j + u] for u in range(ADDS)]
            rs = [w & 32767 for w in words]
            gs = [grad[pl.ds(w >> 15, 1), :] for w in words]
            outs = []
            for u in range(ADDS):
                v = acc[pl.ds(rs[u], 1), :] + gs[u]
                for t in range(u):
                    v = v + jnp.where(rs[t] == rs[u], gs[t], 0.0)
                outs.append(v)
            for u in range(ADDS):
                acc[pl.ds(rs[u], 1), :] = outs[u]
        return 0

    begin = nhead // LANES * LANES
    split = jnp.minimum((nhead + LANES - 1) // LANES * LANES, total)
    lax.fori_loop(begin, split, add_one, 0)
    lax.fori_loop((split + LANES - 1) // LANES, (total + LANES - 1) // LANES, add_row, 0)
    cr = rows // chunks

    def store(c):
        return pltpu.make_async_copy(acc.at[pl.ds(c * cr, cr), :], out_ref.at[pl.ds(c * cr, cr), :], sem.at[c])

    for c in range(chunks):
        store(c).start()
    for c in range(chunks):
        store(c).wait()
    for o in outs:
        o.wait()


def scatter(grads, plist, counts, rows, passed, parts):
    nr = plist.shape[0]
    npos = nr * LANES
    chunks = 8
    n = len(passed)
    dma = pltpu.SemaphoreType.DMA
    return pl.pallas_call(
        functools.partial(scatter_kernel, chunks),
        out_shape=(jax.ShapeDtypeStruct((rows, LANES), F32), jax.ShapeDtypeStruct((1,), F32)) + tuple(jax.ShapeDtypeStruct(p.shape, p.dtype) for p in passed[:-1]),
        in_specs=[SM, HB, HB] + [HB] * n,
        out_specs=(HB, SM) + (HB,) * (n - 1),
        scratch_shapes=[pltpu.VMEM(p.shape, p.dtype) for p in passed]
        + [pltpu.VMEM((rows, LANES), F32), pltpu.VMEM((npos, LANES), BF), pltpu.VMEM((npos + 8, LANES), F32), pltpu.SMEM((nr, LANES), I32), dma((chunks,)), dma, dma((parts,)), dma((n,)), dma((n,))],
        compiler_params=pltpu.CompilerParams(vmem_limit_bytes=VMEM_CAP),
        name="scatter_rows",
    )(counts, plist, grads, *passed)


MESHID = pl.DeviceIdType.MESH
CHIP_DIMS = (1, 2, 4)
SLOTS = tuple(range(8))
CORE_ORDER = (7, 3, 5, 6, 1, 2, 4, 0)
RS_BASE = (0, 4, 6)


def place():
    me = lax.axis_index("dp")
    core = lax.rem(me, 2)
    chip = me // 2
    sign = {d: 1 - 2 * lax.rem(chip // d, 2) for d in CHIP_DIMS}
    return me, core, chip, sign


def chip_at(chip, sign, s):
    for d in CHIP_DIMS:
        if s & d:
            chip = chip + d * sign[d]
    return chip


def locate():
    me, core, chip, sign = place()
    return me, core, 1 - core, chip, sign, lambda s, c: 2 * chip_at(chip, sign, s) + c


def enter(peers):
    barrier = pltpu.get_barrier_semaphore()
    for peer in peers:
        pl.semaphore_signal(barrier, inc=1, device_id=(peer,), device_id_type=MESHID)
    pl.semaphore_wait(barrier, len(peers))


def order_of(k):
    return tuple(CHIP_DIMS[(k + i) % 3] for i in range(3))


def thirds(rows, unit, first=0):
    base = rows // unit
    cuts = [(base * i // 3) * unit for i in range(4)]
    return [(0, first + cuts[i], cuts[i + 1] - cuts[i], i) for i in range(3)]


def remote(src, dst, send, recv, peer):
    return pltpu.make_async_remote_copy(src_ref=src, dst_ref=dst, send_sem=send, recv_sem=recv, device_id=(peer,), device_id_type=MESHID)


def stage_slots(order, t):
    dims = order_of(order)
    live = [s for s in SLOTS if all(not s & d for d in dims[:t])]
    return [(s, s ^ dims[t]) for s in live if s & dims[t]]


def rs_scratch(rows, width, dtype):
    dma = pltpu.SemaphoreType.DMA
    return [pltpu.VMEM((8, rows, width), dtype), pltpu.VMEM((8, rows, width), dtype), pltpu.VMEM((7, rows, width), dtype), dma, dma((8,)), dma, dma((7,))]


def reduce_scatter_steps(get, pieces, scratch, mine=None, produce=None):
    crecv, acc, recv, csend_s, crecv_s, send_s, recv_s = scratch
    me, core, away, chip, sign, at = locate()
    other = at(0, away)

    def core_copy(s):
        return remote(get(at(s, away)), crecv.at[s], csend_s, crecv_s.at[s], other)

    def send(k, t, i, s):
        _, off, ln, order = pieces[k]
        slot = RS_BASE[t] + i
        peer = at(order_of(order)[t], core)
        remote(acc.at[s, pl.ds(off, ln), :], recv.at[slot, pl.ds(off, ln), :], send_s, recv_s.at[slot], peer).start()

    def forward(k, t, s):
        for i, (src, _) in enumerate(stage_slots(pieces[k][3], t)):
            if src == s:
                send(k, t, i, s)

    def absorb(s):
        core_copy(s).wait_recv()
        acc[s] = (mine(s) if mine else get(at(s, core))[...]) + crecv[s]
        for k in range(3):
            forward(k, 0, s)

    for n, s in enumerate(CORE_ORDER):
        if produce:
            produce(s)
        core_copy(s).start()
        if produce and n:
            absorb(CORE_ORDER[n - 1])
    yield
    for s in CORE_ORDER[-1:] if produce else CORE_ORDER:
        absorb(s)
    yield
    for t in range(3):
        for i in reversed(range(4 >> t)):
            slot = RS_BASE[t] + i
            remote(recv.at[slot], recv.at[slot], send_s, recv_s.at[slot], other).wait_recv()
            for k in range(3):
                _, off, ln, order = pieces[k]
                dst = stage_slots(order, t)[i][1]
                p = pl.ds(off, ln)
                acc[dst, p, :] = acc[dst, p, :] + recv[slot, p, :]
                if t < 2:
                    forward(k, t + 1, dst)
        yield
    remote(crecv, crecv, csend_s, crecv_s.at[0], other).wait_send()
    remote(recv, recv, send_s, recv_s.at[0], other).wait_send()


def ag_scratch():
    dma = pltpu.SemaphoreType.DMA
    return [dma, dma, dma, dma((8,))]


def all_gather_steps(own, out, pieces, scratch, landed=None):
    csend_s, crecv_s, send_s, recv_s = scratch
    me, core, away, chip, sign, at = locate()
    other = at(0, away)
    begin = pieces[0][1]
    whole = pl.ds(begin, sum(p[2] for p in pieces))

    def device(s):
        return at(s, core)

    def slot(k, bits):
        d = order_of(pieces[k][3])
        return sum(d[b] for b in range(3) if bits >> b & 1)

    def ends(k, s):
        p = pl.ds(pieces[k][1], pieces[k][2])
        there = out.at[device(s), p, :]
        return (own.at[p, :] if s == 0 else there), there

    def core_send(k, s):
        src, there = ends(k, s)
        remote(src, there, csend_s, crecv_s, other).start()

    def send(k, t, bits):
        src, there = ends(k, slot(k, bits))
        remote(src, there, send_s, recv_s.at[bits | 1 << t], at(order_of(pieces[k][3])[t], core)).start()

    plan = (((), (0, 0)), ((), (1, 0)), ((), (2, 0)), ((1,), (1, 1)), ((), (2, 1)), ((2,), (2, 2)), ((3,), (2, 3)), ((4, 5, 6, 7), None))
    for n, (waits, step) in enumerate(plan):
        for bits in waits:
            remote(out.at[me, whole, :], out.at[me, whole, :], send_s, recv_s.at[bits], other).wait_recv()
            for k in range(len(pieces)):
                core_send(k, slot(k, bits))
                if landed:
                    landed(device(slot(k, bits)), pieces[k][1], pieces[k][2])
        for k in range(len(pieces)):
            if step:
                send(k, *step)
            if n == 0:
                core_send(k, 0)
        yield
    half = out.at[pl.ds(0, 8), whole, :]
    remote(half, half, csend_s, crecv_s, other).wait()
    sent = out.at[pl.ds(0, 7), whole, :]
    remote(sent, sent, send_s, recv_s.at[0], other).wait_send()
    if landed:
        for s in SLOTS:
            landed(at(s, away), begin, whole.size)


def direct_scratch(rows, width):
    dma = pltpu.SemaphoreType.DMA
    return [pltpu.VMEM((8, rows, width), F32)] * 3 + [pltpu.VMEM((rows, width), F32)] + [dma] * 8


def sum_direct_steps(src, out, scratch):
    crecv, acc, recv, tot, cs, cr, s1, r1, s2, r2, s3, r3 = scratch
    me, core, away, chip, sign, at = locate()
    other = at(0, away)
    first = remote(src.at[away], crecv, cs, cr, other)
    first.start()
    yield
    first.wait()
    acc[...] = src[core] + crecv[...]
    far = (7, 3, 5, 6, 1, 2, 4)

    def to(s):
        return at(s, core)

    for s in far:
        remote(acc.at[chip_at(chip, sign, s)], recv.at[s], s1, r1, to(s)).start()
    yield
    seven = recv.at[pl.ds(1, 7)]
    remote(seven, seven, s1, r1, other).wait()
    total = acc[chip]
    for s in far:
        total = total + recv[s]
    tot[...] = total
    for s in far:
        remote(tot, out.at[me], s2, r2, to(s)).start()
    remote(tot, out.at[me], s3, r3, other).start()
    out[me] = total
    yield
    seven = out.at[pl.ds(0, 7)]
    remote(seven, seven, s2, r2, other).wait()
    for s in far:
        remote(out.at[to(s)], out.at[to(s)], s3, r3, other).start()
    yield
    eight = out.at[pl.ds(0, 8)]
    remote(eight, eight, s3, r3, other).wait()


def drain(*steps):
    live = list(steps)
    while live:
        live = [g for g in live if next(g, StopIteration) is not StopIteration]


def kernel_call(body, name, cid, out_shape, scratch, *args, in_hbm=(), out_hbm=()):
    names = tuple(n for n, _ in scratch)

    def kernel(*refs):
        n = len(args) + len(jax.tree.leaves(out_shape))
        body(*refs[:n], dict(zip(names, refs[n:])))

    return pl.pallas_call(
        kernel,
        out_shape=out_shape,
        in_specs=[HB if i in in_hbm else VM for i in range(len(args))],
        out_specs=tuple(HB if i in out_hbm else VM for i in range(len(out_shape))),
        scratch_shapes=[s for _, s in scratch],
        compiler_params=pltpu.CompilerParams(collective_id=cid, has_side_effects=True, vmem_limit_bytes=VMEM_CAP),
        name=name,
    )(*args)


def grouped(name, items):
    return [(f"{name}.{i}", s) for i, s in enumerate(items)]


def group(scratch, name):
    return [v for k, v in scratch.items() if k.startswith(name + ".")]
LOG2E = 1.4426950408889634
GELU_C = math.sqrt(2.0 / math.pi)
GELU_A = 0.044715
ROW_BLK = 256
COL_BLK = 256


def gelu_both(x):
    x2 = x * x
    t = jnp.tanh(GELU_C * (x + GELU_A * (x2 * x)))
    half = 0.5 * (1.0 + t)
    return x * half, half + (0.5 * GELU_C) * x * (1.0 - t * t) * (1.0 + (3.0 * GELU_A) * x2)


def dot_nn(a, b):
    return jnp.dot(a, b, preferred_element_type=F32)


def dot_nt(a, b):
    return lax.dot_general(a, b, (((1,), (1,)), ((), ())), preferred_element_type=F32)


def turn(x):
    return x.astype(F32).T.astype(BF)


def tower_into(rows, load, w_in, w_out, slope_ref, hid_ref, out_ref):
    def blk(i, _):
        s = pl.ds(pl.multiple_of(i * ROW_BLK, ROW_BLK), ROW_BLK)
        act, slope = gelu_both(dot_nn(load(s), w_in[...]))
        slope_ref[s, :] = slope
        hid_ref[s, :] = act.astype(BF)
        out_ref[s, :] = dot_nn(hid_ref[s, :], w_out[...]).astype(BF)

        return 0

    lax.fori_loop(0, rows // ROW_BLK, blk, 0)


def start_kernel(targ_ref, targ_out, v):
    me, core, away, chip, sign, at = locate()
    peers = [at(s, c) for s in reversed(SLOTS) for c in ((core, away) if s else (away,))]
    enter(peers)
    send_s, recv_s = v["sems.0"], v["sems.1"]
    targ_out[me] = targ_ref[...]
    for peer in peers:
        remote(targ_ref, targ_out.at[me], send_s, recv_s, peer).start()
    most = targ_out.at[pl.ds(0, len(peers))]
    remote(most, most, send_s, recv_s, peers[-1]).wait()


def start(targ, parts, cid):
    dma = pltpu.SemaphoreType.DMA
    outs = (jax.ShapeDtypeStruct((parts,) + targ.shape, I32),)
    return kernel_call(start_kernel, "start_step", cid, outs, grouped("sems", [dma, dma]), targ)[0]


def packed_grads(row_t, grad_t, pre_ref, hid_ref, loss, part_of):
    d_in = dot_nn(row_t, pre_ref[...])
    d_out = dot_nn(grad_t, hid_ref[...]).T
    wide = d_in.shape[1] // LANES
    parts = 16
    n_in, n_out = d_in.shape[0] // parts, d_out.shape[0] // parts
    for dev in range(parts):
        part = part_of(dev)
        for c in range(wide):
            part[c * n_in:(c + 1) * n_in, :] = d_in[dev * n_in:(dev + 1) * n_in, c * LANES:(c + 1) * LANES]
        part[wide * n_in:wide * n_in + n_out, :] = d_out[dev * n_out:(dev + 1) * n_out, :]
        if loss is not None:
            part[wide * n_in + n_out:, :] = jnp.broadcast_to(loss if dev == 0 else 0.0 * loss, (8, LANES))


def unpack_grads(sums_ref, in_ref, out_ref, loss_ref):
    parts, n_in, width = in_ref.shape
    n_out = out_ref.shape[1]
    wide = width // LANES
    for dev in range(parts):
        for c in range(wide):
            in_ref[dev, :, c * LANES:(c + 1) * LANES] = sums_ref[dev, c * n_in:(c + 1) * n_in, :]
        out_ref[dev] = sums_ref[dev, wide * n_in:wide * n_in + n_out, :]
    if loss_ref is not None:
        loss_ref[...] = sums_ref[0, wide * n_in + n_out:, :]


def step_kernel(x_ref, *refs):
    (rows_out, *outs), v = refs[8:-1], refs[-1]
    ins = [pltpu.make_async_copy(src, v[f"in.{i}"], v["in_sem"].at[i]) for i, src in enumerate(refs[:8])]
    for c in ins:
        c.start()
    tok_ref, w1, w2, wi1, wi2, cand_ref, logq_ref, targ_ref = group(v, "in")
    di_in_out, di_out_out, dq_in_out, dq_out_out, loss_out = group(v, "out")
    leaves = [pltpu.make_async_copy(v[f"out.{i}"], dst, v["out_sem"].at[i]) for i, dst in enumerate(outs)]
    parts, n_item, _ = x_ref.shape
    n_tok = tok_ref.shape[0]
    n_cand = n_item - n_tok
    total = float(n_tok * parts)
    scale = SCORE_GAIN / math.sqrt(LANES)
    me, core, away, chip, sign, at = locate()
    other = at(0, away)
    diag = at(6, core)
    rounds = ((other, at(1, core), at(1, away)), (at(2, core), at(4, core), diag))
    enter([other, at(1, away)] + [at(s, core) for s in SLOTS[1:]])
    x_mine, x_sem = v["x_mine"], v["x_sem"]

    def fetch(s):
        return pltpu.make_async_copy(x_ref.at[at(s, core)], x_mine.at[s], x_sem.at[s])

    def own_part(s):
        fetch(s).wait()
        return x_mine[s]

    rs_rows = reduce_scatter_steps(lambda dev: x_ref.at[dev], thirds(n_item, 16), group(v, "rs"), mine=own_part)
    next(rs_rows)
    for s in CORE_ORDER:
        fetch(s).start()
    for c in ins[:3]:
        c.wait()
    tower_into(n_tok, lambda s: tok_ref[s, :], w1, w2, v["q_slope"], v["q_hid"], v["q_vec"])
    q_all = v["q_all"]
    q_all[me] = v["q_vec"][...]
    q_send, q_recv, q_csend, q_crecv = group(v, "agq")

    def q_tile(s, c):
        return q_all.at[at(s, c)]

    def q_go(s, d):
        src = v["q_vec"] if s == 0 else q_tile(s, core)
        if d:
            c = remote(src, q_tile(s, core), q_send, q_recv.at[s ^ d], at(d, core))
        else:
            c = remote(src, q_tile(s, core), q_csend, q_crecv.at[s // 4], other)
        c.start()

    def q_have(s, onward):
        remote(q_tile(s, core), q_tile(s, core), q_send, q_recv.at[s], other).wait_recv()
        for d in onward:
            q_go(s, d)
        q_go(s, 0)

    def q_other(upper):
        four = q_all.at[pl.ds(0, 4)]
        remote(four, four, q_csend, q_crecv.at[upper], other).wait_recv()

    for d in (1, 2, 4, 0):
        q_go(0, d)
    next(rs_rows)
    for c in ins[3:]:
        c.wait()
    n_sub = n_cand // LANES
    for r in range(n_sub):
        s = pl.ds(r * LANES, LANES)
        row = pl.ds(me * n_sub + r, 1)
        v["lq"][s, :] = jnp.broadcast_to(logq_ref[row, :] * LOG2E, (LANES, LANES)).T
        v["ids"][s, :] = jnp.broadcast_to(cand_ref[row, :].astype(F32), (LANES, LANES)).T
    drain(rs_rows)
    raw = v["rs.1"].at[0]
    q_have(1, (2, 4))
    q_have(2, (4,))
    q_have(4, ())
    tower_into(n_item, lambda s: raw[s, :], wi1, wi2, v["i_slope"], v["i_hid"], v["i_vec"])
    q_have(3, (4,))
    vec = v["i_vec"]
    z_ref, top_ref, den_ref, own_ref = v["z"], v["top"], v["den"], v["own"]
    own = pl.ds(me, 1)
    targ_vec = vec[pl.ds(n_cand, n_tok), :]
    q_own = v["q_vec"][...]
    eye = lax.broadcasted_iota(I32, (n_tok, n_tok), 0) == lax.broadcasted_iota(I32, (n_tok, n_tok), 1)
    z_own = jnp.sum(jnp.where(eye, dot_nt(targ_vec, q_own), 0.0), axis=0, keepdims=True) * (scale * LOG2E)
    own_ref[...] = jnp.full(own_ref.shape, -jnp.inf, F32)
    own_ref[own, :] = z_own

    def pass_one(i, upper):
        t = 2 * (chip + sign[1] * lax.rem(i // 2, 2) + 2 * sign[2] * (i // 4) + upper * 4 * sign[4]) + lax.rem(i, 2)
        q_t = q_all[t]
        targ = jnp.concatenate([targ_ref[t, pl.ds(i, 1), :] for i in range(n_tok // LANES)], axis=1).astype(F32)
        z_t = own_ref[pl.ds(t, 1), :]
        top8 = jnp.broadcast_to(z_t, (8, n_tok))
        for j in range(n_cand // COL_BLK):
            s = pl.ds(j * COL_BLK, COL_BLK)
            lq = jnp.concatenate([v["lq"][s, :]] * (n_tok // LANES), axis=1)
            ids = jnp.concatenate([v["ids"][s, :]] * (n_tok // LANES), axis=1)
            z = dot_nt(vec[s, :], q_t) * (scale * LOG2E) - lq
            z = jnp.where(ids == targ, HIT_VALUE * LOG2E, z)
            z_ref[t, s, :] = z
            top8 = jnp.maximum(top8, jnp.max(z.reshape(COL_BLK // 8, 8, n_tok), axis=0))
        top = jnp.max(top8, axis=0, keepdims=True)
        den8 = jnp.zeros((8, n_tok), F32)
        for j in range(n_cand // COL_BLK):
            e = jnp.exp2(z_ref[t, pl.ds(j * COL_BLK, COL_BLK), :] - top)
            den8 = den8 + jnp.sum(e.reshape(COL_BLK // 8, 8, n_tok), axis=0)
        top_ref[pl.ds(t, 1), :] = top
        den_ref[pl.ds(t, 1), :] = jnp.sum(den8, axis=0, keepdims=True) + jnp.exp2(z_t - top)
        return upper

    q_other(0)
    lax.fori_loop(0, parts // 2, pass_one, 0)
    for s in (5, 6, 7):
        q_have(s, ())
    q_other(1)
    lax.fori_loop(0, parts // 2, pass_one, 1)
    for sem, tiles in ((q_send, 7), (q_csend, 8)):
        some = q_all.at[pl.ds(0, tiles)]
        remote(some, some, sem, q_recv.at[0], other).wait_send()
    held, got, st_send, st_recv = group(v, "st")
    held[0] = top_ref[...] + jnp.log2(den_ref[...])
    for r, peers in enumerate(rounds):
        for i, peer in enumerate(peers):
            remote(held.at[r], got.at[r, i], st_send.at[r], st_recv.at[r], peer).start()
        remote(got.at[r], got.at[r], st_send.at[r], st_recv.at[r], other).wait()
        logs = [held[r]] + [got[r, i] for i in range(len(peers))]
        top = functools.reduce(jnp.maximum, logs)
        held[r + 1] = top + jnp.log2(sum(jnp.exp2(x - top) for x in logs))
    lse_ref, norm = held.at[len(rounds)], v["norm"]
    norm[...] = lse_ref[...] + math.log2(total)
    lse = lse_ref[own, :]
    loss = jnp.sum(lse - z_own, axis=1, keepdims=True) * (1.0 / (LOG2E * total))
    dz_row = ((jnp.exp2(z_own - lse) - 1.0) * (1.0 / total)).astype(BF).astype(F32)
    dz_col = jnp.sum(jnp.where(eye, dz_row, 0.0), axis=1, keepdims=True)
    grad = v["i_grad"]
    grad[pl.ds(n_cand, n_tok), :] = (scale * dz_col * q_own.astype(F32)).astype(BF)
    i_pre, i_slope = v["i_pre"], v["i_slope"]
    rows_v, row_sem = v["rows"], v["row_sem"]
    mine = rows_v.at[me]

    def item_back(first, rows):
        for r in range(first, first + rows, ROW_BLK):
            s = pl.ds(r, ROW_BLK)
            i_pre[s, :] = (i_slope[s, :] * dot_nt(grad[s, :], wi2[...])).astype(BF)
            mine[s, :] = dot_nt(i_pre[s, :], wi1[...]).astype(BF)

    def send_back(n, first, rows):
        p = pl.ds(first, rows)

        def leave(dev, begin, num):
            q = pl.ds(begin, num)
            pltpu.make_async_copy(rows_v.at[dev, q, :], rows_out.at[dev, q, :], row_sem.at[n]).start()

        leave(me, first, rows)
        yield from all_gather_steps(mine, rows_v, thirds(rows, 16, first), group(v, f"agr{n}"), leave)
        pltpu.make_async_copy(rows_v.at[:, p, :], rows_out.at[:, p, :], row_sem.at[n]).wait()

    item_back(n_cand, n_tok)
    back_t = send_back(0, n_cand, n_tok)
    for _ in range(3):
        next(back_t)
    vec_t = v["vec_t"]
    vec_t[...] = turn(vec[:n_cand, :])
    d_acc, dz_s, dh = v["d_acc"], v["dz"], v["dh"]
    d_acc[...] = jnp.zeros_like(d_acc)

    def pass_two(t):
        shift = norm[pl.ds(t, 1), :]
        for j in range(n_cand // COL_BLK):
            s = pl.ds(j * COL_BLK, COL_BLK)
            dz_s[s, :] = jnp.exp2(z_ref[t, s, :] - shift).astype(BF)
        d_acc[...] += dot_nn(dz_s[...], q_all[t])
        dh[t] = dot_nn(vec_t[...], dz_s[...])

    def both(s):
        def one(c, _):
            pass_two(at(s, c))
            return 0

        lax.fori_loop(0, 2, one, 0)
        if s not in CORE_ORDER[:2]:
            next(back_t, None)

    rs_dh = reduce_scatter_steps(lambda dev: dh.at[dev], thirds(LANES, 8), group(v, "rsd"), produce=both)
    next(rs_dh)
    next(rs_dh)
    grad[pl.ds(0, n_cand), :] = (d_acc[...] * scale).astype(BF)
    item_back(0, n_cand)
    next(rs_dh)
    back_c = send_back(1, 0, n_cand)
    next(back_c)
    packed_grads(turn(raw[...]), turn(grad[...]), i_pre, v["i_hid"], None, lambda dev: v["i_part"].at[dev % 2, dev // 2])
    next(rs_dh)
    next(back_c)
    ar_i = sum_direct_steps(v["i_part"], v["i_sum"], group(v, "ai"))
    next(back_c)
    next(ar_i)
    next(rs_dh)
    next(ar_i)
    next(back_c)
    next(back_c)
    d_query = ((dz_col * targ_vec.astype(F32) + v["rsd.1"][0].T) * scale).astype(BF)
    q_pre = v["q_pre"]
    q_pre[...] = (v["q_slope"][...] * dot_nt(d_query, w2[...])).astype(BF)
    packed_grads(turn(tok_ref[...]), turn(d_query), q_pre, v["q_hid"], loss, lambda dev: v["q_part"].at[dev % 2, dev // 2])
    ar_q = sum_direct_steps(v["q_part"], v["q_sum"], group(v, "aq"))
    for _ in range(4):
        for g in (ar_q, ar_i, back_c):
            next(g, None)
    drain(ar_i)
    unpack_grads(v["i_sum"], di_in_out, di_out_out, None)
    for c in leaves[:2]:
        c.start()
    drain(ar_q)
    unpack_grads(v["q_sum"], dq_in_out, dq_out_out, loss_out)
    for c in leaves[2:]:
        c.start()
    drain(back_c, back_t, rs_dh)
    for c in leaves:
        c.wait()


def step(x, tokens, weights, cand, logq, targ, cid):
    parts, n_item, _ = x.shape
    n_tok = tokens.shape[0]
    n_cand = n_item - n_tok
    ff = weights[0].shape[1]
    dma = pltpu.SemaphoreType.DMA
    n_in, n_out = LANES // parts, ff // parts
    spec = grouped("rs", rs_scratch(n_item, LANES, BF))
    spec += grouped("st", [pltpu.VMEM((3, parts, n_tok), F32), pltpu.VMEM((2, 3, parts, n_tok), F32), dma((2,)), dma((2,))])
    spec += grouped("rsd", rs_scratch(LANES, n_tok, F32))
    for n in range(2):
        spec += grouped(f"agr{n}", ag_scratch())
    i_rows = n_in * (ff // LANES) + n_out
    q_rows = i_rows + 8
    spec += grouped("ai", direct_scratch(i_rows, LANES))
    spec += grouped("aq", direct_scratch(q_rows, LANES))
    spec += grouped("agq", [dma, dma((8,)), dma, dma((2,))])
    spec += [("x_sem", dma((8,))), ("row_sem", dma((2,)))]

    def add(name, shape, dtype=F32):
        spec.append((name, pltpu.VMEM(shape, dtype)))

    for n, pre in ((n_tok, "q"), (n_item, "i")):
        add(pre + "_slope", (n, ff))
        add(pre + "_hid", (n, ff), BF)
        add(pre + "_pre", (n, ff), BF)
        add(pre + "_vec", (n, LANES), BF)
    add("i_grad", (n_item, LANES), BF)
    add("i_part", (2, parts // 2, i_rows, LANES))
    add("i_sum", (parts, i_rows, LANES))
    add("q_part", (2, parts // 2, q_rows, LANES))
    add("q_sum", (parts, q_rows, LANES))
    add("x_mine", (8, n_item, LANES), BF)
    add("rows", (parts, n_item, LANES), BF)
    add("q_all", (parts, n_tok, LANES), BF)
    for name in ("lq", "ids", "d_acc"):
        add(name, (n_cand, LANES))
    add("z", (parts, n_cand, n_tok))
    for name in ("top", "den", "norm", "own"):
        add(name, (parts, n_tok))
    add("vec_t", (LANES, n_cand), BF)
    add("dz", (n_cand, n_tok), BF)
    add("dh", (parts, LANES, n_tok))
    sums = (jax.ShapeDtypeStruct((parts, n_in, ff), F32), jax.ShapeDtypeStruct((parts, n_out, LANES), F32))
    outs = (jax.ShapeDtypeStruct((parts, n_item, LANES), BF),) + sums + sums + (jax.ShapeDtypeStruct((8, LANES), F32),)
    args = (tokens, *weights, cand, logq, targ)
    spec += grouped("in", [pltpu.VMEM(a.shape, a.dtype) for a in args]) + grouped("out", [pltpu.VMEM(o.shape, o.dtype) for o in outs[1:]])
    spec += [("in_sem", dma((8,))), ("out_sem", dma((5,)))]
    return kernel_call(step_kernel, "softmax_step", cid, outs, spec, x, *args, in_hbm=range(9), out_hbm=range(6))


def solution(mesh):
    num_dev = mesh.shape["dp"]

    def local_step(tokens, w_one, w_two, wi_one, wi_two, table_loc, cand_ids, log_q, targ_loc):
        rows_loc, dim = table_loc.shape
        n_item = cand_ids.shape[0] // num_dev + tokens.shape[0]
        cand = cand_ids.reshape(-1, LANES)
        targ = start(targ_loc.reshape(-1, LANES), num_dev, 1)
        owned, plist, counts = gather(table_loc, cand, targ)
        back, *sums = step(owned.reshape(num_dev, n_item, dim), tokens, (w_one, w_two, wi_one, wi_two), cand, log_q.reshape(-1, LANES), targ, 2)
        d_table, loss, di_in, di_out, dq_in, dq_out = scatter(back.reshape(-1, dim), plist, counts, rows_loc, sums, num_dev)
        shaped = [g.reshape(w.shape) for g, w in zip((dq_in, dq_out, di_in, di_out), (w_one, w_two, wi_one, wi_two))]
        return (loss.reshape(()), d_table) + tuple(shaped)

    return jax.shard_map(local_step, mesh=mesh, in_specs=(P("dp", None), P(), P(), P(), P(), P("dp", None), P(), P(), P("dp")), out_specs=(P(), P("dp", None), P(), P(), P(), P()), check_vma=False)
```
